256 devices in a mesh: grp: 4 (over z_lo), au: 4 (over z_hi, core), vert: 16 (over y, x).
Axes of the slice: x: 4, y: 4, z: 8 (z_hi: 2, z_lo: 4; z = z_hi * 4 + z_lo), core: 2. Of those that a mesh axis runs over, the one named last changes fastest.
Arguments:
- visibility: float32 [65536, 2], P(('grp', 'au', 'vert')), may hold values from -6 to 6
- destination: int32 [65536, 1], P(('grp', 'au', 'vert')), may hold values from 0 to 63; in each aligned block of 256 rows (0 to 255, 256 to 511, ...) at most 16 rows name the same one
- tile_slot: int32 [65536], P(('grp', 'au', 'vert')), may hold values from 0 to 63
- offsets: int32 [65536, 2], P(('grp', 'au', 'vert')), may hold values from 0 to 120
- taper: float32 [8], replicated, may hold values from 0.2 to 1
Outputs:
- dirty_facet: float32 [512, 512], P(('grp', 'au', 'vert'))
The draws below stay inside these ranges and needn't reach their ends.
Inputs may be any that keep to these rules, and one draw needn't show every extreme that they name: `destination`: among the rows of one device (aligned blocks of 256 rows) no grid block is named more than 16 times, and in some blocks one is named exactly 16 times. `tile_slot`: A tile number within the owning grid block. `offsets`: the kernel's 8 taps stay inside the tile.
All inputs are finite; a program needn't handle non-finite values.
Results may differ from the reference program's by a relative error of at most 0.0003.
Values sent between devices are 32-bit elements.
A program may use at most 64 MiB of HBM per device.

```python
import math
import jax
import jax.numpy as jnp
import numpy as np
from jax import lax

TILE = 128
SUP = 8
ROWS_DEV = 2048
COLS_DEV = 512
VIS_DEV = 256
IMG = 512
NU = 8192
NV = 8192
CAP = 16
VIS_TOTAL = 65536
TILES_DEV = 64
N_AU = 4
N_VERT = 16


def plant(result, own_key, smallest, top_value):
    extent = result.shape
    place = [jax.random.randint(jax.random.fold_in(own_key, axis), (), 0, extent[axis]) for axis in range(len(extent))]
    result = result.at[tuple(place)].set(smallest)
    longest = extent.index(max(extent))
    place[longest] = (place[longest] + 1) % extent[longest]
    return result.at[tuple(place)].set(top_value)


def block_scale(own_key, extent, cuts, low, top_value):
    loudness = 1.0
    for dim, parts in cuts:
        heights = jax.random.uniform(jax.random.fold_in(jax.random.fold_in(own_key, 6), dim), (parts,), jnp.float32, low / len(cuts), top_value / len(cuts))
        loudness = loudness * jnp.repeat(jnp.exp(heights), extent[dim] // parts).reshape((-1,) + (1,) * (len(extent) - 1 - dim))
    return loudness


def shared_out(stream_key, own, number, rows, number_of, top, bound, lean):
    order = jax.random.permutation(stream_key, number_of)
    packed, ordinary = load_shares(number_of, rows * top, bound, lean, True), load_shares(number_of, rows * top, bound, lean, False)
    places = jnp.arange(number_of)

    def named(tallies, offset_by):
        used = int((tallies > 0).sum())
        fixed = max(1, used // 4)
        shifted = fixed + (places - fixed + offset_by * (used - fixed)) % max(1, number_of - fixed)
        return jnp.zeros((number_of,), jnp.int32).at[order[jnp.where(places < fixed, places, shifted)]].set(jnp.asarray(tallies, jnp.int32))

    tallies = jnp.where(number % 4 == 0, named(packed, number // 4), named(ordinary, number - number // 4 - 1))
    mixed = jax.random.permutation(jax.random.fold_in(own, 3), number_of)
    source_of, taker = mixed[0:number_of // 2 * 2:2], mixed[1:number_of // 2 * 2:2]
    slack = jnp.minimum(tallies[source_of] - 1, bound - tallies[taker]) // 2
    slack = jnp.where((source_of == order[0]) | (taker == order[0]) | (tallies[taker] == 0), 0, jnp.maximum(slack, 0))
    shifted = jax.random.randint(jax.random.fold_in(own, 4), (number_of // 2,), 0, 1 << 20) % (slack + 1)
    tallies = tallies.at[source_of].add(-shifted).at[taker].add(shifted)
    members = jnp.searchsorted(jnp.cumsum(tallies), jnp.arange(rows * top), side="right").astype(jnp.int32)
    grid = members.reshape(top, rows).T
    grid = grid[jax.random.permutation(jax.random.fold_in(own, 1), rows)]
    offset_by = jax.random.randint(jax.random.fold_in(own, 2), (rows, 1), 0, top)
    return jnp.take_along_axis(grid, (jnp.arange(top)[None, :] + offset_by) % top, axis=1)


def load_shares(count, total, reach, slope, full):
    loads = [(1 << 20) // math.isqrt(grade ** slope) + 1 for grade in range(1, count + 1)]
    largest = reach if full else min(reach, max(-(-total // count), total * loads[0] // sum(loads)))
    least = 1 if total - largest >= count - 1 else 0
    given, rest = [largest] + [least] * (count - 1), total - largest - least * (count - 1)
    while rest > 0:
        free = [i for i in range(1, count) if given[i] < largest] or [i for i in range(1, count) if given[i] < reach]
        pool, budget = sum([loads[i] for i in free]), rest
        for i in free:
            extra = min(reach - given[i], max(1, budget * loads[i] // pool), rest)
            given[i] = given[i] + extra
            rest = rest - extra
    return np.array(given)


def normal_values(key, dims, scale, bound, pieces=(), held_as=jnp.bfloat16):
    array = jax.random.normal(key, dims, jnp.float32) * scale
    if len(pieces) > 0:
        array = block_scale(key, dims, pieces, -0.22, 0.18) * array
    return jnp.clip(array, min=-bound, max=bound).astype(held_as)


def setup_inputs(seed: int = 0) -> dict:
    streams_of = jax.random.split(jax.random.key(seed), 6)
    visibility = normal_values(streams_of[0], (VIS_TOTAL, 2), 1.0, 6.0, ((0, 256),), jnp.float32)
    destination_keys = jax.random.split(jax.random.fold_in(streams_of[1], 1), VIS_TOTAL // VIS_DEV)
    destination_turns = jax.random.permutation(jax.random.fold_in(streams_of[1], 3), VIS_TOTAL // VIS_DEV)
    destination = jax.vmap(lambda own, number: shared_out(jax.random.fold_in(streams_of[1], 2), own, number, VIS_DEV, N_AU * N_VERT, 1, CAP, 2))(destination_keys, destination_turns).reshape((VIS_TOTAL, 1))
    tile_slot = plant(jax.random.randint(streams_of[2], (VIS_TOTAL,), 0, TILES_DEV), jax.random.fold_in(streams_of[2], 1), 0, TILES_DEV - 1).astype(jnp.int32)
    offsets = plant(jax.random.randint(streams_of[3], (VIS_TOTAL, 2), 0, TILE - SUP + 1), jax.random.fold_in(streams_of[3], 1), 0, TILE - SUP).astype(jnp.int32)
    taper = jnp.clip(jax.random.uniform(streams_of[4], (SUP,), jnp.float32, 0.2, 1.0), 0.2, 1.0)
    return dict(visibility=visibility, destination=destination, tile_slot=tile_slot, offsets=offsets, taper=taper)


def matmul(factor_a, factor_b):
    return jnp.dot(factor_a, factor_b, precision=lax.Precision.HIGHEST, preferred_element_type=jnp.float32)

def phases(pixels, grid_cells, modulus):
    turn_count = pixels[:, None] * (grid_cells[None, :] - modulus // 2) % modulus
    angles = turn_count.astype(jnp.float32) * (2.0 * math.pi / modulus)
    return (jnp.cos(angles), jnp.sin(angles))

def reference(visibility, destination, tile_slot, offsets, taper):
    tiles_across = COLS_DEV // TILE
    target = destination[:, 0]
    row_anchor = target // N_VERT * ROWS_DEV + tile_slot // tiles_across * TILE + offsets[:, 0]
    col_anchor = target % N_VERT * COLS_DEV + tile_slot % tiles_across * TILE + offsets[:, 1]
    tap_range = jnp.arange(SUP, dtype=jnp.int32)
    row_index = row_anchor[:, None, None] + tap_range[None, :, None]
    col_index = col_anchor[:, None, None] + tap_range[None, None, :]
    kernel = taper[:, None] * taper[None, :]
    grid_re = jnp.zeros((NU, NV), jnp.float32).at[row_index, col_index].add(visibility[:, 0, None, None] * kernel[None])
    grid_im = jnp.zeros((NU, NV), jnp.float32).at[row_index, col_index].add(visibility[:, 1, None, None] * kernel[None])
    pixels = jnp.arange(IMG, dtype=jnp.int32) - IMG // 2
    cos_v, sin_v = phases(pixels, jnp.arange(NV, dtype=jnp.int32), NV)
    part_re = matmul(grid_re, cos_v.T) - matmul(grid_im, sin_v.T)
    part_im = matmul(grid_re, sin_v.T) + matmul(grid_im, cos_v.T)
    cos_u, sin_u = phases(pixels, jnp.arange(NU, dtype=jnp.int32), NU)
    normalise = 1.0 / (SUP * math.sqrt(VIS_TOTAL))
    return (matmul(cos_u, part_re) - matmul(sin_u, part_im)) * normalise
```

```python
import math

import jax
import jax.numpy as jnp
from jax import lax
from jax.experimental import pallas as pl
from jax.experimental.pallas import tpu as pltpu
from jax.sharding import PartitionSpec as P

TILE = 128
SUP = 8
ROWS_DEV = 2048
COLS_DEV = 512
IMG = 512
CELLS = 8192
MESH = pl.DeviceIdType.MESH

RING = 8
OWN = 32
ROWS = 64
HALF = IMG // 2
VIS = 256


def sincos(turns):
    turns = turns - jnp.floor(turns + 0.5)
    square = turns * turns
    sine = jnp.full_like(turns, -(math.pi**11) / math.factorial(11))
    for order in (9, 7, 5, 3, 1):
        sign = 1.0 if order % 4 == 1 else -1.0
        sine = sine * square + sign * math.pi**order / math.factorial(order)
    sine = sine * turns
    cosine = jnp.full_like(turns, math.pi**12 / math.factorial(12))
    for order in (10, 8, 6, 4, 2, 0):
        sign = 1.0 if order % 4 == 0 else -1.0
        cosine = cosine * square + sign * math.pi**order / math.factorial(order)
    return 1.0 - 2.0 * sine * sine, 2.0 * sine * cosine


def times(a, b):
    return a[0] * b[0] - a[1] * b[1], a[0] * b[1] + a[1] * b[0]


def stack(a, b):
    return jnp.concatenate([a[0], b[0]], axis=0), jnp.concatenate([a[1], b[1]], axis=0)


def split(value):
    high = value.astype(jnp.bfloat16)
    return high, (value - high.astype(jnp.float32)).astype(jnp.bfloat16)


def taper_sum(taper, pixel):
    step = sincos(pixel * (1.0 / CELLS))
    total = (jnp.full_like(pixel, taper[SUP - 1]), jnp.zeros_like(pixel))
    for tap in range(SUP - 2, -1, -1):
        re, im = times(total, step)
        total = (re + taper[tap], im)
    return total


def rows_of(shape):
    return lax.broadcasted_iota(jnp.int32, shape, 0)


def lanes_of(shape):
    return lax.broadcasted_iota(jnp.int32, shape, 1)


def phases(fields, first_pixel, v_ref, w_ref):
    re, im, x, y = (fields[i : i + 1, :] for i in range(4))
    row = rows_of((8, VIS))
    rowf = row.astype(jnp.float32)
    unit = 1.0 / CELLS
    col = sincos((rowf + 0.5) * y * unit)
    line = sincos(((first_pixel + 2.0 * rowf) * x - 0.5 * y) * unit)
    power = jnp.where(row < 5, 8 << jnp.minimum(row, 4), jnp.where(row == 7, 1, 16 << jnp.maximum(row - 5, 0)))
    turn = sincos(power.astype(jnp.float32) * jnp.where(row < 5, y, x) * unit)

    def step(i):
        return turn[0][i : i + 1, :], turn[1][i : i + 1, :]

    line = times((re, im), line)
    tiles = [stack(line, times(line, step(5)))]
    tiles.append(times(tiles[0], step(6)))
    tiles += [times(tile, step(7)) for tile in tiles]
    for i, tile in enumerate(tiles):
        for part in range(2):
            high, low = split(tile[part])
            w_ref[64 * part + 16 * i : 64 * part + 16 * i + 16, :] = high
            w_ref[128 + 64 * part + 16 * i : 128 + 64 * part + 16 * i + 16, :] = low
    tiles = [stack(col, times(col, step(0)))]
    for level in range(1, 5):
        tiles += [times(tile, step(level)) for tile in tiles]
    for i, tile in enumerate(tiles):
        for part in range(2):
            high, low = split(tile[part])
            v_ref[256 * part + 16 * i : 256 * part + 16 * i + 16, 0:VIS] = high
            v_ref[256 * part + 16 * i : 256 * part + 16 * i + 16, VIS : 2 * VIS] = low


def kernel(
    vis_hbm, dest_hbm, slot_hbm, off_hbm, taper_hbm, out_ref,
    vis, dest, slot, off, taper, fields, v_ref, w_ref, acc, tt, sends, recvs,
    load_sem, a_send, a_recv, b_send, b_recv,
):
    grp, au, vert = lax.axis_index("grp"), lax.axis_index("au"), lax.axis_index("vert")
    core = au % 2
    z = (au // 2) * 4 + grp
    y, x = vert // 4, vert % 4

    def ring_peer(offset):
        there = (z + offset) % RING
        return there % 4, (there // 4) * 2 + core, vert

    shifts = [(c, b, a) for c in range(2) for b in range(4) for a in range(4)]
    shifts.sort(key=lambda s: -(min(s[1], 4 - s[1]) + min(s[2], 4 - s[2]) + 0.5 * s[0]))
    shifts = shifts[:-1]

    def own_index(shift):
        return ((core + shift[0]) % 2) * 16 + ((y + shift[1]) % 4) * 4 + (x + shift[2]) % 4

    def own_peer(shift):
        return grp, (au // 2) * 2 + (core + shift[0]) % 2, ((y + shift[1]) % 4) * 4 + (x + shift[2]) % 4

    barrier = pltpu.get_barrier_semaphore()
    for offset in range(1, RING):
        pl.semaphore_signal(barrier, inc=1, device_id=ring_peer(offset), device_id_type=MESH)
    for shift in shifts:
        pl.semaphore_signal(barrier, inc=1, device_id=own_peer(shift), device_id_type=MESH)

    loads = [
        pltpu.make_async_copy(src, dst, load_sem.at[i])
        for i, (src, dst) in enumerate(
            ((vis_hbm, vis), (dest_hbm, dest), (slot_hbm, slot), (off_hbm, off), (taper_hbm, taper))
        )
    ]
    for load in loads:
        load.start()
    for load in loads[:4]:
        load.wait()
    target, tile = dest[...], slot[...]
    row0 = target // 16 * ROWS_DEV + tile // 4 * TILE + off[0:1, :]
    col0 = target % 16 * COLS_DEV + tile % 4 * TILE + off[1:2, :]
    fields[0, 0:2, :] = vis[...]
    fields[0, 2:3, :] = (row0 - CELLS // 2).astype(jnp.float32)
    fields[0, 3:4, :] = (col0 - CELLS // 2).astype(jnp.float32)

    pl.semaphore_wait(barrier, RING - 1 + len(shifts))
    order = [1, 7, 2, 6, 3, 5, 4]
    gathers = {}
    for offset in order[::-1]:
        gathers[offset] = pltpu.make_async_remote_copy(
            src_ref=fields.at[0],
            dst_ref=fields.at[offset],
            send_sem=a_send.at[offset],
            recv_sem=a_recv.at[offset],
            device_id=ring_peer(offset),
            device_id_type=MESH,
        )
        gathers[offset].start()

    position = grp * 2 + au // 2
    first_pixel = (position * ROWS - HALF).astype(jnp.float32)
    loads[4].wait()
    taps = [taper[i] for i in range(SUP)]
    lane = lanes_of((8, 128))
    left = lane < 64
    within = lane % 64
    pixel = first_pixel + (2 * (within % 32) + within // 32).astype(jnp.float32)
    norm = 1.0 / (SUP * math.sqrt(65536))
    line_re, line_im = taper_sum(taps, pixel)
    line_taper = (line_re * norm, line_im * norm)

    def table(i, carry):
        k = (rows_of((8, 128)) + 8 * i).astype(jnp.float32)
        pair = times(taper_sum(taps, jnp.where(left, k, -1.0 - k)), line_taper)
        rows = pl.ds(pl.multiple_of(8 * i, 8), 8)
        tt[0, rows, :] = pair[0]
        tt[1, rows, :] = pair[1]
        return carry

    lax.fori_loop(0, HALF // 8, table, 0)

    for index, offset in enumerate([0] + order):
        if offset:
            gathers[offset].wait_recv()
        phases(fields[offset], first_pixel, v_ref.at[index % 2], w_ref.at[index % 2])
        weights = w_ref[index % 2]
        part = None
        for half in range(2):
            product = lax.dot_general(
                v_ref[index % 2, :, half * VIS : (half + 1) * VIS],
                weights,
                (((1,), (1,)), ((), ())),
                preferred_element_type=jnp.float32,
            )
            part = product if part is None else part + product
        if index == 0:
            acc[...] = part
        else:
            acc[...] += part

    for i in range(2):
        rows = slice(128 * i, 128 * i + 128)
        cos_sum = acc[rows, 0:128] + acc[rows, 128:256]
        rows2 = slice(256 + 128 * i, 256 + 128 * i + 128)
        sin_sum = acc[rows2, 0:128] + acc[rows2, 128:256]
        minus = cos_sum - pltpu.roll(sin_sum, 64, 1)
        plus = pltpu.roll(cos_sum, 64, 1) + sin_sum
        mask = lanes_of((128, 128)) < 64
        facet = tt[0, rows, :] * jnp.where(mask, minus, plus) - tt[1, rows, :] * jnp.where(mask, plus, minus)
        facet = facet.T
        for group in range(4):
            for t in range(4):
                sends[pl.ds(64 * t + 2 * group + i, 8, stride=8), :] = facet[
                    32 * group + 8 * t : 32 * group + 8 * t + 8, :
                ]

    exchanges = []
    for i, shift in enumerate(shifts):
        start = pl.multiple_of(8 * own_index(shift), 8)
        exchanges.append(
            pltpu.make_async_remote_copy(
                src_ref=sends.at[pl.ds(start, 8), :],
                dst_ref=recvs.at[i],
                send_sem=b_send.at[i],
                recv_sem=b_recv.at[i],
                device_id=own_peer(shift),
                device_id_type=MESH,
            )
        )
        exchanges[-1].start()
    mine = pl.multiple_of(8 * (core * 16 + vert), 8)
    total = sends[pl.ds(mine, 8), :]
    for i in range(len(shifts) - 1, -1, -1):
        exchanges[i].wait_recv()
        total = total + recvs[i]
    mirrored = jnp.take_along_axis(total, 127 - lane, axis=1)
    for e in range(2):
        for h in range(2):
            out_ref[e : e + 1, 256 + 128 * h : 384 + 128 * h] = total[2 * e + h : 2 * e + h + 1, :]
            out_ref[e : e + 1, 128 * (1 - h) : 128 * (2 - h)] = mirrored[4 + 2 * e + h : 5 + 2 * e + h, :]
    for offset in order:
        gathers[offset].wait_send()
    for exchange in exchanges:
        exchange.wait_send()


def body(visibility, destination, tile_slot, offsets, taper):
    any_space = pl.BlockSpec(memory_space=pl.ANY)
    return pl.pallas_call(
        kernel,
        out_shape=jax.ShapeDtypeStruct((2, IMG), jnp.float32),
        in_specs=[any_space] * 5,
        out_specs=pl.BlockSpec(memory_space=pltpu.VMEM),
        scratch_shapes=[
            pltpu.VMEM((2, VIS), jnp.float32),
            pltpu.VMEM((1, VIS), jnp.int32),
            pltpu.VMEM((1, VIS), jnp.int32),
            pltpu.VMEM((2, VIS), jnp.int32),
            pltpu.SMEM((SUP,), jnp.float32),
            pltpu.VMEM((RING, 4, VIS), jnp.float32),
            pltpu.VMEM((2, IMG, 2 * VIS), jnp.bfloat16),
            pltpu.VMEM((2, 4 * ROWS, VIS), jnp.bfloat16),
            pltpu.VMEM((IMG, 4 * ROWS), jnp.float32),
            pltpu.VMEM((2, HALF, 128), jnp.float32),
            pltpu.VMEM((OWN * 8, 128), jnp.float32),
            pltpu.VMEM((OWN - 1, 8, 128), jnp.float32),
            pltpu.SemaphoreType.DMA((5,)),
            pltpu.SemaphoreType.DMA((RING,)),
            pltpu.SemaphoreType.DMA((RING,)),
            pltpu.SemaphoreType.DMA((OWN - 1,)),
            pltpu.SemaphoreType.DMA((OWN - 1,)),
        ],
        compiler_params=pltpu.CompilerParams(collective_id=0, has_side_effects=True),
    )(visibility.T, destination.T, tile_slot.reshape(1, -1), offsets.T, taper)


def solution(mesh):
    return jax.shard_map(
        body,
        mesh=mesh,
        in_specs=(
            P(("grp", "au", "vert"), None),
            P(("grp", "au", "vert"), None),
            P(("grp", "au", "vert")),
            P(("grp", "au", "vert"), None),
            P(),
        ),
        out_specs=P(("grp", "au", "vert"), None),
        check_vma=False,
    )
```

```python
import math

import jax
import jax.numpy as jnp
from jax import lax
from jax.experimental import pallas as pl
from jax.experimental.pallas import tpu as pltpu
from jax.sharding import PartitionSpec as P

TILE = 128
SUP = 8
ROWS_DEV = 2048
COLS_DEV = 512
IMG = 512
CELLS = 8192
MESH = pl.DeviceIdType.MESH

RING = 8
OWN = 32
ROWS = 64
HALF = IMG // 2
VIS = 256


def sincos(turns):
    turns = turns - jnp.floor(turns + 0.5)
    square = turns * turns
    sine = jnp.full_like(turns, -(math.pi**11) / math.factorial(11))
    for order in (9, 7, 5, 3, 1):
        sign = 1.0 if order % 4 == 1 else -1.0
        sine = sine * square + sign * math.pi**order / math.factorial(order)
    sine = sine * turns
    cosine = jnp.full_like(turns, math.pi**12 / math.factorial(12))
    for order in (10, 8, 6, 4, 2, 0):
        sign = 1.0 if order % 4 == 0 else -1.0
        cosine = cosine * square + sign * math.pi**order / math.factorial(order)
    return 1.0 - 2.0 * sine * sine, 2.0 * sine * cosine


def times(a, b):
    return a[0] * b[0] - a[1] * b[1], a[0] * b[1] + a[1] * b[0]


def stack(a, b):
    return jnp.concatenate([a[0], b[0]], axis=0), jnp.concatenate([a[1], b[1]], axis=0)


def split(value):
    high = value.astype(jnp.bfloat16)
    return high, (value - high.astype(jnp.float32)).astype(jnp.bfloat16)


def taper_sum(taper, pixel):
    step = sincos(pixel * (1.0 / CELLS))
    total = (jnp.full_like(pixel, taper[SUP - 1]), jnp.zeros_like(pixel))
    for tap in range(SUP - 2, -1, -1):
        re, im = times(total, step)
        total = (re + taper[tap], im)
    return total


def rows_of(shape):
    return lax.broadcasted_iota(jnp.int32, shape, 0)


def lanes_of(shape):
    return lax.broadcasted_iota(jnp.int32, shape, 1)


def phases(fields, first_pixel, v_ref, w_ref):
    re, im, x, y = (fields[i : i + 1, :] for i in range(4))
    row = rows_of((8, VIS))
    rowf = row.astype(jnp.float32)
    unit = 1.0 / CELLS
    col = sincos((rowf + 0.5) * y * unit)
    line = sincos(((first_pixel + 2.0 * rowf) * x - 0.5 * y) * unit)
    power = jnp.where(row < 5, 8 << jnp.minimum(row, 4), jnp.where(row == 7, 1, 16 << jnp.maximum(row - 5, 0)))
    turn = sincos(power.astype(jnp.float32) * jnp.where(row < 5, y, x) * unit)

    def step(i):
        return turn[0][i : i + 1, :], turn[1][i : i + 1, :]

    line = times((re, im), line)
    tiles = [stack(line, times(line, step(5)))]
    tiles.append(times(tiles[0], step(6)))
    tiles += [times(tile, step(7)) for tile in tiles]
    for i, tile in enumerate(tiles):
        for part in range(2):
            high, low = split(tile[part])
            w_ref[64 * part + 16 * i : 64 * part + 16 * i + 16, :] = high
            w_ref[128 + 64 * part + 16 * i : 128 + 64 * part + 16 * i + 16, :] = low
    tiles = [stack(col, times(col, step(0)))]
    for level in range(1, 5):
        tiles += [times(tile, step(level)) for tile in tiles]
    for i, tile in enumerate(tiles):
        for part in range(2):
            high, low = split(tile[part])
            v_ref[256 * part + 16 * i : 256 * part + 16 * i + 16, 0:VIS] = high
            v_ref[256 * part + 16 * i : 256 * part + 16 * i + 16, VIS : 2 * VIS] = low


def kernel(
    vis_hbm, dest_hbm, slot_hbm, off_hbm, taper_hbm, out_ref,
    vis, dest, slot, off, taper, fields, v_ref, w_ref, acc, sends, recvs,
    load_sem, a_send, a_recv, b_send, b_recv, plane_sem, pair_sem,
):
    grp, au, vert = lax.axis_index("grp"), lax.axis_index("au"), lax.axis_index("vert")
    core = au % 2
    z = (au // 2) * 4 + grp
    y, x = vert // 4, vert % 4

    def ring_peer(offset):
        there = (z + offset) % RING
        return there % 4, (there // 4) * 2 + core, vert

    shifts = [(c, b, a) for c in range(2) for b in range(4) for a in range(4)]
    shifts.sort(key=lambda s: -(min(s[1], 4 - s[1]) + min(s[2], 4 - s[2]) + 0.5 * s[0]))
    shifts = shifts[:-1]

    def own_vert(shift):
        return ((y + shift[1]) % 4) * 4 + (x + shift[2]) % 4

    def own_peer(shift):
        return grp, (au // 2) * 2 + (core + shift[0]) % 2, own_vert(shift)

    def signal(sem, peers):
        for peer in peers:
            pl.semaphore_signal(sem, inc=1, device_id=peer, device_id_type=MESH)

    row = [own_peer((0, 0, a)) for a in range(1, 4)]
    column = [own_peer((0, b, 0)) for b in range(1, 4)]
    pair = own_peer((1, 0, 0))
    ring = [ring_peer(offset) for offset in range(1, RING)]
    barrier = pltpu.get_barrier_semaphore()
    signal(barrier, ring + row + column + [pair])

    loads = [
        pltpu.make_async_copy(src, dst, load_sem.at[i])
        for i, (src, dst) in enumerate(
            ((vis_hbm, vis), (dest_hbm, dest), (slot_hbm, slot), (off_hbm, off), (taper_hbm, taper))
        )
    ]
    for load in loads:
        load.start()
    for load in loads[:4]:
        load.wait()
    target, tile = dest[...], slot[...]
    row0 = target // 16 * ROWS_DEV + tile // 4 * TILE + off[0:1, :]
    col0 = target % 16 * COLS_DEV + tile % 4 * TILE + off[1:2, :]
    fields[0, 0:2, :] = vis[...]
    fields[0, 2:3, :] = (row0 - CELLS // 2).astype(jnp.float32)
    fields[0, 3:4, :] = (col0 - CELLS // 2).astype(jnp.float32)

    pl.semaphore_wait(barrier, len(ring + row + column) + 1)
    order = [1, 7, 2, 6, 3, 5, 4]
    gathers = {}
    for offset in order[::-1]:
        gathers[offset] = pltpu.make_async_remote_copy(
            src_ref=fields.at[0],
            dst_ref=fields.at[offset],
            send_sem=a_send.at[offset],
            recv_sem=a_recv.at[offset],
            device_id=ring_peer(offset),
            device_id_type=MESH,
        )
        gathers[offset].start()
    signal(plane_sem, row + [pair])

    position = grp * 2 + au // 2
    first_pixel = (position * ROWS - HALF).astype(jnp.float32)

    def project(index):
        weights = w_ref[index % 2]
        part = None
        for half in range(2):
            product = lax.dot_general(
                v_ref[index % 2, :, half * VIS : (half + 1) * VIS],
                weights,
                (((1,), (1,)), ((), ())),
                preferred_element_type=jnp.float32,
            )
            part = product if part is None else part + product
        if index == 0:
            acc[...] = part
        else:
            acc[...] += part

    phases(fields[0], first_pixel, v_ref.at[0], w_ref.at[0])
    loads[4].wait()
    taps = [taper[i] for i in range(SUP)]
    lane, level = lanes_of((8, 128)), rows_of((8, 128))
    within = lane % 64
    line_re, line_im = taper_sum(taps, first_pixel + (2 * (within % 32) + within // 32).astype(jnp.float32))
    norm = 1.0 / (SUP * math.sqrt(65536))
    line_re, line_im = line_re[0:1, :] * norm, line_im[0:1, :] * norm
    column_pixel = lane + 128 * (level % 2)
    col_re, col_im = taper_sum(taps, jnp.where(level < 2, column_pixel, -1 - column_pixel).astype(jnp.float32))
    pl.semaphore_wait(plane_sem, len(row) + 1)
    signal(pair_sem, [pair])

    for index, offset in enumerate(order, 1):
        gathers[offset].wait_recv()
        project(index - 1)
        phases(fields[offset], first_pixel, v_ref.at[index % 2], w_ref.at[index % 2])
    project(RING - 1)

    for i in range(2):
        rows = slice(128 * i, 128 * i + 128)
        cos_sum = acc[rows, 0:128] + acc[rows, 128:256]
        rows = slice(256 + 128 * i, 256 + 128 * i + 128)
        sin_sum = acc[rows, 0:128] + acc[rows, 128:256]
        minus = cos_sum - pltpu.roll(sin_sum, 64, 1)
        plus = pltpu.roll(cos_sum, 64, 1) + sin_sum
        mask = lanes_of((128, 128)) < 64
        real, imag = jnp.where(mask, minus, plus), jnp.where(mask, plus, minus)
        real, imag = (line_re * real - line_im * imag).T, (line_re * imag + line_im * real).T
        for group in range(4):
            part = slice(32 * group, 32 * group + 32)
            tap = slice(group // 2 * 2 + i, group // 2 * 2 + i + 1)
            facet = col_re[tap, :] * real[part, :] - col_im[tap, :] * imag[part, :]
            for t in range(4):
                sends[pl.ds(64 * t + 2 * group + i, 8, stride=8), :] = facet[8 * t : 8 * t + 8, :]

    pl.semaphore_wait(pair_sem, 1)
    exchanges = []
    for i, shift in enumerate(shifts):
        start = pl.multiple_of(8 * ((core + shift[0]) % 2 * 16 + own_vert(shift)), 8)
        exchanges.append(
            pltpu.make_async_remote_copy(
                src_ref=sends.at[pl.ds(start, 8), :],
                dst_ref=recvs.at[i],
                send_sem=b_send.at[i],
                recv_sem=b_recv.at[i],
                device_id=own_peer(shift),
                device_id_type=MESH,
            )
        )
        exchanges[-1].start()
    mine = pl.multiple_of(8 * (core * 16 + vert), 8)
    total = sends[pl.ds(mine, 8), :]
    for offset in order:
        gathers[offset].wait_send()
    for i in range(len(shifts) - 1, -1, -1):
        exchanges[i].wait_recv()
        total = total + recvs[i]
    mirrored = jnp.take_along_axis(total, 127 - lane, axis=1)
    for e in range(2):
        for h in range(2):
            out_ref[e : e + 1, 256 + 128 * h : 384 + 128 * h] = total[2 * e + h : 2 * e + h + 1, :]
            out_ref[e : e + 1, 128 * (1 - h) : 128 * (2 - h)] = mirrored[4 + 2 * e + h : 5 + 2 * e + h, :]
    for exchange in exchanges:
        exchange.wait_send()


def body(visibility, destination, tile_slot, offsets, taper):
    any_space = pl.BlockSpec(memory_space=pl.ANY)
    return pl.pallas_call(
        kernel,
        out_shape=pltpu.VMEM((2, IMG), jnp.float32),
        in_specs=[any_space] * 5,
        out_specs=pl.BlockSpec(memory_space=pltpu.VMEM),
        scratch_shapes=[
            pltpu.VMEM((2, VIS), jnp.float32),
            pltpu.VMEM((1, VIS), jnp.int32),
            pltpu.VMEM((1, VIS), jnp.int32),
            pltpu.VMEM((2, VIS), jnp.int32),
            pltpu.SMEM((SUP,), jnp.float32),
            pltpu.VMEM((RING, 4, VIS), jnp.float32),
            pltpu.VMEM((2, IMG, 2 * VIS), jnp.bfloat16),
            pltpu.VMEM((2, 4 * ROWS, VIS), jnp.bfloat16),
            pltpu.VMEM((IMG, 4 * ROWS), jnp.float32),
            pltpu.VMEM((OWN * 8, 128), jnp.float32),
            pltpu.VMEM((OWN - 1, 8, 128), jnp.float32),
            pltpu.SemaphoreType.DMA((5,)),
            pltpu.SemaphoreType.DMA((RING,)),
            pltpu.SemaphoreType.DMA((RING,)),
            pltpu.SemaphoreType.DMA((OWN - 1,)),
            pltpu.SemaphoreType.DMA((OWN - 1,)),
            pltpu.SemaphoreType.REGULAR,
            pltpu.SemaphoreType.REGULAR,
        ],
        compiler_params=pltpu.CompilerParams(collective_id=0, has_side_effects=True),
    )(visibility.T, destination.T, tile_slot.reshape(1, -1), offsets.T, taper)


def solution(mesh):
    return jax.shard_map(
        body,
        mesh=mesh,
        in_specs=(
            P(("grp", "au", "vert"), None),
            P(("grp", "au", "vert"), None),
            P(("grp", "au", "vert")),
            P(("grp", "au", "vert"), None),
            P(),
        ),
        out_specs=P(("grp", "au", "vert"), None),
        check_vma=False,
    )
```

```python
import math

import jax
import jax.numpy as jnp
from jax import lax
from jax.experimental import pallas as pl
from jax.experimental.pallas import tpu as pltpu
from jax.sharding import PartitionSpec as P

TILE = 128
SUP = 8
ROWS_DEV = 2048
COLS_DEV = 512
IMG = 512
CELLS = 8192
MESH = pl.DeviceIdType.MESH

RING = 8
OWN = 32
ROWS = 64
HALF = IMG // 2
VIS = 256


def sincos(turns):
    turns = turns - jnp.floor(turns + 0.5)
    square = turns * turns
    sine = jnp.full_like(turns, -(math.pi**11) / math.factorial(11))
    for order in (9, 7, 5, 3, 1):
        sign = 1.0 if order % 4 == 1 else -1.0
        sine = sine * square + sign * math.pi**order / math.factorial(order)
    sine = sine * turns
    cosine = jnp.full_like(turns, math.pi**12 / math.factorial(12))
    for order in (10, 8, 6, 4, 2, 0):
        sign = 1.0 if order % 4 == 0 else -1.0
        cosine = cosine * square + sign * math.pi**order / math.factorial(order)
    return 1.0 - 2.0 * sine * sine, 2.0 * sine * cosine


def times(a, b):
    return a[0] * b[0] - a[1] * b[1], a[0] * b[1] + a[1] * b[0]


def stack(a, b):
    return jnp.concatenate([a[0], b[0]], axis=0), jnp.concatenate([a[1], b[1]], axis=0)


def split(value):
    high = value.astype(jnp.bfloat16)
    return high, (value - high.astype(jnp.float32)).astype(jnp.bfloat16)


def taper_sum(taper, pixel):
    step = sincos(pixel * (1.0 / CELLS))
    total = (jnp.full_like(pixel, taper[SUP - 1]), jnp.zeros_like(pixel))
    for tap in range(SUP - 2, -1, -1):
        re, im = times(total, step)
        total = (re + taper[tap], im)
    return total


def rows_of(shape):
    return lax.broadcasted_iota(jnp.int32, shape, 0)


def lanes_of(shape):
    return lax.broadcasted_iota(jnp.int32, shape, 1)


def phases(fields, first_pixel, v_ref, w_ref):
    re, im, x, y = (fields[i : i + 1, :] for i in range(4))
    row = rows_of((8, VIS))
    rowf = row.astype(jnp.float32)
    unit = 1.0 / CELLS
    col = sincos((rowf + 0.5) * y * unit)
    line = sincos(((first_pixel + 2.0 * rowf) * x - 0.5 * y) * unit)
    power = jnp.where(row < 5, 8 << jnp.minimum(row, 4), jnp.where(row == 7, 1, 16 << jnp.maximum(row - 5, 0)))
    turn = sincos(power.astype(jnp.float32) * jnp.where(row < 5, y, x) * unit)

    def step(i):
        return turn[0][i : i + 1, :], turn[1][i : i + 1, :]

    line = times((re, im), line)
    tiles = [stack(line, times(line, step(5)))]
    tiles.append(times(tiles[0], step(6)))
    tiles += [times(tile, step(7)) for tile in tiles]
    for i, tile in enumerate(tiles):
        for part in range(2):
            high, low = split(tile[part])
            w_ref[64 * part + 16 * i : 64 * part + 16 * i + 16, :] = high
            w_ref[128 + 64 * part + 16 * i : 128 + 64 * part + 16 * i + 16, :] = low
    tiles = [stack(col, times(col, step(0)))]
    for level in range(1, 5):
        tiles += [times(tile, step(level)) for tile in tiles]
    for i, tile in enumerate(tiles):
        for part in range(2):
            high, low = split(tile[part])
            v_ref[256 * part + 16 * i : 256 * part + 16 * i + 16, 0:VIS] = high
            v_ref[256 * part + 16 * i : 256 * part + 16 * i + 16, VIS : 2 * VIS] = low


def kernel(
    vis_hbm, dest_hbm, slot_hbm, off_hbm, taper_hbm, out_ref,
    vis, dest, slot, off, taper, fields, v_ref, w_ref, acc, sends, recvs,
    load_sem, a_send, a_recv, b_send, b_recv, plane_sem, pair_sem,
):
    grp, au, vert = lax.axis_index("grp"), lax.axis_index("au"), lax.axis_index("vert")
    core = au % 2
    z = (au // 2) * 4 + grp
    y, x = vert // 4, vert % 4

    def ring_peer(offset):
        there = (z + offset) % RING
        return there % 4, (there // 4) * 2 + core, vert

    shifts = [(c, b, a) for c in range(2) for b in range(4) for a in range(4)]
    shifts.sort(key=lambda s: -(min(s[1], 4 - s[1]) + min(s[2], 4 - s[2]) + 0.5 * s[0]))
    shifts = shifts[:-1]

    def own_vert(shift):
        return ((y + shift[1]) % 4) * 4 + (x + shift[2]) % 4

    def own_peer(shift):
        return grp, (au // 2) * 2 + (core + shift[0]) % 2, own_vert(shift)

    def signal(sem, peers):
        for peer in peers:
            pl.semaphore_signal(sem, inc=1, device_id=peer, device_id_type=MESH)

    row = [own_peer((0, 0, a)) for a in range(1, 4)]
    column = [own_peer((0, b, 0)) for b in range(1, 4)]
    pair = own_peer((1, 0, 0))
    ring = [ring_peer(offset) for offset in range(1, RING)]
    barrier = pltpu.get_barrier_semaphore()
    signal(barrier, ring + row + column + [pair])

    loads = [
        pltpu.make_async_copy(src, dst, load_sem.at[i])
        for i, (src, dst) in enumerate(
            ((vis_hbm, vis), (dest_hbm, dest), (slot_hbm, slot), (off_hbm, off), (taper_hbm, taper))
        )
    ]
    for load in loads:
        load.start()
    for load in loads[:4]:
        load.wait()
    target, tile = dest[...], slot[...]
    row0 = target // 16 * ROWS_DEV + tile // 4 * TILE + off[0:1, :]
    col0 = target % 16 * COLS_DEV + tile % 4 * TILE + off[1:2, :]
    fields[0, 0:2, :] = vis[...]
    fields[0, 2:3, :] = (row0 - CELLS // 2).astype(jnp.float32)
    fields[0, 3:4, :] = (col0 - CELLS // 2).astype(jnp.float32)

    pl.semaphore_wait(barrier, len(ring + row + column) + 1)
    order = [7, 6, 5, 1, 2, 3, 4]
    gathers = {}
    for offset in order[::-1]:
        gathers[offset] = pltpu.make_async_remote_copy(
            src_ref=fields.at[0],
            dst_ref=fields.at[offset],
            send_sem=a_send,
            recv_sem=a_recv.at[offset],
            device_id=ring_peer(offset),
            device_id_type=MESH,
        )
        gathers[offset].start()
    signal(plane_sem, row + [pair])

    position = grp * 2 + au // 2
    first_pixel = (position * ROWS - HALF).astype(jnp.float32)

    def project(index):
        weights = w_ref[index % 2]
        part = None
        for half in range(2):
            product = lax.dot_general(
                v_ref[index % 2, :, half * VIS : (half + 1) * VIS],
                weights,
                (((1,), (1,)), ((), ())),
                preferred_element_type=jnp.float32,
            )
            part = product if part is None else part + product
        if index == 0:
            acc[...] = part
        else:
            acc[...] += part

    phases(fields[0], first_pixel, v_ref.at[0], w_ref.at[0])
    loads[4].wait()
    taps = [taper[i] for i in range(SUP)]
    lane, level = lanes_of((8, 128)), rows_of((8, 128))
    within = lane % 64
    line_re, line_im = taper_sum(taps, first_pixel + (2 * (within % 32) + within // 32).astype(jnp.float32))
    norm = 1.0 / (SUP * math.sqrt(65536))
    line_re, line_im = line_re[0:1, :] * norm, line_im[0:1, :] * norm
    column_pixel = lane + 128 * (level % 2)
    col_re, col_im = taper_sum(taps, jnp.where(level < 2, column_pixel, -1 - column_pixel).astype(jnp.float32))

    for index, offset in enumerate(order, 1):
        gathers[offset].wait_recv()
        project(index - 1)
        if index == 4:
            pl.semaphore_wait(plane_sem, len(row) + 1)
            signal(pair_sem, [pair])
        phases(fields[offset], first_pixel, v_ref.at[index % 2], w_ref.at[index % 2])
    project(RING - 1)

    for i in range(2):
        rows = slice(128 * i, 128 * i + 128)
        cos_sum = acc[rows, 0:128] + acc[rows, 128:256]
        rows = slice(256 + 128 * i, 256 + 128 * i + 128)
        sin_sum = acc[rows, 0:128] + acc[rows, 128:256]
        minus = cos_sum - pltpu.roll(sin_sum, 64, 1)
        plus = pltpu.roll(cos_sum, 64, 1) + sin_sum
        mask = lanes_of((128, 128)) < 64
        real, imag = jnp.where(mask, minus, plus), jnp.where(mask, plus, minus)
        real, imag = (line_re * real - line_im * imag).T, (line_re * imag + line_im * real).T
        for group in range(4):
            part = slice(32 * group, 32 * group + 32)
            tap = slice(group // 2 * 2 + i, group // 2 * 2 + i + 1)
            facet = col_re[tap, :] * real[part, :] - col_im[tap, :] * imag[part, :]
            for t in range(4):
                sends[pl.ds(64 * t + 2 * group + i, 8, stride=8), :] = facet[8 * t : 8 * t + 8, :]

    pl.semaphore_wait(pair_sem, 1)
    for i, shift in enumerate(shifts):
        start = pl.multiple_of(8 * ((core + shift[0]) % 2 * 16 + own_vert(shift)), 8)
        pltpu.make_async_remote_copy(
            src_ref=sends.at[pl.ds(start, 8), :],
            dst_ref=recvs.at[i],
            send_sem=b_send,
            recv_sem=b_recv,
            device_id=own_peer(shift),
            device_id_type=MESH,
        ).start()
    mine = pl.multiple_of(8 * (core * 16 + vert), 8)
    total = sends[pl.ds(mine, 8), :]
    batch = pltpu.make_async_remote_copy(
        src_ref=recvs, dst_ref=recvs, send_sem=b_send, recv_sem=b_recv, device_id=pair, device_id_type=MESH
    )
    batch.wait_recv()
    for i in range(len(shifts)):
        total = total + recvs[i]
    mirrored = jnp.take_along_axis(total, 127 - lane, axis=1)
    for e in range(2):
        for h in range(2):
            out_ref[e : e + 1, 256 + 128 * h : 384 + 128 * h] = total[2 * e + h : 2 * e + h + 1, :]
            out_ref[e : e + 1, 128 * (1 - h) : 128 * (2 - h)] = mirrored[4 + 2 * e + h : 5 + 2 * e + h, :]
    batch.wait_send()
    rest = fields.at[pl.ds(1, RING - 1)]
    pltpu.make_async_remote_copy(
        src_ref=rest, dst_ref=rest, send_sem=a_send, recv_sem=a_recv.at[0], device_id=pair, device_id_type=MESH
    ).wait_send()


def body(visibility, destination, tile_slot, offsets, taper):
    any_space = pl.BlockSpec(memory_space=pl.ANY)
    return pl.pallas_call(
        kernel,
        out_shape=pltpu.VMEM((2, IMG), jnp.float32),
        in_specs=[any_space] * 5,
        out_specs=pl.BlockSpec(memory_space=pltpu.VMEM),
        scratch_shapes=[
            pltpu.VMEM((2, VIS), jnp.float32),
            pltpu.VMEM((1, VIS), jnp.int32),
            pltpu.VMEM((1, VIS), jnp.int32),
            pltpu.VMEM((2, VIS), jnp.int32),
            pltpu.SMEM((SUP,), jnp.float32),
            pltpu.VMEM((RING, 4, VIS), jnp.float32),
            pltpu.VMEM((2, IMG, 2 * VIS), jnp.bfloat16),
            pltpu.VMEM((2, 4 * ROWS, VIS), jnp.bfloat16),
            pltpu.VMEM((IMG, 4 * ROWS), jnp.float32),
            pltpu.VMEM((OWN * 8, 128), jnp.float32),
            pltpu.VMEM((OWN - 1, 8, 128), jnp.float32),
            pltpu.SemaphoreType.DMA((5,)),
            pltpu.SemaphoreType.DMA,
            pltpu.SemaphoreType.DMA((RING,)),
            pltpu.SemaphoreType.DMA,
            pltpu.SemaphoreType.DMA,
            pltpu.SemaphoreType.REGULAR,
            pltpu.SemaphoreType.REGULAR,
        ],
        compiler_params=pltpu.CompilerParams(collective_id=0, has_side_effects=True),
    )(visibility.T, destination.T, tile_slot.reshape(1, -1), offsets.T, taper)


def solution(mesh):
    return jax.shard_map(
        body,
        mesh=mesh,
        in_specs=(
            P(("grp", "au", "vert"), None),
            P(("grp", "au", "vert"), None),
            P(("grp", "au", "vert")),
            P(("grp", "au", "vert"), None),
            P(),
        ),
        out_specs=P(("grp", "au", "vert"), None),
        check_vma=False,
    )
```

```python
import math

import jax
import jax.numpy as jnp
from jax import lax
from jax.experimental import pallas as pl
from jax.experimental.pallas import tpu as pltpu
from jax.sharding import PartitionSpec as P

TILE = 128
SUP = 8
ROWS_DEV = 2048
COLS_DEV = 512
IMG = 512
CELLS = 8192
MESH = pl.DeviceIdType.MESH

RING = 8
OWN = 32
ROWS = 64
HALF = IMG // 2
VIS = 256


def sincos(turns):
    turns = turns - jnp.floor(turns + 0.5)
    square = turns * turns
    sine = jnp.full_like(turns, -(math.pi**11) / math.factorial(11))
    for order in (9, 7, 5, 3, 1):
        sign = 1.0 if order % 4 == 1 else -1.0
        sine = sine * square + sign * math.pi**order / math.factorial(order)
    sine = sine * turns
    cosine = jnp.full_like(turns, math.pi**12 / math.factorial(12))
    for order in (10, 8, 6, 4, 2, 0):
        sign = 1.0 if order % 4 == 0 else -1.0
        cosine = cosine * square + sign * math.pi**order / math.factorial(order)
    return 1.0 - 2.0 * sine * sine, 2.0 * sine * cosine


def times(a, b):
    return a[0] * b[0] - a[1] * b[1], a[0] * b[1] + a[1] * b[0]


def stack(a, b):
    return jnp.concatenate([a[0], b[0]], axis=0), jnp.concatenate([a[1], b[1]], axis=0)


def split(value):
    high = value.astype(jnp.bfloat16)
    return high, (value - high.astype(jnp.float32)).astype(jnp.bfloat16)


def taper_sum(taper, pixel):
    step = sincos(pixel * (1.0 / CELLS))
    total = (jnp.full_like(pixel, taper[SUP - 1]), jnp.zeros_like(pixel))
    for tap in range(SUP - 2, -1, -1):
        re, im = times(total, step)
        total = (re + taper[tap], im)
    return total


def rows_of(shape):
    return lax.broadcasted_iota(jnp.int32, shape, 0)


def lanes_of(shape):
    return lax.broadcasted_iota(jnp.int32, shape, 1)


def phases(fields, first_pixel, v_ref, w_ref):
    re, im, x, y = (fields[i : i + 1, :] for i in range(4))
    row = rows_of((8, VIS))
    rowf = row.astype(jnp.float32)
    unit = 1.0 / CELLS
    col = sincos((rowf + 0.5) * y * unit)
    line = sincos(((first_pixel + 2.0 * rowf) * x - 0.5 * y) * unit)
    power = jnp.where(row < 5, 8 << jnp.minimum(row, 4), jnp.where(row == 7, 1, 16 << jnp.maximum(row - 5, 0)))
    turn = sincos(power.astype(jnp.float32) * jnp.where(row < 5, y, x) * unit)

    def step(i):
        return turn[0][i : i + 1, :], turn[1][i : i + 1, :]

    line = times((re, im), line)
    tiles = [stack(line, times(line, step(5)))]
    tiles.append(times(tiles[0], step(6)))
    tiles += [times(tile, step(7)) for tile in tiles]
    for i, tile in enumerate(tiles):
        for part in range(2):
            high, low = split(tile[part])
            w_ref[64 * part + 16 * i : 64 * part + 16 * i + 16, :] = high
            w_ref[128 + 64 * part + 16 * i : 128 + 64 * part + 16 * i + 16, :] = low
    tiles = [stack(col, times(col, step(0)))]
    for level in range(1, 5):
        tiles += [times(tile, step(level)) for tile in tiles]
    for i, tile in enumerate(tiles):
        for part in range(2):
            high, low = split(tile[part])
            v_ref[256 * part + 16 * i : 256 * part + 16 * i + 16, 0:VIS] = high
            v_ref[256 * part + 16 * i : 256 * part + 16 * i + 16, VIS : 2 * VIS] = low


def kernel(
    vis_hbm, dest_hbm, slot_hbm, off_hbm, taper_hbm, out_ref,
    vis, dest, slot, off, taper, fields, v_ref, w_ref, acc, sends, recvs,
    load_sem, a_send, a_recv, b_send, b_recv, rounds, late_sem,
):
    grp, au, vert = lax.axis_index("grp"), lax.axis_index("au"), lax.axis_index("vert")
    core, half = au % 2, au // 2
    z = half * 4 + grp
    y, x = vert // 4, vert % 4

    shifts = [(c, b, a) for c in range(2) for b in range(4) for a in range(4)]
    shifts.sort(key=lambda s: -(min(s[1], 4 - s[1]) + min(s[2], 4 - s[2]) + 0.5 * s[0]))
    shifts = shifts[:-1]

    def own_vert(shift):
        return ((y + shift[1]) % 4) * 4 + (x + shift[2]) % 4

    def own_peer(shift):
        return grp, half * 2 + (core + shift[0]) % 2, own_vert(shift)

    def signal(sem, peer):
        pl.semaphore_signal(sem, inc=1, device_id=peer, device_id_type=MESH)

    def near(step):
        return (grp + step) % 4, au, vert

    def across(there):
        return there, (1 - half) * 2 + core, vert

    def inside(step):
        return (grp + step >= 0) & (grp + step < 4)

    pair = own_peer((1, 0, 0))
    plane = [own_peer((0, 0, 1)), own_peer((0, 0, 3)), own_peer((0, 1, 0)), own_peer((0, 3, 0)), pair]
    neighbours = len(plane) + inside(1).astype(jnp.int32) + inside(-1).astype(jnp.int32)

    def signal_near(sem):
        for peer in plane:
            signal(sem, peer)
        for step in (1, -1):

            @pl.when(inside(step))
            def _():
                signal(sem, near(step))

    def gather(peer):
        pltpu.make_async_remote_copy(
            src_ref=fields.at[z],
            dst_ref=fields.at[z],
            send_sem=a_send,
            recv_sem=a_recv.at[z],
            device_id=peer,
            device_id_type=MESH,
        ).start()

    def gather_near(distance):
        for step in (distance, -distance):

            @pl.when(inside(step))
            def _():
                gather(near(step))

    barrier = pltpu.get_barrier_semaphore()
    signal_near(barrier)

    @pl.when(half == 0)
    def _():
        for there in range(4):
            signal(barrier, across(there))

    loads = [
        pltpu.make_async_copy(src, dst, load_sem.at[i])
        for i, (src, dst) in enumerate(
            ((vis_hbm, vis), (dest_hbm, dest), (slot_hbm, slot), (off_hbm, off), (taper_hbm, taper))
        )
    ]
    for load in loads:
        load.start()
    for load in loads[:4]:
        load.wait()
    target, tile = dest[...], slot[...]
    row0 = target // 16 * ROWS_DEV + tile // 4 * TILE + off[0:1, :]
    col0 = target % 16 * COLS_DEV + tile % 4 * TILE + off[1:2, :]
    fields[z, 0:2, :] = vis[...]
    fields[z, 2:3, :] = (row0 - CELLS // 2).astype(jnp.float32)
    fields[z, 3:4, :] = (col0 - CELLS // 2).astype(jnp.float32)

    pl.semaphore_wait(barrier, neighbours + 4 * half)

    @pl.when(half == 1)
    def _():
        for there in range(4):
            gather(across(there))
        for there in range(4):
            signal(late_sem, across(there))

    gather_near(1)
    signal_near(rounds.at[0])
    position = grp * 2 + half
    first_pixel = (position * ROWS - HALF).astype(jnp.float32)

    def project(index):
        weights = w_ref[index % 2]
        part = None
        for low in range(2):
            product = lax.dot_general(
                v_ref[index % 2, :, low * VIS : (low + 1) * VIS],
                weights,
                (((1,), (1,)), ((), ())),
                preferred_element_type=jnp.float32,
            )
            part = product if part is None else part + product
        if index == 0:
            acc[...] = part
        else:
            acc[...] += part

    phases(fields[z], first_pixel, v_ref.at[0], w_ref.at[0])
    loads[4].wait()
    taps = [taper[i] for i in range(SUP)]
    lane, level = lanes_of((8, 128)), rows_of((8, 128))
    within = lane % 64
    line_re, line_im = taper_sum(taps, first_pixel + (2 * (within % 32) + within // 32).astype(jnp.float32))
    norm = 1.0 / (SUP * math.sqrt(65536))
    line_re, line_im = line_re[0:1, :] * norm, line_im[0:1, :] * norm
    column_pixel = lane + 128 * (level % 2)
    col_re, col_im = taper_sum(taps, jnp.where(level < 2, column_pixel, -1 - column_pixel).astype(jnp.float32))
    for distance in (2, 3):
        pl.semaphore_wait(rounds.at[distance - 2], neighbours)
        gather_near(distance)
        signal_near(rounds.at[distance - 1])
    for index in range(1, RING):
        if index < 4:
            source = half * 4 + (grp + index) % 4
        else:
            source = (1 - half) * 4 + (grp + 7 - index) % 4
        pltpu.make_async_remote_copy(
            src_ref=fields.at[source],
            dst_ref=fields.at[source],
            send_sem=a_send,
            recv_sem=a_recv.at[source],
            device_id=pair,
            device_id_type=MESH,
        ).wait_recv()
        project(index - 1)
        phases(fields[source], first_pixel, v_ref.at[index % 2], w_ref.at[index % 2])
        if index == 3:
            pl.semaphore_wait(rounds.at[2], neighbours)
            signal_near(rounds.at[3])

            @pl.when(half == 0)
            def _():
                pl.semaphore_wait(late_sem, 4)
                for there in range(4):
                    gather(across(there))

    project(RING - 1)
    for i in range(2):
        rows = slice(128 * i, 128 * i + 128)
        cos_sum = acc[rows, 0:128] + acc[rows, 128:256]
        rows = slice(256 + 128 * i, 256 + 128 * i + 128)
        sin_sum = acc[rows, 0:128] + acc[rows, 128:256]
        minus = cos_sum - pltpu.roll(sin_sum, 64, 1)
        plus = pltpu.roll(cos_sum, 64, 1) + sin_sum
        mask = lanes_of((128, 128)) < 64
        real, imag = jnp.where(mask, minus, plus), jnp.where(mask, plus, minus)
        real, imag = (line_re * real - line_im * imag).T, (line_re * imag + line_im * real).T
        for group in range(4):
            part = slice(32 * group, 32 * group + 32)
            tap = slice(group // 2 * 2 + i, group // 2 * 2 + i + 1)
            facet = col_re[tap, :] * real[part, :] - col_im[tap, :] * imag[part, :]
            for t in range(4):
                sends[pl.ds(64 * t + 2 * group + i, 8, stride=8), :] = facet[8 * t : 8 * t + 8, :]

    pl.semaphore_wait(rounds.at[3], neighbours)
    for i, shift in enumerate(shifts):
        start = pl.multiple_of(8 * ((core + shift[0]) % 2 * 16 + own_vert(shift)), 8)
        pltpu.make_async_remote_copy(
            src_ref=sends.at[pl.ds(start, 8), :],
            dst_ref=recvs.at[i],
            send_sem=b_send,
            recv_sem=b_recv,
            device_id=own_peer(shift),
            device_id_type=MESH,
        ).start()
    mine = pl.multiple_of(8 * (core * 16 + vert), 8)
    total = sends[pl.ds(mine, 8), :]
    batch = pltpu.make_async_remote_copy(
        src_ref=recvs, dst_ref=recvs, send_sem=b_send, recv_sem=b_recv, device_id=pair, device_id_type=MESH
    )
    batch.wait_recv()
    for i in range(len(shifts)):
        total = total + recvs[i]
    mirrored = jnp.take_along_axis(total, 127 - lane, axis=1)
    for e in range(2):
        for h in range(2):
            out_ref[e : e + 1, 256 + 128 * h : 384 + 128 * h] = total[2 * e + h : 2 * e + h + 1, :]
            out_ref[e : e + 1, 128 * (1 - h) : 128 * (2 - h)] = mirrored[4 + 2 * e + h : 5 + 2 * e + h, :]
    batch.wait_send()
    rest = fields.at[pl.ds(1, RING - 1)]
    pltpu.make_async_remote_copy(
        src_ref=rest, dst_ref=rest, send_sem=a_send, recv_sem=a_recv.at[0], device_id=pair, device_id_type=MESH
    ).wait_send()


def body(visibility, destination, tile_slot, offsets, taper):
    any_space = pl.BlockSpec(memory_space=pl.ANY)
    return pl.pallas_call(
        kernel,
        out_shape=pltpu.VMEM((2, IMG), jnp.float32),
        in_specs=[any_space] * 5,
        out_specs=pl.BlockSpec(memory_space=pltpu.VMEM),
        scratch_shapes=[
            pltpu.VMEM((2, VIS), jnp.float32),
            pltpu.VMEM((1, VIS), jnp.int32),
            pltpu.VMEM((1, VIS), jnp.int32),
            pltpu.VMEM((2, VIS), jnp.int32),
            pltpu.SMEM((SUP,), jnp.float32),
            pltpu.VMEM((RING, 4, VIS), jnp.float32),
            pltpu.VMEM((2, IMG, 2 * VIS), jnp.bfloat16),
            pltpu.VMEM((2, 4 * ROWS, VIS), jnp.bfloat16),
            pltpu.VMEM((IMG, 4 * ROWS), jnp.float32),
            pltpu.VMEM((OWN * 8, 128), jnp.float32),
            pltpu.VMEM((OWN - 1, 8, 128), jnp.float32),
            pltpu.SemaphoreType.DMA((5,)),
            pltpu.SemaphoreType.DMA,
            pltpu.SemaphoreType.DMA((RING,)),
            pltpu.SemaphoreType.DMA,
            pltpu.SemaphoreType.DMA,
            pltpu.SemaphoreType.REGULAR((4,)),
            pltpu.SemaphoreType.REGULAR,
        ],
        compiler_params=pltpu.CompilerParams(collective_id=0, has_side_effects=True),
    )(visibility.T, destination.T, tile_slot.reshape(1, -1), offsets.T, taper)


def solution(mesh):
    return jax.shard_map(
        body,
        mesh=mesh,
        in_specs=(
            P(("grp", "au", "vert"), None),
            P(("grp", "au", "vert"), None),
            P(("grp", "au", "vert")),
            P(("grp", "au", "vert"), None),
            P(),
        ),
        out_specs=P(("grp", "au", "vert"), None),
        check_vma=False,
    )
```

```python
import math

import jax
import jax.numpy as jnp
from jax import lax
from jax.experimental import pallas as pl
from jax.experimental.pallas import tpu as pltpu
from jax.sharding import PartitionSpec as P

TILE = 128
SUP = 8
ROWS_DEV = 2048
COLS_DEV = 512
IMG = 512
CELLS = 8192
MESH = pl.DeviceIdType.MESH

RING = 8
OWN = 32
ROWS = 64
HALF = IMG // 2
VIS = 256

ORDER = (
    (1, 2, 3, 7, 6, 5, 4),
    (2, 3, 0, 7, 4, 6, 5),
    (3, 1, 0, 4, 5, 7, 6),
    (4, 5, 6, 7, 2, 1, 0),
    (5, 6, 7, 3, 2, 1, 0),
    (6, 7, 4, 3, 2, 1, 0),
    (7, 5, 4, 3, 0, 2, 1),
    (6, 5, 4, 0, 3, 1, 2),
)


def sincos(turns):
    turns = turns - jnp.floor(turns + 0.5)
    square = turns * turns
    sine = jnp.full_like(turns, -(math.pi**11) / math.factorial(11))
    for order in (9, 7, 5, 3, 1):
        sign = 1.0 if order % 4 == 1 else -1.0
        sine = sine * square + sign * math.pi**order / math.factorial(order)
    sine = sine * turns
    cosine = jnp.full_like(turns, math.pi**12 / math.factorial(12))
    for order in (10, 8, 6, 4, 2, 0):
        sign = 1.0 if order % 4 == 0 else -1.0
        cosine = cosine * square + sign * math.pi**order / math.factorial(order)
    return 1.0 - 2.0 * sine * sine, 2.0 * sine * cosine


def times(a, b):
    return a[0] * b[0] - a[1] * b[1], a[0] * b[1] + a[1] * b[0]


def stack(a, b):
    return jnp.concatenate([a[0], b[0]], axis=0), jnp.concatenate([a[1], b[1]], axis=0)


def split(value):
    high = value.astype(jnp.bfloat16)
    return high, (value - high.astype(jnp.float32)).astype(jnp.bfloat16)


def taper_sum(taper, pixel):
    step = sincos(pixel * (1.0 / CELLS))
    total = (jnp.full_like(pixel, taper[SUP - 1]), jnp.zeros_like(pixel))
    for tap in range(SUP - 2, -1, -1):
        re, im = times(total, step)
        total = (re + taper[tap], im)
    return total


def rows_of(shape):
    return lax.broadcasted_iota(jnp.int32, shape, 0)


def lanes_of(shape):
    return lax.broadcasted_iota(jnp.int32, shape, 1)


def phases(fields, first_pixel, v_ref, w_ref):
    re, im, x, y = (fields[i : i + 1, :] for i in range(4))
    row = rows_of((8, VIS))
    rowf = row.astype(jnp.float32)
    unit = 1.0 / CELLS
    col = sincos((rowf + 0.5) * y * unit)
    line = sincos(((first_pixel + 2.0 * rowf) * x - 0.5 * y) * unit)
    power = jnp.where(row < 5, 8 << jnp.minimum(row, 4), jnp.where(row == 7, 1, 16 << jnp.maximum(row - 5, 0)))
    turn = sincos(power.astype(jnp.float32) * jnp.where(row < 5, y, x) * unit)

    def step(i):
        return turn[0][i : i + 1, :], turn[1][i : i + 1, :]

    line = times((re, im), line)
    tiles = [stack(line, times(line, step(5)))]
    tiles.append(times(tiles[0], step(6)))
    tiles += [times(tile, step(7)) for tile in tiles]
    for i, tile in enumerate(tiles):
        for part in range(2):
            high, low = split(tile[part])
            w_ref[64 * part + 16 * i : 64 * part + 16 * i + 16, :] = high
            w_ref[128 + 64 * part + 16 * i : 128 + 64 * part + 16 * i + 16, :] = low
    tiles = [stack(col, times(col, step(0)))]
    for level in range(1, 5):
        tiles += [times(tile, step(level)) for tile in tiles]
    for i, tile in enumerate(tiles):
        for part in range(2):
            high, low = split(tile[part])
            v_ref[256 * part + 16 * i : 256 * part + 16 * i + 16, 0:VIS] = high
            v_ref[256 * part + 16 * i : 256 * part + 16 * i + 16, VIS : 2 * VIS] = low


def kernel(
    vis_hbm, dest_hbm, slot_hbm, off_hbm, taper_hbm, out_ref,
    vis, dest, slot, off, taper, fields, v_ref, w_ref, acc, sends, recvs,
    load_sem, a_send, a_recv, b_send, b_recv, rounds,
):
    grp, au, vert = lax.axis_index("grp"), lax.axis_index("au"), lax.axis_index("vert")
    core, half = au % 2, au // 2
    z = half * 4 + grp
    y, x = vert // 4, vert % 4

    shifts = [(c, b, a) for c in range(2) for b in range(4) for a in range(4)]
    shifts.sort(key=lambda s: -(min(s[1], 4 - s[1]) + min(s[2], 4 - s[2]) + 0.5 * s[0]))
    shifts = shifts[:-1]

    def own_vert(shift):
        return ((y + shift[1]) % 4) * 4 + (x + shift[2]) % 4

    def own_peer(shift):
        return grp, half * 2 + (core + shift[0]) % 2, own_vert(shift)

    def signal(sem, peer):
        pl.semaphore_signal(sem, inc=1, device_id=peer, device_id_type=MESH)

    def ring_peer(there):
        return there % 4, there // 4 * 2 + core, vert

    def wave(place):
        return 2 - jnp.abs(place - 2)

    pair = own_peer((1, 0, 0))
    plane = []
    for step in (1, 3):
        plane.append((wave((x + step) % 4) < wave(x), own_peer((0, 0, step))))
        plane.append((wave((y + step) % 4) < wave(y), own_peer((0, step, 0))))
    plane.append((core == 0, pair))
    before = sum(first.astype(jnp.int32) for first, _ in plane)

    def signal_if(sem, wanted, peer):
        @pl.when(wanted)
        def _():
            signal(sem, peer)

    def wait_if(sem, count):
        @pl.when(count > 0)
        def _():
            pl.semaphore_wait(sem, count)

    def signal_plane(sem):
        for _, peer in plane:
            signal(sem, peer)

    def gather(there):
        pltpu.make_async_remote_copy(
            src_ref=fields.at[z],
            dst_ref=fields.at[z],
            send_sem=a_send,
            recv_sem=a_recv.at[z],
            device_id=ring_peer(there),
            device_id_type=MESH,
        ).start()

    def gather_if(wanted, there):
        @pl.when(wanted)
        def _():
            gather(there)

    barrier = pltpu.get_barrier_semaphore()
    for there in range(1, RING):
        signal_if(barrier, z < there, ring_peer(there))
    for first, peer in plane:
        signal_if(barrier, jnp.logical_not(first), peer)

    loads = [
        pltpu.make_async_copy(src, dst, load_sem.at[i])
        for i, (src, dst) in enumerate(
            ((vis_hbm, vis), (dest_hbm, dest), (slot_hbm, slot), (off_hbm, off), (taper_hbm, taper))
        )
    ]
    for load in loads:
        load.start()
    for load in loads[:4]:
        load.wait()
    target, tile = dest[...], slot[...]
    row0 = target // 16 * ROWS_DEV + tile // 4 * TILE + off[0:1, :]
    col0 = target % 16 * COLS_DEV + tile % 4 * TILE + off[1:2, :]
    fields[z, 0:2, :] = vis[...]
    fields[z, 2:3, :] = (row0 - CELLS // 2).astype(jnp.float32)
    fields[z, 3:4, :] = (col0 - CELLS // 2).astype(jnp.float32)

    wait_if(barrier, before + z)
    for there in range(RING - 1):
        gather_if(there < z, there)
    for first, peer in plane:
        signal_if(rounds.at[0], first, peer)

    position = grp * 2 + half
    first_pixel = (position * ROWS - HALF).astype(jnp.float32)

    def project(index):
        weights = w_ref[index % 2]
        part = None
        for low in range(2):
            product = lax.dot_general(
                v_ref[index % 2, :, low * VIS : (low + 1) * VIS],
                weights,
                (((1,), (1,)), ((), ())),
                preferred_element_type=jnp.float32,
            )
            part = product if part is None else part + product
        if index == 0:
            acc[...] = part
        else:
            acc[...] += part

    phases(fields[z], first_pixel, v_ref.at[0], w_ref.at[0])
    loads[4].wait()
    taps = [taper[i] for i in range(SUP)]
    lane, level = lanes_of((8, 128)), rows_of((8, 128))
    within = lane % 64
    line_re, line_im = taper_sum(taps, first_pixel + (2 * (within % 32) + within // 32).astype(jnp.float32))
    norm = 1.0 / (SUP * math.sqrt(65536))
    line_re, line_im = line_re[0:1, :] * norm, line_im[0:1, :] * norm
    column_pixel = lane + 128 * (level % 2)
    col_re, col_im = taper_sum(taps, jnp.where(level < 2, column_pixel, -1 - column_pixel).astype(jnp.float32))
    wait_if(rounds.at[0], len(plane) - before)
    signal_plane(rounds.at[1])
    for index in range(1, RING):
        source = ORDER[0][index - 1]
        for place in range(1, RING):
            source = jnp.where(z == place, ORDER[place][index - 1], source)
        pltpu.make_async_remote_copy(
            src_ref=fields.at[source],
            dst_ref=fields.at[source],
            send_sem=a_send,
            recv_sem=a_recv.at[source],
            device_id=pair,
            device_id_type=MESH,
        ).wait_recv()
        gather_if(source > z, source)
        project(index - 1)
        phases(fields[source], first_pixel, v_ref.at[index % 2], w_ref.at[index % 2])
        if index < 4:
            pl.semaphore_wait(rounds.at[index], len(plane))
            signal_plane(rounds.at[index + 1])

    project(RING - 1)
    for i in range(2):
        rows = slice(128 * i, 128 * i + 128)
        cos_sum = acc[rows, 0:128] + acc[rows, 128:256]
        rows = slice(256 + 128 * i, 256 + 128 * i + 128)
        sin_sum = acc[rows, 0:128] + acc[rows, 128:256]
        minus = cos_sum - pltpu.roll(sin_sum, 64, 1)
        plus = pltpu.roll(cos_sum, 64, 1) + sin_sum
        mask = lanes_of((128, 128)) < 64
        real, imag = jnp.where(mask, minus, plus), jnp.where(mask, plus, minus)
        real, imag = (line_re * real - line_im * imag).T, (line_re * imag + line_im * real).T
        for group in range(4):
            part = slice(32 * group, 32 * group + 32)
            tap = slice(group // 2 * 2 + i, group // 2 * 2 + i + 1)
            facet = col_re[tap, :] * real[part, :] - col_im[tap, :] * imag[part, :]
            for t in range(4):
                sends[pl.ds(64 * t + 2 * group + i, 8, stride=8), :] = facet[8 * t : 8 * t + 8, :]

    pl.semaphore_wait(rounds.at[4], len(plane))
    for i, shift in enumerate(shifts):
        start = pl.multiple_of(8 * ((core + shift[0]) % 2 * 16 + own_vert(shift)), 8)
        pltpu.make_async_remote_copy(
            src_ref=sends.at[pl.ds(start, 8), :],
            dst_ref=recvs.at[i],
            send_sem=b_send,
            recv_sem=b_recv,
            device_id=own_peer(shift),
            device_id_type=MESH,
        ).start()
    mine = pl.multiple_of(8 * (core * 16 + vert), 8)
    total = sends[pl.ds(mine, 8), :]
    batch = pltpu.make_async_remote_copy(
        src_ref=recvs, dst_ref=recvs, send_sem=b_send, recv_sem=b_recv, device_id=pair, device_id_type=MESH
    )
    batch.wait_recv()
    for i in range(len(shifts)):
        total = total + recvs[i]
    mirrored = jnp.take_along_axis(total, 127 - lane, axis=1)
    for e in range(2):
        for h in range(2):
            out_ref[e : e + 1, 256 + 128 * h : 384 + 128 * h] = total[2 * e + h : 2 * e + h + 1, :]
            out_ref[e : e + 1, 128 * (1 - h) : 128 * (2 - h)] = mirrored[4 + 2 * e + h : 5 + 2 * e + h, :]
    batch.wait_send()
    rest = fields.at[pl.ds(1, RING - 1)]
    pltpu.make_async_remote_copy(
        src_ref=rest, dst_ref=rest, send_sem=a_send, recv_sem=a_recv.at[0], device_id=pair, device_id_type=MESH
    ).wait_send()


def body(visibility, destination, tile_slot, offsets, taper):
    any_space = pl.BlockSpec(memory_space=pl.ANY)
    return pl.pallas_call(
        kernel,
        out_shape=pltpu.VMEM((2, IMG), jnp.float32),
        in_specs=[any_space] * 5,
        out_specs=pl.BlockSpec(memory_space=pltpu.VMEM),
        scratch_shapes=[
            pltpu.VMEM((2, VIS), jnp.float32),
            pltpu.VMEM((1, VIS), jnp.int32),
            pltpu.VMEM((1, VIS), jnp.int32),
            pltpu.VMEM((2, VIS), jnp.int32),
            pltpu.SMEM((SUP,), jnp.float32),
            pltpu.VMEM((RING, 4, VIS), jnp.float32),
            pltpu.VMEM((2, IMG, 2 * VIS), jnp.bfloat16),
            pltpu.VMEM((2, 4 * ROWS, VIS), jnp.bfloat16),
            pltpu.VMEM((IMG, 4 * ROWS), jnp.float32),
            pltpu.VMEM((OWN * 8, 128), jnp.float32),
            pltpu.VMEM((OWN - 1, 8, 128), jnp.float32),
            pltpu.SemaphoreType.DMA((5,)),
            pltpu.SemaphoreType.DMA,
            pltpu.SemaphoreType.DMA((RING,)),
            pltpu.SemaphoreType.DMA,
            pltpu.SemaphoreType.DMA,
            pltpu.SemaphoreType.REGULAR((5,)),
        ],
        compiler_params=pltpu.CompilerParams(collective_id=0, has_side_effects=True),
    )(visibility.T, destination.T, tile_slot.reshape(1, -1), offsets.T, taper)


def solution(mesh):
    return jax.shard_map(
        body,
        mesh=mesh,
        in_specs=(
            P(("grp", "au", "vert"), None),
            P(("grp", "au", "vert"), None),
            P(("grp", "au", "vert")),
            P(("grp", "au", "vert"), None),
            P(),
        ),
        out_specs=P(("grp", "au", "vert"), None),
        check_vma=False,
    )
```

```python
import math

import jax
import jax.numpy as jnp
from jax import lax
from jax.experimental import pallas as pl
from jax.experimental.pallas import tpu as pltpu
from jax.sharding import PartitionSpec as P

TILE = 128
SUP = 8
ROWS_DEV = 2048
COLS_DEV = 512
IMG = 512
CELLS = 8192
MESH = pl.DeviceIdType.MESH

RING = 8
OWN = 32
ROWS = 64
HALF = IMG // 2
VIS = 256

ORDER = (
    (1, 2, 3, 7, 6, 5, 4),
    (2, 3, 0, 7, 6, 4, 5),
    (3, 1, 0, 4, 5, 7, 6),
    (2, 1, 0, 4, 5, 6, 7),
    (5, 6, 7, 3, 2, 1, 0),
    (6, 7, 4, 3, 0, 2, 1),
    (7, 5, 0, 4, 3, 1, 2),
    (6, 0, 5, 1, 2, 4, 3),
)


def sincos(turns):
    turns = turns - jnp.floor(turns + 0.5)
    square = turns * turns
    sine = jnp.full_like(turns, -(math.pi**11) / math.factorial(11))
    for order in (9, 7, 5, 3, 1):
        sign = 1.0 if order % 4 == 1 else -1.0
        sine = sine * square + sign * math.pi**order / math.factorial(order)
    sine = sine * turns
    cosine = jnp.full_like(turns, math.pi**12 / math.factorial(12))
    for order in (10, 8, 6, 4, 2, 0):
        sign = 1.0 if order % 4 == 0 else -1.0
        cosine = cosine * square + sign * math.pi**order / math.factorial(order)
    return 1.0 - 2.0 * sine * sine, 2.0 * sine * cosine


def times(a, b):
    return a[0] * b[0] - a[1] * b[1], a[0] * b[1] + a[1] * b[0]


def stack(a, b):
    return jnp.concatenate([a[0], b[0]], axis=0), jnp.concatenate([a[1], b[1]], axis=0)


def split(value):
    high = value.astype(jnp.bfloat16)
    return high, (value - high.astype(jnp.float32)).astype(jnp.bfloat16)


def taper_sum(taper, pixel):
    step = sincos(pixel * (1.0 / CELLS))
    total = (jnp.full_like(pixel, taper[SUP - 1]), jnp.zeros_like(pixel))
    for tap in range(SUP - 2, -1, -1):
        re, im = times(total, step)
        total = (re + taper[tap], im)
    return total


def rows_of(shape):
    return lax.broadcasted_iota(jnp.int32, shape, 0)


def lanes_of(shape):
    return lax.broadcasted_iota(jnp.int32, shape, 1)


def phases(fields, first_pixel, v_ref, w_ref):
    re, im, x, y = (fields[i : i + 1, :] for i in range(4))
    row = rows_of((8, VIS))
    rowf = row.astype(jnp.float32)
    unit = 1.0 / CELLS
    col = sincos((rowf + 0.5) * y * unit)
    line = sincos(((first_pixel + 2.0 * rowf) * x - 0.5 * y) * unit)
    power = jnp.where(row < 5, 8 << jnp.minimum(row, 4), jnp.where(row == 7, 1, 16 << jnp.maximum(row - 5, 0)))
    turn = sincos(power.astype(jnp.float32) * jnp.where(row < 5, y, x) * unit)

    def step(i):
        return turn[0][i : i + 1, :], turn[1][i : i + 1, :]

    line = times((re, im), line)
    tiles = [stack(line, times(line, step(5)))]
    tiles.append(times(tiles[0], step(6)))
    tiles += [times(tile, step(7)) for tile in tiles]
    for i, tile in enumerate(tiles):
        for part in range(2):
            high, low = split(tile[part])
            w_ref[64 * part + 16 * i : 64 * part + 16 * i + 16, :] = high
            w_ref[128 + 64 * part + 16 * i : 128 + 64 * part + 16 * i + 16, :] = low
    tiles = [stack(col, times(col, step(0)))]
    for level in range(1, 5):
        tiles += [times(tile, step(level)) for tile in tiles]
    for i, tile in enumerate(tiles):
        for part in range(2):
            high, low = split(tile[part])
            v_ref[256 * part + 16 * i : 256 * part + 16 * i + 16, 0:VIS] = high
            v_ref[256 * part + 16 * i : 256 * part + 16 * i + 16, VIS : 2 * VIS] = low


def kernel(
    vis_hbm, dest_hbm, slot_hbm, off_hbm, taper_hbm, out_ref,
    vis, dest, slot, off, taper, fields, v_ref, w_ref, acc, sends, recvs,
    load_sem, a_send, a_recv, b_send, b_recv, rounds, ready,
):
    grp, au, vert = lax.axis_index("grp"), lax.axis_index("au"), lax.axis_index("vert")
    core, half = au % 2, au // 2
    z = half * 4 + grp
    y, x = vert // 4, vert % 4

    shifts = [(c, b, a) for c in range(2) for b in range(4) for a in range(4)]
    shifts.sort(key=lambda s: -(min(s[1], 4 - s[1]) + min(s[2], 4 - s[2]) + 0.5 * s[0]))
    shifts = shifts[:-1]

    def own_vert(shift):
        return ((y + shift[1]) % 4) * 4 + (x + shift[2]) % 4

    def own_peer(shift):
        return grp, half * 2 + (core + shift[0]) % 2, own_vert(shift)

    def signal(sem, peer):
        pl.semaphore_signal(sem, inc=1, device_id=peer, device_id_type=MESH)

    def ring_peer(there):
        return there % 4, there // 4 * 2 + core, vert

    def wave(place):
        return 2 - jnp.abs(place - 2)

    pair = own_peer((1, 0, 0))
    plane = []
    for step in (1, 3):
        plane.append((wave((x + step) % 4) < wave(x), own_peer((0, 0, step))))
        plane.append((wave((y + step) % 4) < wave(y), own_peer((0, step, 0))))
    plane.append((core == 0, pair))
    before = sum(first.astype(jnp.int32) for first, _ in plane)

    def signal_if(sem, wanted, peer):
        @pl.when(wanted)
        def _():
            signal(sem, peer)

    def wait_if(sem, count):
        @pl.when(count > 0)
        def _():
            pl.semaphore_wait(sem, count)

    def signal_plane(sem):
        for _, peer in plane:
            signal(sem, peer)

    def gather(there):
        pltpu.make_async_remote_copy(
            src_ref=fields.at[z],
            dst_ref=fields.at[z],
            send_sem=a_send,
            recv_sem=a_recv.at[z],
            device_id=ring_peer(there),
            device_id_type=MESH,
        ).start()

    def gather_if(wanted, there):
        @pl.when(wanted)
        def _():
            gather(there)

    barrier = pltpu.get_barrier_semaphore()
    for there in range(1, RING):
        signal_if(barrier, z < there, ring_peer(there))
    for first, peer in plane:
        signal_if(barrier, jnp.logical_not(first), peer)

    loads = [
        pltpu.make_async_copy(src, dst, load_sem.at[i])
        for i, (src, dst) in enumerate(
            ((vis_hbm, vis), (dest_hbm, dest), (slot_hbm, slot), (off_hbm, off), (taper_hbm, taper))
        )
    ]
    for load in loads:
        load.start()
    for load in loads[:4]:
        load.wait()
    target, tile = dest[...], slot[...]
    row0 = target // 16 * ROWS_DEV + tile // 4 * TILE + off[0:1, :]
    col0 = target % 16 * COLS_DEV + tile % 4 * TILE + off[1:2, :]
    fields[z, 0:2, :] = vis[...]
    fields[z, 2:3, :] = (row0 - CELLS // 2).astype(jnp.float32)
    fields[z, 3:4, :] = (col0 - CELLS // 2).astype(jnp.float32)

    wait_if(barrier, before + z)
    for there in range(RING - 1):
        gather_if(there < z, there)
    for there in range(RING - 1):
        signal_if(ready.at[jnp.where(there // 4 == half, 0, 1)], there < z, ring_peer(there))
    for first, peer in plane:
        signal_if(rounds.at[0], first, peer)

    position = grp * 2 + half
    first_pixel = (position * ROWS - HALF).astype(jnp.float32)

    def project(index):
        weights = w_ref[index % 2]
        part = None
        for low in range(2):
            product = lax.dot_general(
                v_ref[index % 2, :, low * VIS : (low + 1) * VIS],
                weights,
                (((1,), (1,)), ((), ())),
                preferred_element_type=jnp.float32,
            )
            part = product if part is None else part + product
        if index == 0:
            acc[...] = part
        else:
            acc[...] += part

    phases(fields[z], first_pixel, v_ref.at[0], w_ref.at[0])
    loads[4].wait()
    taps = [taper[i] for i in range(SUP)]
    lane, level = lanes_of((8, 128)), rows_of((8, 128))
    within = lane % 64
    line_re, line_im = taper_sum(taps, first_pixel + (2 * (within % 32) + within // 32).astype(jnp.float32))
    norm = 1.0 / (SUP * math.sqrt(65536))
    line_re, line_im = line_re[0:1, :] * norm, line_im[0:1, :] * norm
    column_pixel = lane + 128 * (level % 2)
    col_re, col_im = taper_sum(taps, jnp.where(level < 2, column_pixel, -1 - column_pixel).astype(jnp.float32))
    wait_if(ready.at[0], 3 - grp)
    for there in range(1, RING):
        gather_if((there > z) & (there // 4 == half), there)
    wait_if(rounds.at[0], len(plane) - before)
    signal_plane(rounds.at[1])
    for index in range(1, RING):
        if index == 4:

            @pl.when(half == 0)
            def _():
                pl.semaphore_wait(ready.at[1], 4)
                for there in range(4, RING):
                    gather(there)

        source = ORDER[0][index - 1]
        for place in range(1, RING):
            source = jnp.where(z == place, ORDER[place][index - 1], source)
        pltpu.make_async_remote_copy(
            src_ref=fields.at[source],
            dst_ref=fields.at[source],
            send_sem=a_send,
            recv_sem=a_recv.at[source],
            device_id=pair,
            device_id_type=MESH,
        ).wait_recv()
        project(index - 1)
        phases(fields[source], first_pixel, v_ref.at[index % 2], w_ref.at[index % 2])
        if index < 4:
            pl.semaphore_wait(rounds.at[index], len(plane))
            signal_plane(rounds.at[index + 1])

    project(RING - 1)
    for i in range(2):
        rows = slice(128 * i, 128 * i + 128)
        cos_sum = acc[rows, 0:128] + acc[rows, 128:256]
        rows = slice(256 + 128 * i, 256 + 128 * i + 128)
        sin_sum = acc[rows, 0:128] + acc[rows, 128:256]
        minus = cos_sum - pltpu.roll(sin_sum, 64, 1)
        plus = pltpu.roll(cos_sum, 64, 1) + sin_sum
        mask = lanes_of((128, 128)) < 64
        real, imag = jnp.where(mask, minus, plus), jnp.where(mask, plus, minus)
        real, imag = (line_re * real - line_im * imag).T, (line_re * imag + line_im * real).T
        for group in range(4):
            part = slice(32 * group, 32 * group + 32)
            tap = slice(group // 2 * 2 + i, group // 2 * 2 + i + 1)
            facet = col_re[tap, :] * real[part, :] - col_im[tap, :] * imag[part, :]
            for t in range(4):
                sends[pl.ds(64 * t + 2 * group + i, 8, stride=8), :] = facet[8 * t : 8 * t + 8, :]

    pl.semaphore_wait(rounds.at[4], len(plane))
    for i, shift in enumerate(shifts):
        start = pl.multiple_of(8 * ((core + shift[0]) % 2 * 16 + own_vert(shift)), 8)
        pltpu.make_async_remote_copy(
            src_ref=sends.at[pl.ds(start, 8), :],
            dst_ref=recvs.at[i],
            send_sem=b_send,
            recv_sem=b_recv,
            device_id=own_peer(shift),
            device_id_type=MESH,
        ).start()
    mine = pl.multiple_of(8 * (core * 16 + vert), 8)
    total = sends[pl.ds(mine, 8), :]
    batch = pltpu.make_async_remote_copy(
        src_ref=recvs, dst_ref=recvs, send_sem=b_send, recv_sem=b_recv, device_id=pair, device_id_type=MESH
    )
    batch.wait_recv()
    for i in range(len(shifts)):
        total = total + recvs[i]
    mirrored = jnp.take_along_axis(total, 127 - lane, axis=1)
    for e in range(2):
        for h in range(2):
            out_ref[e : e + 1, 256 + 128 * h : 384 + 128 * h] = total[2 * e + h : 2 * e + h + 1, :]
            out_ref[e : e + 1, 128 * (1 - h) : 128 * (2 - h)] = mirrored[4 + 2 * e + h : 5 + 2 * e + h, :]
    batch.wait_send()
    rest = fields.at[pl.ds(1, RING - 1)]
    pltpu.make_async_remote_copy(
        src_ref=rest, dst_ref=rest, send_sem=a_send, recv_sem=a_recv.at[0], device_id=pair, device_id_type=MESH
    ).wait_send()


def body(visibility, destination, tile_slot, offsets, taper):
    any_space = pl.BlockSpec(memory_space=pl.ANY)
    return pl.pallas_call(
        kernel,
        out_shape=pltpu.VMEM((2, IMG), jnp.float32),
        in_specs=[any_space] * 5,
        out_specs=pl.BlockSpec(memory_space=pltpu.VMEM),
        scratch_shapes=[
            pltpu.VMEM((2, VIS), jnp.float32),
            pltpu.VMEM((1, VIS), jnp.int32),
            pltpu.VMEM((1, VIS), jnp.int32),
            pltpu.VMEM((2, VIS), jnp.int32),
            pltpu.SMEM((SUP,), jnp.float32),
            pltpu.VMEM((RING, 4, VIS), jnp.float32),
            pltpu.VMEM((2, IMG, 2 * VIS), jnp.bfloat16),
            pltpu.VMEM((2, 4 * ROWS, VIS), jnp.bfloat16),
            pltpu.VMEM((IMG, 4 * ROWS), jnp.float32),
            pltpu.VMEM((OWN * 8, 128), jnp.float32),
            pltpu.VMEM((OWN - 1, 8, 128), jnp.float32),
            pltpu.SemaphoreType.DMA((5,)),
            pltpu.SemaphoreType.DMA,
            pltpu.SemaphoreType.DMA((RING,)),
            pltpu.SemaphoreType.DMA,
            pltpu.SemaphoreType.DMA,
            pltpu.SemaphoreType.REGULAR((5,)),
            pltpu.SemaphoreType.REGULAR((2,)),
        ],
        compiler_params=pltpu.CompilerParams(collective_id=0, has_side_effects=True),
    )(visibility.T, destination.T, tile_slot.reshape(1, -1), offsets.T, taper)


def solution(mesh):
    return jax.shard_map(
        body,
        mesh=mesh,
        in_specs=(
            P(("grp", "au", "vert"), None),
            P(("grp", "au", "vert"), None),
            P(("grp", "au", "vert")),
            P(("grp", "au", "vert"), None),
            P(),
        ),
        out_specs=P(("grp", "au", "vert"), None),
        check_vma=False,
    )
```

```python
import math

import jax
import jax.numpy as jnp
from jax import lax
from jax.experimental import pallas as pl
from jax.experimental.pallas import tpu as pltpu
from jax.sharding import PartitionSpec as P

TILE = 128
SUP = 8
ROWS_DEV = 2048
COLS_DEV = 512
IMG = 512
CELLS = 8192
MESH = pl.DeviceIdType.MESH

RING = 8
OWN = 32
ROWS = 64
HALF = IMG // 2
VIS = 256

ORDER = (
    (1, 2, 3, 7, 6, 5, 4),
    (2, 3, 0, 7, 6, 4, 5),
    (3, 1, 0, 4, 5, 7, 6),
    (2, 1, 0, 4, 5, 6, 7),
    (5, 6, 7, 3, 2, 1, 0),
    (6, 7, 4, 3, 0, 2, 1),
    (7, 5, 0, 4, 3, 1, 2),
    (6, 0, 5, 1, 2, 4, 3),
)


def sincos(turns):
    turns = turns - jnp.floor(turns + 0.5)
    square = turns * turns
    sine = jnp.full_like(turns, -(math.pi**11) / math.factorial(11))
    for order in (9, 7, 5, 3, 1):
        sign = 1.0 if order % 4 == 1 else -1.0
        sine = sine * square + sign * math.pi**order / math.factorial(order)
    sine = sine * turns
    cosine = jnp.full_like(turns, math.pi**12 / math.factorial(12))
    for order in (10, 8, 6, 4, 2, 0):
        sign = 1.0 if order % 4 == 0 else -1.0
        cosine = cosine * square + sign * math.pi**order / math.factorial(order)
    return 1.0 - 2.0 * sine * sine, 2.0 * sine * cosine


def times(a, b):
    return a[0] * b[0] - a[1] * b[1], a[0] * b[1] + a[1] * b[0]


def stack(a, b):
    return jnp.concatenate([a[0], b[0]], axis=0), jnp.concatenate([a[1], b[1]], axis=0)


def split(value):
    high = value.astype(jnp.bfloat16)
    return high, (value - high.astype(jnp.float32)).astype(jnp.bfloat16)


def taper_sum(taper, pixel):
    step = sincos(pixel * (1.0 / CELLS))
    total = (jnp.full_like(pixel, taper[SUP - 1]), jnp.zeros_like(pixel))
    for tap in range(SUP - 2, -1, -1):
        re, im = times(total, step)
        total = (re + taper[tap], im)
    return total


def rows_of(shape):
    return lax.broadcasted_iota(jnp.int32, shape, 0)


def lanes_of(shape):
    return lax.broadcasted_iota(jnp.int32, shape, 1)


def phases(fields, first_pixel, v_ref, w_ref):
    re, im, x, y = (fields[i : i + 1, :] for i in range(4))
    row = rows_of((8, VIS))
    rowf = row.astype(jnp.float32)
    unit = 1.0 / CELLS
    col = sincos((rowf + 0.5) * y * unit)
    line = sincos(((first_pixel + 2.0 * rowf) * x - 0.5 * y) * unit)
    power = jnp.where(row < 5, 8 << jnp.minimum(row, 4), jnp.where(row == 7, 1, 16 << jnp.maximum(row - 5, 0)))
    turn = sincos(power.astype(jnp.float32) * jnp.where(row < 5, y, x) * unit)

    def step(i):
        return turn[0][i : i + 1, :], turn[1][i : i + 1, :]

    line = times((re, im), line)
    tiles = [stack(line, times(line, step(5)))]
    tiles.append(times(tiles[0], step(6)))
    tiles += [times(tile, step(7)) for tile in tiles]
    for i, tile in enumerate(tiles):
        for part in range(2):
            high, low = split(tile[part])
            w_ref[64 * part + 16 * i : 64 * part + 16 * i + 16, :] = high
            w_ref[128 + 64 * part + 16 * i : 128 + 64 * part + 16 * i + 16, :] = low
    tiles = [stack(col, times(col, step(0)))]
    for level in range(1, 5):
        tiles += [times(tile, step(level)) for tile in tiles]
    for i, tile in enumerate(tiles):
        for part in range(2):
            high, low = split(tile[part])
            v_ref[256 * part + 16 * i : 256 * part + 16 * i + 16, 0:VIS] = high
            v_ref[256 * part + 16 * i : 256 * part + 16 * i + 16, VIS : 2 * VIS] = low


def kernel(
    vis_hbm, dest_hbm, slot_hbm, off_hbm, taper_hbm, out_ref,
    vis, dest, slot, off, taper, fields, v_ref, w_ref, acc, sends, recvs,
    load_sem, a_send, a_recv, b_send, b_recv, rounds, ready,
):
    grp, au, vert = lax.axis_index("grp"), lax.axis_index("au"), lax.axis_index("vert")
    core, half = au % 2, au // 2
    z = half * 4 + grp
    y, x = vert // 4, vert % 4

    shifts = [(c, b, a) for c in range(2) for b in range(4) for a in range(4)]
    shifts.sort(key=lambda s: -(min(s[1], 4 - s[1]) + min(s[2], 4 - s[2]) + 0.5 * s[0]))
    shifts = shifts[:-1]

    def own_vert(shift):
        return ((y + shift[1]) % 4) * 4 + (x + shift[2]) % 4

    def own_peer(shift):
        return grp, half * 2 + (core + shift[0]) % 2, own_vert(shift)

    def signal(sem, peer):
        pl.semaphore_signal(sem, inc=1, device_id=peer, device_id_type=MESH)

    def ring_peer(there):
        return there % 4, there // 4 * 2 + core, vert

    def wave(place):
        return 2 - jnp.abs(place - 2)

    pair = own_peer((1, 0, 0))
    plane = []
    for step in (1, 3):
        plane.append((wave((x + step) % 4) < wave(x), own_peer((0, 0, step))))
        plane.append((wave((y + step) % 4) < wave(y), own_peer((0, step, 0))))
    plane.append((core == 0, pair))
    before = sum(first.astype(jnp.int32) for first, _ in plane)

    def signal_if(sem, wanted, peer):
        @pl.when(wanted)
        def _():
            signal(sem, peer)

    def wait_if(sem, count):
        @pl.when(count > 0)
        def _():
            pl.semaphore_wait(sem, count)

    def signal_plane(sem):
        for _, peer in plane:
            signal(sem, peer)

    def gather(there):
        pltpu.make_async_remote_copy(
            src_ref=fields.at[z],
            dst_ref=fields.at[z],
            send_sem=a_send,
            recv_sem=a_recv.at[z],
            device_id=ring_peer(there),
            device_id_type=MESH,
        ).start()

    def gather_if(wanted, there):
        @pl.when(wanted)
        def _():
            gather(there)

    barrier = pltpu.get_barrier_semaphore()
    for there in range(1, RING):
        signal_if(barrier, z < there, ring_peer(there))
    for first, peer in plane:
        signal_if(barrier, jnp.logical_not(first), peer)

    loads = [
        pltpu.make_async_copy(src, dst, load_sem.at[i])
        for i, (src, dst) in enumerate(
            ((vis_hbm, vis), (dest_hbm, dest), (slot_hbm, slot), (off_hbm, off), (taper_hbm, taper))
        )
    ]
    for load in loads:
        load.start()
    for load in loads[:4]:
        load.wait()
    target, tile = dest[...], slot[...]
    row0 = target // 16 * ROWS_DEV + tile // 4 * TILE + off[0:1, :]
    col0 = target % 16 * COLS_DEV + tile % 4 * TILE + off[1:2, :]
    fields[z, 0:2, :] = vis[...]
    fields[z, 2:3, :] = (row0 - CELLS // 2).astype(jnp.float32)
    fields[z, 3:4, :] = (col0 - CELLS // 2).astype(jnp.float32)

    wait_if(barrier, before + z)
    for there in range(RING - 1):
        gather_if(there < z, there)
    for there in range(RING - 1):
        signal_if(ready.at[jnp.where(there // 4 == half, 0, 1)], there < z, ring_peer(there))
    for first, peer in plane:
        signal_if(rounds.at[0], first, peer)

    position = grp * 2 + half
    first_pixel = (position * ROWS - HALF).astype(jnp.float32)

    def project(index):
        weights = w_ref[index % 2]
        part = None
        for low in range(2):
            product = lax.dot_general(
                v_ref[index % 2, :, low * VIS : (low + 1) * VIS],
                weights,
                (((1,), (1,)), ((), ())),
                preferred_element_type=jnp.float32,
            )
            part = product if part is None else part + product
        if index == 0:
            acc[...] = part
        else:
            acc[...] += part

    phases(fields[z], first_pixel, v_ref.at[0], w_ref.at[0])
    loads[4].wait()
    taps = [taper[i] for i in range(SUP)]
    lane, level = lanes_of((8, 128)), rows_of((8, 128))
    within = lane % 64
    line_re, line_im = taper_sum(taps, first_pixel + (2 * (within % 32) + within // 32).astype(jnp.float32))
    norm = 1.0 / (SUP * math.sqrt(65536))
    line_re, line_im = line_re[0:1, :] * norm, line_im[0:1, :] * norm
    column_pixel = lane + 128 * (level % 2)
    col_re, col_im = taper_sum(taps, jnp.where(level < 2, column_pixel, -1 - column_pixel).astype(jnp.float32))
    def plane_round(number):
        pl.semaphore_wait(rounds.at[number], len(plane))
        signal_plane(rounds.at[number + 1])

    wait_if(rounds.at[0], len(plane) - before)
    signal_plane(rounds.at[1])

    @pl.when(half == 0)
    def _():
        for number in range(1, 4):
            plane_round(number)

    wait_if(ready.at[0], 3 - grp)
    for there in range(1, RING):
        gather_if((there > z) & (there // 4 == half), there)
    for index in range(1, RING):
        if index == 3:

            @pl.when(half == 0)
            def _():
                pl.semaphore_wait(ready.at[1], 4)
                for there in range(4, RING):
                    gather(there)

        source = ORDER[0][index - 1]
        for place in range(1, RING):
            source = jnp.where(z == place, ORDER[place][index - 1], source)
        pltpu.make_async_remote_copy(
            src_ref=fields.at[source],
            dst_ref=fields.at[source],
            send_sem=a_send,
            recv_sem=a_recv.at[source],
            device_id=pair,
            device_id_type=MESH,
        ).wait_recv()
        project(index - 1)
        phases(fields[source], first_pixel, v_ref.at[index % 2], w_ref.at[index % 2])
        if index < 4:

            @pl.when(half == 1)
            def _():
                plane_round(index)

    project(RING - 1)
    for i in range(2):
        rows = slice(128 * i, 128 * i + 128)
        cos_sum = acc[rows, 0:128] + acc[rows, 128:256]
        rows = slice(256 + 128 * i, 256 + 128 * i + 128)
        sin_sum = acc[rows, 0:128] + acc[rows, 128:256]
        minus = cos_sum - pltpu.roll(sin_sum, 64, 1)
        plus = pltpu.roll(cos_sum, 64, 1) + sin_sum
        mask = lanes_of((128, 128)) < 64
        real, imag = jnp.where(mask, minus, plus), jnp.where(mask, plus, minus)
        real, imag = (line_re * real - line_im * imag).T, (line_re * imag + line_im * real).T
        for group in range(4):
            part = slice(32 * group, 32 * group + 32)
            tap = slice(group // 2 * 2 + i, group // 2 * 2 + i + 1)
            facet = col_re[tap, :] * real[part, :] - col_im[tap, :] * imag[part, :]
            for t in range(4):
                sends[pl.ds(64 * t + 2 * group + i, 8, stride=8), :] = facet[8 * t : 8 * t + 8, :]

    pl.semaphore_wait(rounds.at[4], len(plane))
    for i, shift in enumerate(shifts):
        start = pl.multiple_of(8 * ((core + shift[0]) % 2 * 16 + own_vert(shift)), 8)
        pltpu.make_async_remote_copy(
            src_ref=sends.at[pl.ds(start, 8), :],
            dst_ref=recvs.at[i],
            send_sem=b_send,
            recv_sem=b_recv,
            device_id=own_peer(shift),
            device_id_type=MESH,
        ).start()
    mine = pl.multiple_of(8 * (core * 16 + vert), 8)
    total = sends[pl.ds(mine, 8), :]
    batch = pltpu.make_async_remote_copy(
        src_ref=recvs, dst_ref=recvs, send_sem=b_send, recv_sem=b_recv, device_id=pair, device_id_type=MESH
    )
    batch.wait_recv()
    for i in range(len(shifts)):
        total = total + recvs[i]
    mirrored = jnp.take_along_axis(total, 127 - lane, axis=1)
    for e in range(2):
        for h in range(2):
            out_ref[e : e + 1, 256 + 128 * h : 384 + 128 * h] = total[2 * e + h : 2 * e + h + 1, :]
            out_ref[e : e + 1, 128 * (1 - h) : 128 * (2 - h)] = mirrored[4 + 2 * e + h : 5 + 2 * e + h, :]
    batch.wait_send()
    rest = fields.at[pl.ds(1, RING - 1)]
    pltpu.make_async_remote_copy(
        src_ref=rest, dst_ref=rest, send_sem=a_send, recv_sem=a_recv.at[0], device_id=pair, device_id_type=MESH
    ).wait_send()


def body(visibility, destination, tile_slot, offsets, taper):
    any_space = pl.BlockSpec(memory_space=pl.ANY)
    return pl.pallas_call(
        kernel,
        out_shape=pltpu.VMEM((2, IMG), jnp.float32),
        in_specs=[any_space] * 5,
        out_specs=pl.BlockSpec(memory_space=pltpu.VMEM),
        scratch_shapes=[
            pltpu.VMEM((2, VIS), jnp.float32),
            pltpu.VMEM((1, VIS), jnp.int32),
            pltpu.VMEM((1, VIS), jnp.int32),
            pltpu.VMEM((2, VIS), jnp.int32),
            pltpu.SMEM((SUP,), jnp.float32),
            pltpu.VMEM((RING, 4, VIS), jnp.float32),
            pltpu.VMEM((2, IMG, 2 * VIS), jnp.bfloat16),
            pltpu.VMEM((2, 4 * ROWS, VIS), jnp.bfloat16),
            pltpu.VMEM((IMG, 4 * ROWS), jnp.float32),
            pltpu.VMEM((OWN * 8, 128), jnp.float32),
            pltpu.VMEM((OWN - 1, 8, 128), jnp.float32),
            pltpu.SemaphoreType.DMA((5,)),
            pltpu.SemaphoreType.DMA,
            pltpu.SemaphoreType.DMA((RING,)),
            pltpu.SemaphoreType.DMA,
            pltpu.SemaphoreType.DMA,
            pltpu.SemaphoreType.REGULAR((5,)),
            pltpu.SemaphoreType.REGULAR((2,)),
        ],
        compiler_params=pltpu.CompilerParams(collective_id=0, has_side_effects=True),
    )(visibility.T, destination.T, tile_slot.reshape(1, -1), offsets.T, taper)


def solution(mesh):
    return jax.shard_map(
        body,
        mesh=mesh,
        in_specs=(
            P(("grp", "au", "vert"), None),
            P(("grp", "au", "vert"), None),
            P(("grp", "au", "vert")),
            P(("grp", "au", "vert"), None),
            P(),
        ),
        out_specs=P(("grp", "au", "vert"), None),
        check_vma=False,
    )
```

```python
import math

import jax
import jax.numpy as jnp
from jax import lax
from jax.experimental import pallas as pl
from jax.experimental.pallas import tpu as pltpu
from jax.sharding import PartitionSpec as P

TILE = 128
SUP = 8
ROWS_DEV = 2048
COLS_DEV = 512
IMG = 512
CELLS = 8192
MESH = pl.DeviceIdType.MESH

RING = 8
OWN = 32
ROWS = 64
HALF = IMG // 2
VIS = 256

ORDER = (
    (1, 2, 3, 7, 6, 5, 4),
    (2, 3, 0, 7, 6, 4, 5),
    (3, 1, 0, 4, 5, 7, 6),
    (2, 1, 0, 4, 5, 6, 7),
    (5, 6, 7, 3, 2, 1, 0),
    (6, 7, 4, 3, 0, 2, 1),
    (7, 5, 0, 4, 3, 1, 2),
    (6, 0, 5, 1, 2, 4, 3),
)


def sincos(turns):
    turns = turns - jnp.floor(turns + 0.5)
    square = turns * turns
    sine = jnp.full_like(turns, -(math.pi**11) / math.factorial(11))
    for order in (9, 7, 5, 3, 1):
        sign = 1.0 if order % 4 == 1 else -1.0
        sine = sine * square + sign * math.pi**order / math.factorial(order)
    sine = sine * turns
    cosine = jnp.full_like(turns, math.pi**12 / math.factorial(12))
    for order in (10, 8, 6, 4, 2, 0):
        sign = 1.0 if order % 4 == 0 else -1.0
        cosine = cosine * square + sign * math.pi**order / math.factorial(order)
    return 1.0 - 2.0 * sine * sine, 2.0 * sine * cosine


def times(a, b):
    return a[0] * b[0] - a[1] * b[1], a[0] * b[1] + a[1] * b[0]


def stack(a, b):
    return jnp.concatenate([a[0], b[0]], axis=0), jnp.concatenate([a[1], b[1]], axis=0)


def split(value):
    high = value.astype(jnp.bfloat16)
    return high, (value - high.astype(jnp.float32)).astype(jnp.bfloat16)


def taper_sum(taper, pixel):
    step = sincos(pixel * (1.0 / CELLS))
    total = (jnp.full_like(pixel, taper[SUP - 1]), jnp.zeros_like(pixel))
    for tap in range(SUP - 2, -1, -1):
        re, im = times(total, step)
        total = (re + taper[tap], im)
    return total


def rows_of(shape):
    return lax.broadcasted_iota(jnp.int32, shape, 0)


def lanes_of(shape):
    return lax.broadcasted_iota(jnp.int32, shape, 1)


def phases(fields, first_pixel, v_ref, w_ref):
    re, im, x, y = (fields[i : i + 1, :] for i in range(4))
    row = rows_of((8, VIS))
    rowf = row.astype(jnp.float32)
    unit = 1.0 / CELLS
    col = sincos((rowf + 0.5) * y * unit)
    line = sincos(((first_pixel + 2.0 * rowf) * x - 0.5 * y) * unit)
    power = jnp.where(row < 5, 8 << jnp.minimum(row, 4), jnp.where(row == 7, 1, 16 << jnp.maximum(row - 5, 0)))
    turn = sincos(power.astype(jnp.float32) * jnp.where(row < 5, y, x) * unit)

    def step(i):
        return turn[0][i : i + 1, :], turn[1][i : i + 1, :]

    line = times((re, im), line)
    tiles = [stack(line, times(line, step(5)))]
    tiles.append(times(tiles[0], step(6)))
    tiles += [times(tile, step(7)) for tile in tiles]
    for i, tile in enumerate(tiles):
        for part in range(2):
            high, low = split(tile[part])
            w_ref[64 * part + 16 * i : 64 * part + 16 * i + 16, :] = high
            w_ref[128 + 64 * part + 16 * i : 128 + 64 * part + 16 * i + 16, :] = low
    tiles = [stack(col, times(col, step(0)))]
    for level in range(1, 5):
        tiles += [times(tile, step(level)) for tile in tiles]
    for i, tile in enumerate(tiles):
        for part in range(2):
            high, low = split(tile[part])
            v_ref[256 * part + 16 * i : 256 * part + 16 * i + 16, 0:VIS] = high
            v_ref[256 * part + 16 * i : 256 * part + 16 * i + 16, VIS : 2 * VIS] = low


def kernel(
    vis_hbm, dest_hbm, slot_hbm, off_hbm, taper_hbm, out_ref,
    vis, dest, slot, off, taper, fields, v_ref, w_ref, acc, sends, recvs,
    load_sem, a_send, a_recv, b_send, b_recv, ready, here, everyone,
):
    grp, au, vert = lax.axis_index("grp"), lax.axis_index("au"), lax.axis_index("vert")
    core, half = au % 2, au // 2
    z = half * 4 + grp
    y, x = vert // 4, vert % 4

    shifts = [(c, b, a) for c in range(2) for b in range(4) for a in range(4)]
    shifts.sort(key=lambda s: -(min(s[1], 4 - s[1]) + min(s[2], 4 - s[2]) + 0.5 * s[0]))
    shifts = shifts[:-1]

    def own_vert(shift):
        return ((y + shift[1]) % 4) * 4 + (x + shift[2]) % 4

    def own_peer(shift):
        return grp, half * 2 + (core + shift[0]) % 2, own_vert(shift)

    def signal(sem, peer):
        pl.semaphore_signal(sem, inc=1, device_id=peer, device_id_type=MESH)

    def ring_peer(there):
        return there % 4, there // 4 * 2 + core, vert

    pair = own_peer((1, 0, 0))
    hub = grp, half * 2 + 1, 0
    is_hub = (core == 1) & (vert == 0)

    def greet_plane(sem):
        for shift in shifts:
            signal(sem, own_peer(shift))

    def signal_if(sem, wanted, peer):
        @pl.when(wanted)
        def _():
            signal(sem, peer)

    def wait_if(sem, count):
        @pl.when(count > 0)
        def _():
            pl.semaphore_wait(sem, count)

    def gather(there):
        pltpu.make_async_remote_copy(
            src_ref=fields.at[z],
            dst_ref=fields.at[z],
            send_sem=a_send,
            recv_sem=a_recv.at[z],
            device_id=ring_peer(there),
            device_id_type=MESH,
        ).start()

    def gather_if(wanted, there):
        @pl.when(wanted)
        def _():
            gather(there)

    barrier = pltpu.get_barrier_semaphore()
    for there in range(1, RING):
        signal_if(barrier, z < there, ring_peer(there))
    pl.when(is_hub)(lambda: greet_plane(barrier))

    loads = [
        pltpu.make_async_copy(src, dst, load_sem.at[i])
        for i, (src, dst) in enumerate(
            ((vis_hbm, vis), (dest_hbm, dest), (slot_hbm, slot), (off_hbm, off), (taper_hbm, taper))
        )
    ]
    for load in loads:
        load.start()
    for load in loads[:4]:
        load.wait()
    target, tile = dest[...], slot[...]
    row0 = target // 16 * ROWS_DEV + tile // 4 * TILE + off[0:1, :]
    col0 = target % 16 * COLS_DEV + tile % 4 * TILE + off[1:2, :]
    fields[z, 0:2, :] = vis[...]
    fields[z, 2:3, :] = (row0 - CELLS // 2).astype(jnp.float32)
    fields[z, 3:4, :] = (col0 - CELLS // 2).astype(jnp.float32)

    wait_if(barrier, z + jnp.where(is_hub, 0, 1))
    for there in range(RING - 1):
        gather_if(there < z, there)
    for there in range(RING - 1):
        signal_if(ready.at[jnp.where(there // 4 == half, 0, 1)], there < z, ring_peer(there))
    signal_if(here, jnp.logical_not(is_hub), hub)

    position = grp * 2 + half
    first_pixel = (position * ROWS - HALF).astype(jnp.float32)

    def project(index):
        weights = w_ref[index % 2]
        part = None
        for low in range(2):
            product = lax.dot_general(
                v_ref[index % 2, :, low * VIS : (low + 1) * VIS],
                weights,
                (((1,), (1,)), ((), ())),
                preferred_element_type=jnp.float32,
            )
            part = product if part is None else part + product
        if index == 0:
            acc[...] = part
        else:
            acc[...] += part

    phases(fields[z], first_pixel, v_ref.at[0], w_ref.at[0])
    loads[4].wait()
    taps = [taper[i] for i in range(SUP)]
    lane, level = lanes_of((8, 128)), rows_of((8, 128))
    within = lane % 64
    line_re, line_im = taper_sum(taps, first_pixel + (2 * (within % 32) + within // 32).astype(jnp.float32))
    norm = 1.0 / (SUP * math.sqrt(65536))
    line_re, line_im = line_re[0:1, :] * norm, line_im[0:1, :] * norm
    column_pixel = lane + 128 * (level % 2)
    col_re, col_im = taper_sum(taps, jnp.where(level < 2, column_pixel, -1 - column_pixel).astype(jnp.float32))
    wait_if(ready.at[0], 3 - grp)
    for there in range(1, RING):
        gather_if((there > z) & (there // 4 == half), there)
    @pl.when(is_hub)
    def _():
        pl.semaphore_wait(here, OWN - 1)
        greet_plane(everyone)

    for index in range(1, RING):
        if index == 3:

            @pl.when(half == 0)
            def _():
                pl.semaphore_wait(ready.at[1], 4)
                for there in range(4, RING):
                    gather(there)

        source = ORDER[0][index - 1]
        for place in range(1, RING):
            source = jnp.where(z == place, ORDER[place][index - 1], source)
        pltpu.make_async_remote_copy(
            src_ref=fields.at[source],
            dst_ref=fields.at[source],
            send_sem=a_send,
            recv_sem=a_recv.at[source],
            device_id=pair,
            device_id_type=MESH,
        ).wait_recv()
        project(index - 1)
        phases(fields[source], first_pixel, v_ref.at[index % 2], w_ref.at[index % 2])
    project(RING - 1)
    for i in range(2):
        rows = slice(128 * i, 128 * i + 128)
        cos_sum = acc[rows, 0:128] + acc[rows, 128:256]
        rows = slice(256 + 128 * i, 256 + 128 * i + 128)
        sin_sum = acc[rows, 0:128] + acc[rows, 128:256]
        minus = cos_sum - pltpu.roll(sin_sum, 64, 1)
        plus = pltpu.roll(cos_sum, 64, 1) + sin_sum
        mask = lanes_of((128, 128)) < 64
        real, imag = jnp.where(mask, minus, plus), jnp.where(mask, plus, minus)
        real, imag = (line_re * real - line_im * imag).T, (line_re * imag + line_im * real).T
        for group in range(4):
            part = slice(32 * group, 32 * group + 32)
            tap = slice(group // 2 * 2 + i, group // 2 * 2 + i + 1)
            facet = col_re[tap, :] * real[part, :] - col_im[tap, :] * imag[part, :]
            for t in range(4):
                sends[pl.ds(64 * t + 2 * group + i, 8, stride=8), :] = facet[8 * t : 8 * t + 8, :]

    wait_if(everyone, jnp.where(is_hub, 0, 1))
    for i, shift in enumerate(shifts):
        start = pl.multiple_of(8 * ((core + shift[0]) % 2 * 16 + own_vert(shift)), 8)
        pltpu.make_async_remote_copy(
            src_ref=sends.at[pl.ds(start, 8), :],
            dst_ref=recvs.at[i],
            send_sem=b_send,
            recv_sem=b_recv,
            device_id=own_peer(shift),
            device_id_type=MESH,
        ).start()
    mine = pl.multiple_of(8 * (core * 16 + vert), 8)
    total = sends[pl.ds(mine, 8), :]
    batch = pltpu.make_async_remote_copy(
        src_ref=recvs, dst_ref=recvs, send_sem=b_send, recv_sem=b_recv, device_id=pair, device_id_type=MESH
    )
    batch.wait_recv()
    for i in range(len(shifts)):
        total = total + recvs[i]
    mirrored = jnp.take_along_axis(total, 127 - lane, axis=1)
    for e in range(2):
        for h in range(2):
            out_ref[e : e + 1, 256 + 128 * h : 384 + 128 * h] = total[2 * e + h : 2 * e + h + 1, :]
            out_ref[e : e + 1, 128 * (1 - h) : 128 * (2 - h)] = mirrored[4 + 2 * e + h : 5 + 2 * e + h, :]
    batch.wait_send()
    rest = fields.at[pl.ds(1, RING - 1)]
    pltpu.make_async_remote_copy(
        src_ref=rest, dst_ref=rest, send_sem=a_send, recv_sem=a_recv.at[0], device_id=pair, device_id_type=MESH
    ).wait_send()


def body(visibility, destination, tile_slot, offsets, taper):
    any_space = pl.BlockSpec(memory_space=pl.ANY)
    return pl.pallas_call(
        kernel,
        out_shape=pltpu.VMEM((2, IMG), jnp.float32),
        in_specs=[any_space] * 5,
        out_specs=pl.BlockSpec(memory_space=pltpu.VMEM),
        scratch_shapes=[
            pltpu.VMEM((2, VIS), jnp.float32),
            pltpu.VMEM((1, VIS), jnp.int32),
            pltpu.VMEM((1, VIS), jnp.int32),
            pltpu.VMEM((2, VIS), jnp.int32),
            pltpu.SMEM((SUP,), jnp.float32),
            pltpu.VMEM((RING, 4, VIS), jnp.float32),
            pltpu.VMEM((2, IMG, 2 * VIS), jnp.bfloat16),
            pltpu.VMEM((2, 4 * ROWS, VIS), jnp.bfloat16),
            pltpu.VMEM((IMG, 4 * ROWS), jnp.float32),
            pltpu.VMEM((OWN * 8, 128), jnp.float32),
            pltpu.VMEM((OWN - 1, 8, 128), jnp.float32),
            pltpu.SemaphoreType.DMA((5,)),
            pltpu.SemaphoreType.DMA,
            pltpu.SemaphoreType.DMA((RING,)),
            pltpu.SemaphoreType.DMA,
            pltpu.SemaphoreType.DMA,
            pltpu.SemaphoreType.REGULAR((2,)),
            pltpu.SemaphoreType.REGULAR,
            pltpu.SemaphoreType.REGULAR,
        ],
        compiler_params=pltpu.CompilerParams(collective_id=0, has_side_effects=True),
    )(visibility.T, destination.T, tile_slot.reshape(1, -1), offsets.T, taper)


def solution(mesh):
    return jax.shard_map(
        body,
        mesh=mesh,
        in_specs=(
            P(("grp", "au", "vert"), None),
            P(("grp", "au", "vert"), None),
            P(("grp", "au", "vert")),
            P(("grp", "au", "vert"), None),
            P(),
        ),
        out_specs=P(("grp", "au", "vert"), None),
        check_vma=False,
    )
```

```python
import math

import jax
import jax.numpy as jnp
from jax import lax
from jax.experimental import pallas as pl
from jax.experimental.pallas import tpu as pltpu
from jax.sharding import PartitionSpec as P

TILE = 128
SUP = 8
ROWS_DEV = 2048
COLS_DEV = 512
IMG = 512
CELLS = 8192
MESH = pl.DeviceIdType.MESH

RING = 8
OWN = 32
ROWS = 64
HALF = IMG // 2
CENTRE = IMG // 4
VIS = 256

ORDER = (
    (1, 2, 3, 7, 6, 5, 4),
    (2, 3, 0, 7, 6, 4, 5),
    (3, 1, 0, 4, 5, 7, 6),
    (2, 1, 0, 4, 5, 6, 7),
    (5, 6, 7, 3, 2, 1, 0),
    (6, 7, 4, 3, 0, 2, 1),
    (7, 5, 0, 4, 3, 1, 2),
    (6, 0, 5, 1, 2, 4, 3),
)


def sincos(turns):
    turns = turns - jnp.floor(turns + 0.5)
    square = turns * turns
    sine = jnp.full_like(turns, -(math.pi**11) / math.factorial(11))
    for order in (9, 7, 5, 3, 1):
        sign = 1.0 if order % 4 == 1 else -1.0
        sine = sine * square + sign * math.pi**order / math.factorial(order)
    sine = sine * turns
    cosine = jnp.full_like(turns, math.pi**12 / math.factorial(12))
    for order in (10, 8, 6, 4, 2, 0):
        sign = 1.0 if order % 4 == 0 else -1.0
        cosine = cosine * square + sign * math.pi**order / math.factorial(order)
    return 1.0 - 2.0 * sine * sine, 2.0 * sine * cosine


def times(a, b):
    return a[0] * b[0] - a[1] * b[1], a[0] * b[1] + a[1] * b[0]


def stack(a, b):
    return jnp.concatenate([a[0], b[0]], axis=0), jnp.concatenate([a[1], b[1]], axis=0)


def split(value):
    high = value.astype(jnp.bfloat16)
    return high, (value - high.astype(jnp.float32)).astype(jnp.bfloat16)


def taper_sum(taper, pixel):
    step = sincos(pixel * (1.0 / CELLS))
    total = (jnp.full_like(pixel, taper[SUP - 1]), jnp.zeros_like(pixel))
    for tap in range(SUP - 2, -1, -1):
        re, im = times(total, step)
        total = (re + taper[tap], im)
    return total


def rows_of(shape):
    return lax.broadcasted_iota(jnp.int32, shape, 0)


def lanes_of(shape):
    return lax.broadcasted_iota(jnp.int32, shape, 1)


def phases(fields, first_pixel, v_ref, w_ref):
    unit = 1.0 / CELLS
    row = rows_of((8, 128))
    rowf = row.astype(jnp.float32)
    power = jnp.where(row < 2, 8 << jnp.minimum(row, 1), jnp.where(row == 2, CENTRE, 16 << jnp.maximum(row - 3, 0)))
    power = jnp.where(row == 5, 1, power).astype(jnp.float32) * unit
    for lane in range(0, VIS, 128):
        re, im, x, y = (fields[i : i + 1, lane : lane + 128] for i in range(4))
        col = sincos((rowf + 0.5) * (y * unit))
        line = sincos(((first_pixel + 2.0 * rowf) * x - 0.5 * y) * unit)
        turn = sincos(power * jnp.where(row < 3, y, x))
        steps = [(turn[0][i : i + 1, :], turn[1][i : i + 1, :]) for i in range(6)]

        def store(ref, place, value):
            high, low = split(value)
            ref[0, place : place + 16, lane : lane + 128] = high
            ref[1, place : place + 16, lane : lane + 128] = low

        line = times((re, im), line)
        tiles = [stack(line, times(line, steps[3]))]
        tiles.append(times(tiles[0], steps[4]))
        tiles += [times(tile, steps[5]) for tile in tiles]
        for i, tile in enumerate(tiles):
            rr, ii, ri, ir = (tile[a] * steps[2][b] for a, b in ((0, 0), (1, 1), (0, 1), (1, 0)))
            for place, value in ((0, rr + ii), (64, ir - ri), (128, rr - ii), (192, ri + ir)):
                store(w_ref, place + 16 * i, value)
        tile = stack(col, times(col, steps[0]))
        for i in range(CENTRE // 16):
            store(v_ref, 16 * i, tile[0])
            store(v_ref, CENTRE + 16 * i, tile[1])
            tile = times(tile, steps[1])


def kernel(
    vis_hbm, dest_hbm, slot_hbm, off_hbm, taper_hbm, out_ref,
    vis, dest, slot, off, taper, fields, v_ref, w_ref, acc, sends, recvs,
    load_sem, a_send, a_recv, b_send, b_recv, ready, here, everyone,
):
    grp, au, vert = lax.axis_index("grp"), lax.axis_index("au"), lax.axis_index("vert")
    core, half = au % 2, au // 2
    z = half * 4 + grp
    y, x = vert // 4, vert % 4

    shifts = [(c, b, a) for c in range(2) for b in range(4) for a in range(4)]
    shifts.sort(key=lambda s: -(min(s[1], 4 - s[1]) + min(s[2], 4 - s[2]) + 0.5 * s[0]))
    shifts = shifts[:-1]

    def own_vert(shift):
        return ((y + shift[1]) % 4) * 4 + (x + shift[2]) % 4

    def own_peer(shift):
        return grp, half * 2 + (core + shift[0]) % 2, own_vert(shift)

    def signal(sem, peer):
        pl.semaphore_signal(sem, inc=1, device_id=peer, device_id_type=MESH)

    def ring_peer(there):
        return there % 4, there // 4 * 2 + core, vert

    pair = own_peer((1, 0, 0))
    hub = grp, half * 2 + 1, 0
    is_hub = (core == 1) & (vert == 0)

    def greet_plane(sem):
        for shift in shifts:
            signal(sem, own_peer(shift))

    def signal_if(sem, wanted, peer):
        @pl.when(wanted)
        def _():
            signal(sem, peer)

    def wait_if(sem, count):
        @pl.when(count > 0)
        def _():
            pl.semaphore_wait(sem, count)

    def gather(there):
        pltpu.make_async_remote_copy(
            src_ref=fields.at[z],
            dst_ref=fields.at[z],
            send_sem=a_send,
            recv_sem=a_recv.at[z],
            device_id=ring_peer(there),
            device_id_type=MESH,
        ).start()

    def gather_if(wanted, there):
        @pl.when(wanted)
        def _():
            gather(there)

    barrier = pltpu.get_barrier_semaphore()
    for there in range(1, RING):
        signal_if(barrier, z < there, ring_peer(there))
    pl.when(is_hub)(lambda: greet_plane(barrier))

    loads = [
        pltpu.make_async_copy(src, dst, load_sem.at[i])
        for i, (src, dst) in enumerate(
            ((vis_hbm, vis), (dest_hbm, dest), (slot_hbm, slot), (off_hbm, off), (taper_hbm, taper))
        )
    ]
    for load in loads:
        load.start()
    for load in loads[:4]:
        load.wait()
    target, tile = dest[...], slot[...]
    row0 = target // 16 * ROWS_DEV + tile // 4 * TILE + off[0:1, :]
    col0 = target % 16 * COLS_DEV + tile % 4 * TILE + off[1:2, :]
    fields[z, 0:2, :] = vis[...]
    fields[z, 2:3, :] = (row0 - CELLS // 2).astype(jnp.float32)
    fields[z, 3:4, :] = (col0 - CELLS // 2).astype(jnp.float32)

    wait_if(barrier, z + jnp.where(is_hub, 0, 1))
    for there in range(RING - 1):
        gather_if(there < z, there)
    for there in range(RING - 1):
        signal_if(ready.at[jnp.where(there // 4 == half, 0, 1)], there < z, ring_peer(there))
    signal_if(here, jnp.logical_not(is_hub), hub)

    position = grp * 2 + half
    first_pixel = (position * ROWS - HALF).astype(jnp.float32)

    def project(index):
        v, w = v_ref.at[index % 2], w_ref.at[index % 2]
        part = None
        for a, b in ((0, 0), (0, 1), (1, 0)):
            product = lax.dot_general(
                v[a], w[b], (((1,), (1,)), ((), ())), preferred_element_type=jnp.float32
            )
            part = product if part is None else part + product
        if index == 0:
            acc[...] = part
        else:
            acc[...] += part

    phases(fields[z], first_pixel, v_ref.at[0], w_ref.at[0])
    loads[4].wait()
    taps = [taper[i] for i in range(SUP)]
    lane, level = lanes_of((8, 128)), rows_of((8, 128))
    within = lane % 64
    line_re, line_im = taper_sum(taps, first_pixel + (2 * (within % 32) + within // 32).astype(jnp.float32))
    norm = 1.0 / (SUP * math.sqrt(65536))
    line_re, line_im = line_re[0:1, :] * norm, line_im[0:1, :] * norm
    centre = CENTRE * (2 * (level % 2) - 1)
    col_re, col_im = taper_sum(taps, centre + jnp.where(level < 2, lane, -1 - lane).astype(jnp.float32))
    wait_if(ready.at[0], 3 - grp)
    for there in range(1, RING):
        gather_if((there > z) & (there // 4 == half), there)
    @pl.when(is_hub)
    def _():
        pl.semaphore_wait(here, OWN - 1)
        greet_plane(everyone)

    for index in range(1, RING):
        if index == 3:

            @pl.when(half == 0)
            def _():
                pl.semaphore_wait(ready.at[1], 4)
                for there in range(4, RING):
                    gather(there)

        source = ORDER[0][index - 1]
        for place in range(1, RING):
            source = jnp.where(z == place, ORDER[place][index - 1], source)
        pltpu.make_async_remote_copy(
            src_ref=fields.at[source],
            dst_ref=fields.at[source],
            send_sem=a_send,
            recv_sem=a_recv.at[source],
            device_id=pair,
            device_id_type=MESH,
        ).wait_recv()
        project(index - 1)
        phases(fields[source], first_pixel, v_ref.at[index % 2], w_ref.at[index % 2])
    project(RING - 1)
    for i in range(2):
        cos_sum = acc[0:128, 128 * i : 128 * i + 128]
        sin_sum = acc[128:256, 128 * i : 128 * i + 128]
        minus = cos_sum - pltpu.roll(sin_sum, 64, 1)
        plus = pltpu.roll(cos_sum, 64, 1) + sin_sum
        mask = lanes_of((128, 128)) < 64
        real, imag = jnp.where(mask, minus, plus), jnp.where(mask, plus, minus)
        real, imag = (line_re * real - line_im * imag).T, (line_re * imag + line_im * real).T
        for group in range(4):
            part = slice(32 * group, 32 * group + 32)
            tap = slice(group // 2 * 2 + i, group // 2 * 2 + i + 1)
            facet = col_re[tap, :] * real[part, :] - col_im[tap, :] * imag[part, :]
            for t in range(4):
                sends[pl.ds(64 * t + 2 * group + i, 8, stride=8), :] = facet[8 * t : 8 * t + 8, :]

    wait_if(everyone, jnp.where(is_hub, 0, 1))
    for i, shift in enumerate(shifts):
        start = pl.multiple_of(8 * ((core + shift[0]) % 2 * 16 + own_vert(shift)), 8)
        pltpu.make_async_remote_copy(
            src_ref=sends.at[pl.ds(start, 8), :],
            dst_ref=recvs.at[i],
            send_sem=b_send,
            recv_sem=b_recv,
            device_id=own_peer(shift),
            device_id_type=MESH,
        ).start()
    mine = pl.multiple_of(8 * (core * 16 + vert), 8)
    total = sends[pl.ds(mine, 8), :]
    batch = pltpu.make_async_remote_copy(
        src_ref=recvs, dst_ref=recvs, send_sem=b_send, recv_sem=b_recv, device_id=pair, device_id_type=MESH
    )
    batch.wait_recv()
    for i in range(len(shifts)):
        total = total + recvs[i]
    mirrored = jnp.take_along_axis(total, 127 - lane, axis=1)
    for e in range(2):
        for c in range(2):
            out_ref[e : e + 1, 256 * c + 128 : 256 * c + 256] = total[2 * e + c : 2 * e + c + 1, :]
            out_ref[e : e + 1, 256 * c : 256 * c + 128] = mirrored[4 + 2 * e + c : 5 + 2 * e + c, :]
    batch.wait_send()
    rest = fields.at[pl.ds(1, RING - 1)]
    pltpu.make_async_remote_copy(
        src_ref=rest, dst_ref=rest, send_sem=a_send, recv_sem=a_recv.at[0], device_id=pair, device_id_type=MESH
    ).wait_send()


def body(visibility, destination, tile_slot, offsets, taper):
    any_space = pl.BlockSpec(memory_space=pl.ANY)
    return pl.pallas_call(
        kernel,
        out_shape=pltpu.VMEM((2, IMG), jnp.float32),
        in_specs=[any_space] * 5,
        out_specs=pl.BlockSpec(memory_space=pltpu.VMEM),
        scratch_shapes=[
            pltpu.VMEM((2, VIS), jnp.float32),
            pltpu.VMEM((1, VIS), jnp.int32),
            pltpu.VMEM((1, VIS), jnp.int32),
            pltpu.VMEM((2, VIS), jnp.int32),
            pltpu.SMEM((SUP,), jnp.float32),
            pltpu.VMEM((RING, 4, VIS), jnp.float32),
            pltpu.VMEM((2, 2, 2 * CENTRE, VIS), jnp.bfloat16),
            pltpu.VMEM((2, 2, 4 * ROWS, VIS), jnp.bfloat16),
            pltpu.VMEM((2 * CENTRE, 4 * ROWS), jnp.float32),
            pltpu.VMEM((OWN * 8, 128), jnp.float32),
            pltpu.VMEM((OWN - 1, 8, 128), jnp.float32),
            pltpu.SemaphoreType.DMA((5,)),
            pltpu.SemaphoreType.DMA,
            pltpu.SemaphoreType.DMA((RING,)),
            pltpu.SemaphoreType.DMA,
            pltpu.SemaphoreType.DMA,
            pltpu.SemaphoreType.REGULAR((2,)),
            pltpu.SemaphoreType.REGULAR,
            pltpu.SemaphoreType.REGULAR,
        ],
        compiler_params=pltpu.CompilerParams(collective_id=0, has_side_effects=True),
    )(visibility.T, destination.T, tile_slot.reshape(1, -1), offsets.T, taper)


def solution(mesh):
    return jax.shard_map(
        body,
        mesh=mesh,
        in_specs=(
            P(("grp", "au", "vert"), None),
            P(("grp", "au", "vert"), None),
            P(("grp", "au", "vert")),
            P(("grp", "au", "vert"), None),
            P(),
        ),
        out_specs=P(("grp", "au", "vert"), None),
        check_vma=False,
    )
```

```python
import math

import jax
import jax.numpy as jnp
from jax import lax
from jax.experimental import pallas as pl
from jax.experimental.pallas import tpu as pltpu
from jax.sharding import PartitionSpec as P

TILE = 128
SUP = 8
ROWS_DEV = 2048
COLS_DEV = 512
IMG = 512
CELLS = 8192
MESH = pl.DeviceIdType.MESH

RING = 8
OWN = 32
ROWS = 64
HALF = IMG // 2
CENTRE = IMG // 4
VIS = 256

ORDER = (
    (1, 2, 3, 7, 6, 5, 4),
    (2, 3, 0, 7, 6, 4, 5),
    (3, 1, 0, 4, 5, 7, 6),
    (2, 1, 0, 4, 5, 6, 7),
    (5, 6, 7, 3, 2, 1, 0),
    (6, 7, 4, 3, 0, 2, 1),
    (7, 5, 0, 4, 3, 1, 2),
    (6, 0, 5, 1, 2, 4, 3),
)


def sincos(turns):
    turns = turns - jnp.floor(turns + 0.5)
    square = turns * turns
    sine = jnp.full_like(turns, -(math.pi**11) / math.factorial(11))
    for order in (9, 7, 5, 3, 1):
        sign = 1.0 if order % 4 == 1 else -1.0
        sine = sine * square + sign * math.pi**order / math.factorial(order)
    sine = sine * turns
    cosine = jnp.full_like(turns, math.pi**12 / math.factorial(12))
    for order in (10, 8, 6, 4, 2, 0):
        sign = 1.0 if order % 4 == 0 else -1.0
        cosine = cosine * square + sign * math.pi**order / math.factorial(order)
    return 1.0 - 2.0 * sine * sine, 2.0 * sine * cosine


def times(a, b):
    return a[0] * b[0] - a[1] * b[1], a[0] * b[1] + a[1] * b[0]


def stack(a, b):
    return jnp.concatenate([a[0], b[0]], axis=0), jnp.concatenate([a[1], b[1]], axis=0)


def split(value):
    high = value.astype(jnp.bfloat16)
    return high, (value - high.astype(jnp.float32)).astype(jnp.bfloat16)


def taper_sum(taper, pixel):
    step = sincos(pixel * (1.0 / CELLS))
    total = (jnp.full_like(pixel, taper[SUP - 1]), jnp.zeros_like(pixel))
    for tap in range(SUP - 2, -1, -1):
        re, im = times(total, step)
        total = (re + taper[tap], im)
    return total


def rows_of(shape):
    return lax.broadcasted_iota(jnp.int32, shape, 0)


def lanes_of(shape):
    return lax.broadcasted_iota(jnp.int32, shape, 1)


def phases(fields, first_pixel, v_ref, w_ref):
    unit = 1.0 / CELLS
    row = rows_of((8, 128))

    def v_at(part, place):
        return v_ref.at[pl.ds(2 * CENTRE * part + place, 16), :]

    def w_at(part, place):
        return w_ref.at[part, pl.ds(place, 16), :]

    rowf = row.astype(jnp.float32)
    power = jnp.where(row < 2, 8 << jnp.minimum(row, 1), jnp.where(row == 2, CENTRE, 16 << jnp.maximum(row - 3, 0)))
    power = jnp.where(row == 5, 1, power).astype(jnp.float32) * unit
    for lane in range(0, VIS, 128):
        re, im, x, y = (fields[i : i + 1, lane : lane + 128] for i in range(4))
        col = sincos((rowf + 0.5) * (y * unit))
        line = sincos(((first_pixel + 2.0 * rowf) * x - 0.5 * y) * unit)
        turn = sincos(power * jnp.where(row < 3, y, x))
        steps = [(turn[0][i : i + 1, :], turn[1][i : i + 1, :]) for i in range(6)]

        def store(ref, place, value):
            high, low = split(value)
            ref(0, place)[:, lane : lane + 128] = high
            ref(1, place)[:, lane : lane + 128] = low

        line = times((re, im), line)
        tiles = [stack(line, times(line, steps[3]))]
        tiles.append(times(tiles[0], steps[4]))
        tiles += [times(tile, steps[5]) for tile in tiles]
        for i, tile in enumerate(tiles):
            rr, ii, ri, ir = (tile[a] * steps[2][b] for a, b in ((0, 0), (1, 1), (0, 1), (1, 0)))
            for place, value in ((0, rr + ii), (64, ir - ri), (128, rr - ii), (192, ri + ir)):
                store(w_at, place + 16 * i, value)
        tile = stack(col, times(col, steps[0]))
        for i in range(CENTRE // 16):
            store(v_at, 16 * i, tile[0])
            store(v_at, CENTRE + 16 * i, tile[1])
            tile = times(tile, steps[1])


def kernel(
    vis_hbm, dest_hbm, slot_hbm, off_hbm, taper_hbm, out_ref,
    vis, dest, slot, off, taper, fields, v_ref, w_ref, acc, sends, recvs,
    load_sem, a_send, a_recv, b_send, b_recv, ready, here, everyone,
):
    grp, au, vert = lax.axis_index("grp"), lax.axis_index("au"), lax.axis_index("vert")
    core, half = au % 2, au // 2
    z = half * 4 + grp
    y, x = vert // 4, vert % 4

    shifts = [(c, b, a) for c in range(2) for b in range(4) for a in range(4)]
    shifts.sort(key=lambda s: -(min(s[1], 4 - s[1]) + min(s[2], 4 - s[2]) + 0.5 * s[0]))
    shifts = shifts[:-1]

    def own_vert(shift):
        return ((y + shift[1]) % 4) * 4 + (x + shift[2]) % 4

    def own_peer(shift):
        return grp, half * 2 + (core + shift[0]) % 2, own_vert(shift)

    def signal(sem, peer):
        pl.semaphore_signal(sem, inc=1, device_id=peer, device_id_type=MESH)

    def ring_peer(there):
        other = (there // 4 + half) % 2
        return there % 4, there // 4 * 2 + (core + other) % 2, vert

    pair = own_peer((1, 0, 0))
    hub = grp, half * 2 + 1, 0
    is_hub = (core == 1) & (vert == 0)

    def greet_plane(sem):
        for shift in shifts:
            signal(sem, own_peer(shift))

    def signal_if(sem, wanted, peer):
        @pl.when(wanted)
        def _():
            signal(sem, peer)

    def wait_if(sem, count):
        @pl.when(count > 0)
        def _():
            pl.semaphore_wait(sem, count)

    def gather(there):
        pltpu.make_async_remote_copy(
            src_ref=fields.at[z],
            dst_ref=fields.at[z],
            send_sem=a_send,
            recv_sem=a_recv.at[z],
            device_id=ring_peer(there),
            device_id_type=MESH,
        ).start()

    def gather_if(wanted, there):
        @pl.when(wanted)
        def _():
            gather(there)

    loads = [
        pltpu.make_async_copy(src, dst, load_sem.at[i])
        for i, (src, dst) in enumerate(
            ((vis_hbm, vis), (dest_hbm, dest), (slot_hbm, slot), (off_hbm, off), (taper_hbm, taper))
        )
    ]
    for load in loads:
        load.start()
    barrier = pltpu.get_barrier_semaphore()
    for there in range(1, RING):
        signal_if(barrier, z < there, ring_peer(there))
    pl.when(is_hub)(lambda: greet_plane(barrier))

    for load in loads[:4]:
        load.wait()
    target, tile = dest[...], slot[...]
    row0 = target // 16 * ROWS_DEV + tile // 4 * TILE + off[0:1, :]
    col0 = target % 16 * COLS_DEV + tile % 4 * TILE + off[1:2, :]
    fields[z, 0:2, :] = vis[...]
    fields[z, 2:3, :] = (row0 - CELLS // 2).astype(jnp.float32)
    fields[z, 3:4, :] = (col0 - CELLS // 2).astype(jnp.float32)

    wait_if(barrier, z + jnp.where(is_hub, 0, 1))
    for there in range(RING - 1):
        gather_if(there < z, there)
    for there in range(RING - 1):
        signal_if(ready.at[jnp.where(there // 4 == half, 0, 1)], there < z, ring_peer(there))
    signal_if(here, jnp.logical_not(is_hub), hub)

    position = grp * 2 + half
    first_pixel = (position * ROWS - HALF).astype(jnp.float32)

    def project(index):
        v, w = v_ref.at[index % 2], w_ref.at[index % 2]

        def product(a, b):
            return lax.dot_general(a, b, (((1,), (1,)), ((), ())), preferred_element_type=jnp.float32)

        both, cross = product(v[...], w[0]), product(v[0 : 2 * CENTRE, :], w[1])
        if index == 0:
            acc[0 : 4 * CENTRE, :] = both
            acc[4 * CENTRE :, :] = cross
        else:
            acc[0 : 4 * CENTRE, :] += both
            acc[4 * CENTRE :, :] += cross

    phases(fields[z], first_pixel, v_ref.at[0], w_ref.at[0])
    loads[4].wait()
    taps = [taper[i] for i in range(SUP)]
    lane, level = lanes_of((8, 128)), rows_of((8, 128))
    within = lane % 64
    line_re, line_im = taper_sum(taps, first_pixel + (2 * (within % 32) + within // 32).astype(jnp.float32))
    norm = 1.0 / (SUP * math.sqrt(65536))
    line_re, line_im = line_re[0:1, :] * norm, line_im[0:1, :] * norm
    centre = CENTRE * (2 * (level % 2) - 1)
    col_re, col_im = taper_sum(taps, centre + jnp.where(level < 2, lane, -1 - lane).astype(jnp.float32))
    wait_if(ready.at[0], 3 - grp)
    for there in range(1, RING):
        gather_if((there > z) & (there // 4 == half), there)
    @pl.when(is_hub)
    def _():
        pl.semaphore_wait(here, OWN - 1)
        greet_plane(everyone)

    for index in range(1, RING):
        if index == 3:

            @pl.when(half == 0)
            def _():
                pl.semaphore_wait(ready.at[1], 4)
                for there in range(4, RING):
                    gather(there)

        source = ORDER[0][index - 1]
        for place in range(1, RING):
            source = jnp.where(z == place, ORDER[place][index - 1], source)
        pltpu.make_async_remote_copy(
            src_ref=fields.at[source],
            dst_ref=fields.at[source],
            send_sem=a_send,
            recv_sem=a_recv.at[source],
            device_id=pair,
            device_id_type=MESH,
        ).wait_recv()
        project(index - 1)
        phases(fields[source], first_pixel, v_ref.at[index % 2], w_ref.at[index % 2])
    project(RING - 1)
    for i in range(2):
        cos_sum, sin_sum = (
            sum(acc[first + 256 * part : first + 256 * part + 128, 128 * i : 128 * i + 128] for part in range(3))
            for first in (0, 128)
        )
        minus = cos_sum - pltpu.roll(sin_sum, 64, 1)
        plus = pltpu.roll(cos_sum, 64, 1) + sin_sum
        mask = lanes_of((128, 128)) < 64
        real, imag = jnp.where(mask, minus, plus), jnp.where(mask, plus, minus)
        real, imag = (line_re * real - line_im * imag).T, (line_re * imag + line_im * real).T
        for group in range(4):
            part = slice(32 * group, 32 * group + 32)
            tap = slice(group // 2 * 2 + i, group // 2 * 2 + i + 1)
            facet = col_re[tap, :] * real[part, :] - col_im[tap, :] * imag[part, :]
            for t in range(4):
                sends[pl.ds(64 * t + 2 * group + i, 8, stride=8), :] = facet[8 * t : 8 * t + 8, :]

    wait_if(everyone, jnp.where(is_hub, 0, 1))
    for i, shift in enumerate(shifts):
        start = pl.multiple_of(8 * ((core + shift[0]) % 2 * 16 + own_vert(shift)), 8)
        pltpu.make_async_remote_copy(
            src_ref=sends.at[pl.ds(start, 8), :],
            dst_ref=recvs.at[i],
            send_sem=b_send,
            recv_sem=b_recv,
            device_id=own_peer(shift),
            device_id_type=MESH,
        ).start()
    mine = pl.multiple_of(8 * (core * 16 + vert), 8)
    total = sends[pl.ds(mine, 8), :]
    batch = pltpu.make_async_remote_copy(
        src_ref=recvs, dst_ref=recvs, send_sem=b_send, recv_sem=b_recv, device_id=pair, device_id_type=MESH
    )
    batch.wait_recv()
    for i in range(len(shifts)):
        total = total + recvs[i]
    mirrored = jnp.take_along_axis(total, 127 - lane, axis=1)
    for e in range(2):
        for c in range(2):
            out_ref[e : e + 1, 256 * c + 128 : 256 * c + 256] = total[2 * e + c : 2 * e + c + 1, :]
            out_ref[e : e + 1, 256 * c : 256 * c + 128] = mirrored[4 + 2 * e + c : 5 + 2 * e + c, :]
    batch.wait_send()
    rest = fields.at[pl.ds(1, RING - 1)]
    pltpu.make_async_remote_copy(
        src_ref=rest, dst_ref=rest, send_sem=a_send, recv_sem=a_recv.at[0], device_id=pair, device_id_type=MESH
    ).wait_send()


def body(visibility, destination, tile_slot, offsets, taper):
    any_space = pl.BlockSpec(memory_space=pl.ANY)
    return pl.pallas_call(
        kernel,
        out_shape=pltpu.VMEM((2, IMG), jnp.float32),
        in_specs=[any_space] * 5,
        out_specs=pl.BlockSpec(memory_space=pltpu.VMEM),
        scratch_shapes=[
            pltpu.VMEM((2, VIS), jnp.float32),
            pltpu.VMEM((1, VIS), jnp.int32),
            pltpu.VMEM((1, VIS), jnp.int32),
            pltpu.VMEM((2, VIS), jnp.int32),
            pltpu.SMEM((SUP,), jnp.float32),
            pltpu.VMEM((RING, 4, VIS), jnp.float32),
            pltpu.VMEM((2, 4 * CENTRE, VIS), jnp.bfloat16),
            pltpu.VMEM((2, 2, 4 * ROWS, VIS), jnp.bfloat16),
            pltpu.VMEM((6 * CENTRE, 4 * ROWS), jnp.float32),
            pltpu.VMEM((OWN * 8, 128), jnp.float32),
            pltpu.VMEM((OWN - 1, 8, 128), jnp.float32),
            pltpu.SemaphoreType.DMA((5,)),
            pltpu.SemaphoreType.DMA,
            pltpu.SemaphoreType.DMA((RING,)),
            pltpu.SemaphoreType.DMA,
            pltpu.SemaphoreType.DMA,
            pltpu.SemaphoreType.REGULAR((2,)),
            pltpu.SemaphoreType.REGULAR,
            pltpu.SemaphoreType.REGULAR,
        ],
        compiler_params=pltpu.CompilerParams(collective_id=0, has_side_effects=True),
    )(visibility.T, destination.T, tile_slot.reshape(1, -1), offsets.T, taper)


def solution(mesh):
    return jax.shard_map(
        body,
        mesh=mesh,
        in_specs=(
            P(("grp", "au", "vert"), None),
            P(("grp", "au", "vert"), None),
            P(("grp", "au", "vert")),
            P(("grp", "au", "vert"), None),
            P(),
        ),
        out_specs=P(("grp", "au", "vert"), None),
        check_vma=False,
    )
```

```python
import math

import jax
import jax.numpy as jnp
from jax import lax
from jax.experimental import pallas as pl
from jax.experimental.pallas import tpu as pltpu
from jax.sharding import PartitionSpec as P

TILE = 128
SUP = 8
ROWS_DEV = 2048
COLS_DEV = 512
IMG = 512
CELLS = 8192
MESH = pl.DeviceIdType.MESH

RING = 8
OWN = 32
ROWS = 64
HALF = IMG // 2
CENTRE = IMG // 4
VIS = 256

ORDER = (
    (1, 2, 3, 7, 6, 5, 4),
    (2, 3, 0, 7, 6, 4, 5),
    (3, 1, 0, 4, 5, 7, 6),
    (2, 1, 0, 4, 5, 6, 7),
    (5, 6, 3, 2, 7, 1, 0),
    (4, 6, 7, 3, 0, 2, 1),
    (5, 7, 4, 0, 3, 1, 2),
    (6, 5, 0, 1, 4, 2, 3),
)


def sincos(turns):
    turns = turns - jnp.floor(turns + 0.5)
    square = turns * turns
    sine = jnp.full_like(turns, -(math.pi**11) / math.factorial(11))
    for order in (9, 7, 5, 3, 1):
        sign = 1.0 if order % 4 == 1 else -1.0
        sine = sine * square + sign * math.pi**order / math.factorial(order)
    sine = sine * turns
    cosine = jnp.full_like(turns, math.pi**12 / math.factorial(12))
    for order in (10, 8, 6, 4, 2, 0):
        sign = 1.0 if order % 4 == 0 else -1.0
        cosine = cosine * square + sign * math.pi**order / math.factorial(order)
    return 1.0 - 2.0 * sine * sine, 2.0 * sine * cosine


def times(a, b):
    return a[0] * b[0] - a[1] * b[1], a[0] * b[1] + a[1] * b[0]


def stack(a, b):
    return jnp.concatenate([a[0], b[0]], axis=0), jnp.concatenate([a[1], b[1]], axis=0)


def split(value):
    high = value.astype(jnp.bfloat16)
    return high, (value - high.astype(jnp.float32)).astype(jnp.bfloat16)


def taper_sum(taper, pixel):
    step = sincos(pixel * (1.0 / CELLS))
    total = (jnp.full_like(pixel, taper[SUP - 1]), jnp.zeros_like(pixel))
    for tap in range(SUP - 2, -1, -1):
        re, im = times(total, step)
        total = (re + taper[tap], im)
    return total


def rows_of(shape):
    return lax.broadcasted_iota(jnp.int32, shape, 0)


def lanes_of(shape):
    return lax.broadcasted_iota(jnp.int32, shape, 1)


def phases(fields, first_pixel, v_ref, w_ref):
    unit = 1.0 / CELLS
    row = rows_of((8, 128))

    def v_at(part, place):
        return v_ref.at[pl.ds(2 * CENTRE * part + place, 16), :]

    def w_at(part, place):
        return w_ref.at[part, pl.ds(place, 16), :]

    rowf = row.astype(jnp.float32)
    power = jnp.where(row < 2, 8 << jnp.minimum(row, 1), jnp.where(row == 2, CENTRE, 16 << jnp.maximum(row - 3, 0)))
    power = jnp.where(row == 5, 1, power).astype(jnp.float32) * unit
    for lane in range(0, VIS, 128):
        re, im, x, y = (fields[i : i + 1, lane : lane + 128] for i in range(4))
        col = sincos((rowf + 0.5) * (y * unit))
        line = sincos(((first_pixel + 2.0 * rowf) * x - 0.5 * y) * unit)
        turn = sincos(power * jnp.where(row < 3, y, x))
        steps = [(turn[0][i : i + 1, :], turn[1][i : i + 1, :]) for i in range(6)]

        def store(ref, place, value):
            high, low = split(value)
            ref(0, place)[:, lane : lane + 128] = high
            ref(1, place)[:, lane : lane + 128] = low

        line = times((re, im), line)
        tiles = [stack(line, times(line, steps[3]))]
        tiles.append(times(tiles[0], steps[4]))
        tiles += [times(tile, steps[5]) for tile in tiles]
        for i, tile in enumerate(tiles):
            rr, ii, ri, ir = (tile[a] * steps[2][b] for a, b in ((0, 0), (1, 1), (0, 1), (1, 0)))
            for place, value in ((0, rr + ii), (64, ir - ri), (128, rr - ii), (192, ri + ir)):
                store(w_at, place + 16 * i, value)
        tile = stack(col, times(col, steps[0]))
        for i in range(CENTRE // 16):
            store(v_at, 16 * i, tile[0])
            store(v_at, CENTRE + 16 * i, tile[1])
            tile = times(tile, steps[1])


def kernel(
    vis_hbm, dest_hbm, slot_hbm, off_hbm, taper_hbm, out_ref,
    vis, dest, slot, off, taper, fields, v_ref, w_ref, acc, sends, recvs,
    load_sem, a_send, a_recv, b_send, b_recv, ready, chain, here, everyone,
):
    grp, au, vert = lax.axis_index("grp"), lax.axis_index("au"), lax.axis_index("vert")
    core, half = au % 2, au // 2
    z = half * 4 + grp
    y, x = vert // 4, vert % 4

    shifts = [(c, b, a) for c in range(2) for b in range(4) for a in range(4)]
    shifts.sort(key=lambda s: -(min(s[1], 4 - s[1]) + min(s[2], 4 - s[2]) + 0.5 * s[0]))
    shifts = shifts[:-1]

    def own_vert(shift):
        return ((y + shift[1]) % 4) * 4 + (x + shift[2]) % 4

    def own_peer(shift):
        return grp, half * 2 + (core + shift[0]) % 2, own_vert(shift)

    def signal(sem, peer):
        pl.semaphore_signal(sem, inc=1, device_id=peer, device_id_type=MESH)

    def ring_peer(there):
        other = (there // 4 + half) % 2
        return there % 4, there // 4 * 2 + (core + other) % 2, vert

    pair = own_peer((1, 0, 0))
    hub = grp, half * 2 + 1, 0
    is_hub = (core == 1) & (vert == 0)

    def greet_plane(sem):
        for shift in shifts:
            signal(sem, own_peer(shift))

    def signal_if(sem, wanted, peer):
        @pl.when(wanted)
        def _():
            signal(sem, peer)

    def wait_if(sem, count):
        @pl.when(count > 0)
        def _():
            pl.semaphore_wait(sem, count)

    def gather(there):
        pltpu.make_async_remote_copy(
            src_ref=fields.at[z],
            dst_ref=fields.at[z],
            send_sem=a_send,
            recv_sem=a_recv.at[z],
            device_id=ring_peer(there),
            device_id_type=MESH,
        ).start()

    def gather_if(wanted, there):
        @pl.when(wanted)
        def _():
            gather(there)

    loads = [
        pltpu.make_async_copy(src, dst, load_sem.at[i])
        for i, (src, dst) in enumerate(
            ((vis_hbm, vis), (dest_hbm, dest), (slot_hbm, slot), (off_hbm, off), (taper_hbm, taper))
        )
    ]
    for load in loads:
        load.start()
    barrier = pltpu.get_barrier_semaphore()
    for there in range(1, RING):
        signal_if(barrier, (z < there) & ((half == 0) | (there == z + 1)), ring_peer(there))
    pl.when(is_hub)(lambda: greet_plane(barrier))

    for load in loads[:4]:
        load.wait()
    target, tile = dest[...], slot[...]
    row0 = target // 16 * ROWS_DEV + tile // 4 * TILE + off[0:1, :]
    col0 = target % 16 * COLS_DEV + tile % 4 * TILE + off[1:2, :]
    fields[z, 0:2, :] = vis[...]
    fields[z, 2:3, :] = (row0 - CELLS // 2).astype(jnp.float32)
    fields[z, 3:4, :] = (col0 - CELLS // 2).astype(jnp.float32)

    lower = jnp.where(half == 0, z, 4 + jnp.minimum(grp, 1))
    wait_if(barrier, lower + jnp.where(is_hub, 0, 1))
    def below(there):
        return (there < z) & ((half == 0) | (there < 4) | (there == z - 1))

    for there in range(RING - 1):
        gather_if(below(there), there)
    for there in range(RING - 1):
        signal_if(ready.at[jnp.where(there // 4 == half, 0, 1)], below(there), ring_peer(there))
    signal_if(here, jnp.logical_not(is_hub), hub)

    position = grp * 2 + half
    first_pixel = (position * ROWS - HALF).astype(jnp.float32)

    def project(index):
        v, w = v_ref.at[index % 2], w_ref.at[index % 2]

        def product(a, b):
            return lax.dot_general(a, b, (((1,), (1,)), ((), ())), preferred_element_type=jnp.float32)

        both, cross = product(v[...], w[0]), product(v[0 : 2 * CENTRE, :], w[1])
        if index == 0:
            acc[0 : 4 * CENTRE, :] = both
            acc[4 * CENTRE :, :] = cross
        else:
            acc[0 : 4 * CENTRE, :] += both
            acc[4 * CENTRE :, :] += cross

    phases(fields[z], first_pixel, v_ref.at[0], w_ref.at[0])
    loads[4].wait()
    taps = [taper[i] for i in range(SUP)]
    lane, level = lanes_of((8, 128)), rows_of((8, 128))
    within = lane % 64
    line_re, line_im = taper_sum(taps, first_pixel + (2 * (within % 32) + within // 32).astype(jnp.float32))
    norm = 1.0 / (SUP * math.sqrt(65536))
    line_re, line_im = line_re[0:1, :] * norm, line_im[0:1, :] * norm
    centre = CENTRE * (2 * (level % 2) - 1)
    col_re, col_im = taper_sum(taps, centre + jnp.where(level < 2, lane, -1 - lane).astype(jnp.float32))
    @pl.when(half == 0)
    def _():
        wait_if(ready.at[0], 3 - grp)
        for there in range(1, 4):
            gather_if(there > z, there)

    @pl.when(half == 1)
    def _():
        wait_if(ready.at[0], jnp.minimum(3 - grp, 1))
        sides = [(grp + step >= 0) & (grp + step < 4) for step in (1, -1)]
        for there in range(5, RING):
            gather_if(there == z + 1, there)
        for distance in (2, 3):
            for step, side in zip((1, -1), sides):
                signal_if(chain.at[distance - 2], side, ((grp + step) % 4, au, vert))
            pl.semaphore_wait(chain.at[distance - 2], sum(side.astype(jnp.int32) for side in sides))
            for there in range(4, RING):
                gather_if((there == z + distance) | (there == z - distance), there)

    @pl.when(is_hub)
    def _():
        pl.semaphore_wait(here, OWN - 1)
        greet_plane(everyone)

    for index in range(1, RING):
        if index == 3:

            @pl.when(half == 0)
            def _():
                pl.semaphore_wait(ready.at[1], 4)
                for there in range(4, RING):
                    gather(there)

        source = ORDER[0][index - 1]
        for place in range(1, RING):
            source = jnp.where(z == place, ORDER[place][index - 1], source)
        pltpu.make_async_remote_copy(
            src_ref=fields.at[source],
            dst_ref=fields.at[source],
            send_sem=a_send,
            recv_sem=a_recv.at[source],
            device_id=pair,
            device_id_type=MESH,
        ).wait_recv()
        project(index - 1)
        phases(fields[source], first_pixel, v_ref.at[index % 2], w_ref.at[index % 2])
    project(RING - 1)
    for i in range(2):
        cos_sum, sin_sum = (
            sum(acc[first + 256 * part : first + 256 * part + 128, 128 * i : 128 * i + 128] for part in range(3))
            for first in (0, 128)
        )
        minus = cos_sum - pltpu.roll(sin_sum, 64, 1)
        plus = pltpu.roll(cos_sum, 64, 1) + sin_sum
        mask = lanes_of((128, 128)) < 64
        real, imag = jnp.where(mask, minus, plus), jnp.where(mask, plus, minus)
        real, imag = (line_re * real - line_im * imag).T, (line_re * imag + line_im * real).T
        for group in range(4):
            part = slice(32 * group, 32 * group + 32)
            tap = slice(group // 2 * 2 + i, group // 2 * 2 + i + 1)
            facet = col_re[tap, :] * real[part, :] - col_im[tap, :] * imag[part, :]
            for t in range(4):
                sends[pl.ds(64 * t + 2 * group + i, 8, stride=8), :] = facet[8 * t : 8 * t + 8, :]

    wait_if(everyone, jnp.where(is_hub, 0, 1))
    for i, shift in enumerate(shifts):
        start = pl.multiple_of(8 * ((core + shift[0]) % 2 * 16 + own_vert(shift)), 8)
        pltpu.make_async_remote_copy(
            src_ref=sends.at[pl.ds(start, 8), :],
            dst_ref=recvs.at[i],
            send_sem=b_send,
            recv_sem=b_recv,
            device_id=own_peer(shift),
            device_id_type=MESH,
        ).start()
    mine = pl.multiple_of(8 * (core * 16 + vert), 8)
    total = sends[pl.ds(mine, 8), :]
    batch = pltpu.make_async_remote_copy(
        src_ref=recvs, dst_ref=recvs, send_sem=b_send, recv_sem=b_recv, device_id=pair, device_id_type=MESH
    )
    batch.wait_recv()
    for i in range(len(shifts)):
        total = total + recvs[i]
    mirrored = jnp.take_along_axis(total, 127 - lane, axis=1)
    for e in range(2):
        for c in range(2):
            out_ref[e : e + 1, 256 * c + 128 : 256 * c + 256] = total[2 * e + c : 2 * e + c + 1, :]
            out_ref[e : e + 1, 256 * c : 256 * c + 128] = mirrored[4 + 2 * e + c : 5 + 2 * e + c, :]
    batch.wait_send()
    rest = fields.at[pl.ds(1, RING - 1)]
    pltpu.make_async_remote_copy(
        src_ref=rest, dst_ref=rest, send_sem=a_send, recv_sem=a_recv.at[0], device_id=pair, device_id_type=MESH
    ).wait_send()


def body(visibility, destination, tile_slot, offsets, taper):
    any_space = pl.BlockSpec(memory_space=pl.ANY)
    return pl.pallas_call(
        kernel,
        out_shape=pltpu.VMEM((2, IMG), jnp.float32),
        in_specs=[any_space] * 5,
        out_specs=pl.BlockSpec(memory_space=pltpu.VMEM),
        scratch_shapes=[
            pltpu.VMEM((2, VIS), jnp.float32),
            pltpu.VMEM((1, VIS), jnp.int32),
            pltpu.VMEM((1, VIS), jnp.int32),
            pltpu.VMEM((2, VIS), jnp.int32),
            pltpu.SMEM((SUP,), jnp.float32),
            pltpu.VMEM((RING, 4, VIS), jnp.float32),
            pltpu.VMEM((2, 4 * CENTRE, VIS), jnp.bfloat16),
            pltpu.VMEM((2, 2, 4 * ROWS, VIS), jnp.bfloat16),
            pltpu.VMEM((6 * CENTRE, 4 * ROWS), jnp.float32),
            pltpu.VMEM((OWN * 8, 128), jnp.float32),
            pltpu.VMEM((OWN - 1, 8, 128), jnp.float32),
            pltpu.SemaphoreType.DMA((5,)),
            pltpu.SemaphoreType.DMA,
            pltpu.SemaphoreType.DMA((RING,)),
            pltpu.SemaphoreType.DMA,
            pltpu.SemaphoreType.DMA,
            pltpu.SemaphoreType.REGULAR((2,)),
            pltpu.SemaphoreType.REGULAR((2,)),
            pltpu.SemaphoreType.REGULAR,
            pltpu.SemaphoreType.REGULAR,
        ],
        compiler_params=pltpu.CompilerParams(collective_id=0, has_side_effects=True),
    )(visibility.T, destination.T, tile_slot.reshape(1, -1), offsets.T, taper)


def solution(mesh):
    return jax.shard_map(
        body,
        mesh=mesh,
        in_specs=(
            P(("grp", "au", "vert"), None),
            P(("grp", "au", "vert"), None),
            P(("grp", "au", "vert")),
            P(("grp", "au", "vert"), None),
            P(),
        ),
        out_specs=P(("grp", "au", "vert"), None),
        check_vma=False,
    )
```

```python
import math

import jax
import jax.numpy as jnp
from jax import lax
from jax.experimental import pallas as pl
from jax.experimental.pallas import tpu as pltpu
from jax.sharding import PartitionSpec as P

TILE = 128
SUP = 8
ROWS_DEV = 2048
COLS_DEV = 512
IMG = 512
CELLS = 8192
MESH = pl.DeviceIdType.MESH

RING = 8
OWN = 32
ROWS = 64
HALF = IMG // 2
CENTRE = IMG // 4
VIS = 256

ORDER = (
    (1, 2, 3, 7, 6, 5, 4),
    (2, 3, 0, 7, 6, 4, 5),
    (3, 1, 0, 4, 5, 7, 6),
    (2, 1, 0, 4, 5, 6, 7),
    (5, 6, 3, 2, 7, 1, 0),
    (4, 6, 7, 3, 0, 2, 1),
    (5, 7, 4, 0, 3, 1, 2),
    (6, 5, 0, 1, 4, 2, 3),
)


def sincos(turns):
    turns = turns - jnp.floor(turns + 0.5)
    square = turns * turns
    sine = jnp.full_like(turns, -(math.pi**11) / math.factorial(11))
    for order in (9, 7, 5, 3, 1):
        sign = 1.0 if order % 4 == 1 else -1.0
        sine = sine * square + sign * math.pi**order / math.factorial(order)
    sine = sine * turns
    cosine = jnp.full_like(turns, math.pi**12 / math.factorial(12))
    for order in (10, 8, 6, 4, 2, 0):
        sign = 1.0 if order % 4 == 0 else -1.0
        cosine = cosine * square + sign * math.pi**order / math.factorial(order)
    return 1.0 - 2.0 * sine * sine, 2.0 * sine * cosine


def times(a, b):
    return a[0] * b[0] - a[1] * b[1], a[0] * b[1] + a[1] * b[0]


def stack(a, b):
    return jnp.concatenate([a[0], b[0]], axis=0), jnp.concatenate([a[1], b[1]], axis=0)


def split(value):
    high = value.astype(jnp.bfloat16)
    return high, (value - high.astype(jnp.float32)).astype(jnp.bfloat16)


def taper_sum(taper, pixel):
    step = sincos(pixel * (1.0 / CELLS))
    total = (jnp.full_like(pixel, taper[SUP - 1]), jnp.zeros_like(pixel))
    for tap in range(SUP - 2, -1, -1):
        re, im = times(total, step)
        total = (re + taper[tap], im)
    return total


def rows_of(shape):
    return lax.broadcasted_iota(jnp.int32, shape, 0)


def lanes_of(shape):
    return lax.broadcasted_iota(jnp.int32, shape, 1)


def phases(fields, first_pixel, v_ref, w_ref):
    unit = 1.0 / CELLS
    row = rows_of((8, 128))

    def v_at(part, place):
        return v_ref.at[pl.ds(2 * CENTRE * part + place, 16), :]

    def w_at(part, place):
        return w_ref.at[part, pl.ds(place, 16), :]

    rowf = row.astype(jnp.float32)
    power = jnp.where(row < 2, 8 << jnp.minimum(row, 1), jnp.where(row == 2, CENTRE, 16 << jnp.maximum(row - 3, 0)))
    power = jnp.where(row == 5, 1, power).astype(jnp.float32) * unit
    for lane in range(0, VIS, 128):
        re, im, x, y = (fields[i : i + 1, lane : lane + 128] for i in range(4))
        col = sincos((rowf + 0.5) * (y * unit))
        line = sincos(((first_pixel + 2.0 * rowf) * x - 0.5 * y) * unit)
        turn = sincos(power * jnp.where(row < 3, y, x))
        steps = [(turn[0][i : i + 1, :], turn[1][i : i + 1, :]) for i in range(6)]

        def store(ref, place, value):
            high, low = split(value)
            ref(0, place)[:, lane : lane + 128] = high
            ref(1, place)[:, lane : lane + 128] = low

        line = times((re, im), line)
        tiles = [stack(line, times(line, steps[3]))]
        tiles.append(times(tiles[0], steps[4]))
        tiles += [times(tile, steps[5]) for tile in tiles]
        for i, tile in enumerate(tiles):
            rr, ii, ri, ir = (tile[a] * steps[2][b] for a, b in ((0, 0), (1, 1), (0, 1), (1, 0)))
            for place, value in ((0, rr + ii), (64, ir - ri), (128, rr - ii), (192, ri + ir)):
                store(w_at, place + 16 * i, value)
        tile = stack(col, times(col, steps[0]))
        for i in range(CENTRE // 16):
            store(v_at, 16 * i, tile[0])
            store(v_at, CENTRE + 16 * i, tile[1])
            tile = times(tile, steps[1])


def early(place):
    core, y, x = place // 16, place // 4 % 4, place % 4
    return min(y, 4 - y) + min(x, 4 - x) + 0.5 * (1 - core) + (2 if place == 0 else 0)


def kernel(
    vis_hbm, dest_hbm, slot_hbm, off_hbm, taper_hbm, out_ref,
    vis, dest, slot, off, taper, fields, v_ref, w_ref, acc, sends, recvs,
    load_sem, a_send, a_recv, b_send, b_recv, ready, chain, here, everyone,
):
    grp, au, vert = lax.axis_index("grp"), lax.axis_index("au"), lax.axis_index("vert")
    core, half = au % 2, au // 2
    z = half * 4 + grp
    y, x = vert // 4, vert % 4

    shifts = [(c, b, a) for c in range(2) for b in range(4) for a in range(4)]
    shifts.sort(key=lambda s: -(min(s[1], 4 - s[1]) + min(s[2], 4 - s[2]) + 0.5 * s[0]))
    shifts = shifts[:-1]

    def own_vert(shift):
        return ((y + shift[1]) % 4) * 4 + (x + shift[2]) % 4

    def own_peer(shift):
        return grp, half * 2 + (core + shift[0]) % 2, own_vert(shift)

    def signal(sem, peer):
        pl.semaphore_signal(sem, inc=1, device_id=peer, device_id_type=MESH)

    def ring_peer(there):
        other = (there // 4 + half) % 2
        return there % 4, there // 4 * 2 + (core + other) % 2, vert

    pair = own_peer((1, 0, 0))
    hub = grp, half * 2 + 1, 0
    is_hub = (core == 1) & (vert == 0)

    def greet_plane(sem):
        for shift in shifts:
            signal(sem, own_peer(shift))

    step = 1 - 2 * core
    before, after = z - step, z + step
    before_exists = (half == 1) & (before >= 4) & (before < RING)
    after_exists = (half == 1) & (after >= 4) & (after < RING)

    def signal_if(sem, wanted, peer):
        @pl.when(wanted)
        def _():
            signal(sem, peer)

    def wait_if(sem, count):
        @pl.when(count > 0)
        def _():
            pl.semaphore_wait(sem, count)

    def gather(there):
        pltpu.make_async_remote_copy(
            src_ref=fields.at[z],
            dst_ref=fields.at[z],
            send_sem=a_send,
            recv_sem=a_recv.at[z],
            device_id=ring_peer(there),
            device_id_type=MESH,
        ).start()

    def gather_if(wanted, there):
        @pl.when(wanted)
        def _():
            gather(there)

    loads = [
        pltpu.make_async_copy(src, dst, load_sem.at[i])
        for i, (src, dst) in enumerate(
            ((vis_hbm, vis), (dest_hbm, dest), (slot_hbm, slot), (off_hbm, off), (taper_hbm, taper))
        )
    ]
    for load in loads:
        load.start()
    barrier = pltpu.get_barrier_semaphore()
    for there in range(1, RING):
        signal_if(barrier, ((half == 0) & (z < there)) | (after_exists & (there == after)), ring_peer(there))
    pl.when(is_hub)(lambda: greet_plane(barrier))

    for load in loads[:4]:
        load.wait()
    target, tile = dest[...], slot[...]
    row0 = target // 16 * ROWS_DEV + tile // 4 * TILE + off[0:1, :]
    col0 = target % 16 * COLS_DEV + tile % 4 * TILE + off[1:2, :]
    fields[z, 0:2, :] = vis[...]
    fields[z, 2:3, :] = (row0 - CELLS // 2).astype(jnp.float32)
    fields[z, 3:4, :] = (col0 - CELLS // 2).astype(jnp.float32)

    lower = jnp.where(half == 0, z, 4 + before_exists.astype(jnp.int32))
    wait_if(barrier, lower + jnp.where(is_hub, 0, 1))
    def below(there):
        return ((there < z) & ((half == 0) | (there < 4))) | (before_exists & (there == before))

    for there in range(RING):
        gather_if(below(there), there)
    for there in range(RING):
        signal_if(ready.at[jnp.where(there // 4 == half, 0, 1)], below(there), ring_peer(there))
    signal_if(here, jnp.logical_not(is_hub), hub)

    position = grp * 2 + half
    first_pixel = (position * ROWS - HALF).astype(jnp.float32)

    def project(index):
        v, w = v_ref.at[index % 2], w_ref.at[index % 2]

        def product(a, b):
            return lax.dot_general(a, b, (((1,), (1,)), ((), ())), preferred_element_type=jnp.float32)

        both, cross = product(v[...], w[0]), product(v[0 : 2 * CENTRE, :], w[1])
        if index == 0:
            acc[0 : 4 * CENTRE, :] = both
            acc[4 * CENTRE :, :] = cross
        else:
            acc[0 : 4 * CENTRE, :] += both
            acc[4 * CENTRE :, :] += cross

    phases(fields[z], first_pixel, v_ref.at[0], w_ref.at[0])
    loads[4].wait()
    taps = [taper[i] for i in range(SUP)]
    lane, level = lanes_of((8, 128)), rows_of((8, 128))
    within = lane % 64
    line_re, line_im = taper_sum(taps, first_pixel + (2 * (within % 32) + within // 32).astype(jnp.float32))
    norm = 1.0 / (SUP * math.sqrt(65536))
    line_re, line_im = line_re[0:1, :] * norm, line_im[0:1, :] * norm
    centre = CENTRE * (2 * (level % 2) - 1)
    col_re, col_im = taper_sum(taps, centre + jnp.where(level < 2, lane, -1 - lane).astype(jnp.float32))
    @pl.when(half == 0)
    def _():
        wait_if(ready.at[0], 3 - grp)
        for there in range(1, 4):
            gather_if(there > z, there)

    @pl.when(half == 1)
    def _():
        wait_if(ready.at[0], after_exists.astype(jnp.int32))
        sides = [(grp + step >= 0) & (grp + step < 4) for step in (1, -1)]
        for there in range(4, RING):
            gather_if(after_exists & (there == after), there)
        for distance in (2, 3):
            for step, side in zip((1, -1), sides):
                signal_if(chain.at[distance - 2], side, ((grp + step) % 4, au, vert))
            pl.semaphore_wait(chain.at[distance - 2], sum(side.astype(jnp.int32) for side in sides))
            for there in range(4, RING):
                gather_if((there == z + distance) | (there == z - distance), there)

    @pl.when(is_hub)
    def _():
        pl.semaphore_wait(here, OWN - 1)
        greet_plane(everyone)

    for index in range(1, RING):
        if index == 4:

            @pl.when(half == 0)
            def _():
                pl.semaphore_wait(ready.at[1], 4)
                for there in range(4, RING):
                    gather(there)

        source = ORDER[0][index - 1]
        for place in range(1, RING):
            source = jnp.where(z == place, ORDER[place][index - 1], source)
        pltpu.make_async_remote_copy(
            src_ref=fields.at[source],
            dst_ref=fields.at[source],
            send_sem=a_send,
            recv_sem=a_recv.at[source],
            device_id=pair,
            device_id_type=MESH,
        ).wait_recv()
        project(index - 1)
        phases(fields[source], first_pixel, v_ref.at[index % 2], w_ref.at[index % 2])
    project(RING - 1)
    for i in range(2):
        cos_sum, sin_sum = (
            sum(acc[first + 256 * part : first + 256 * part + 128, 128 * i : 128 * i + 128] for part in range(3))
            for first in (0, 128)
        )
        minus = cos_sum - pltpu.roll(sin_sum, 64, 1)
        plus = pltpu.roll(cos_sum, 64, 1) + sin_sum
        mask = lanes_of((128, 128)) < 64
        real, imag = jnp.where(mask, minus, plus), jnp.where(mask, plus, minus)
        real, imag = (line_re * real - line_im * imag).T, (line_re * imag + line_im * real).T
        for group in range(4):
            part = slice(32 * group, 32 * group + 32)
            tap = slice(group // 2 * 2 + i, group // 2 * 2 + i + 1)
            facet = col_re[tap, :] * real[part, :] - col_im[tap, :] * imag[part, :]
            for t in range(4):
                sends[pl.ds(64 * t + 2 * group + i, 8, stride=8), :] = facet[8 * t : 8 * t + 8, :]

    wait_if(everyone, jnp.where(is_hub, 0, 1))
    mine = core * 16 + vert
    for place in sorted(range(OWN), key=early):
        there = grp, half * 2 + place // 16, place % 16

        @pl.when(mine != place)
        def _():
            pltpu.make_async_remote_copy(
                src_ref=sends.at[pl.ds(8 * place, 8), :],
                dst_ref=recvs.at[mine],
                send_sem=b_send,
                recv_sem=b_recv,
                device_id=there,
                device_id_type=MESH,
            ).start()

    recvs[mine] = sends[pl.ds(pl.multiple_of(8 * mine, 8), 8), :]
    others = recvs.at[pl.ds(1, OWN - 1)]
    batch = pltpu.make_async_remote_copy(
        src_ref=others, dst_ref=others, send_sem=b_send, recv_sem=b_recv, device_id=pair, device_id_type=MESH
    )
    batch.wait_recv()
    total = recvs[0]
    for i in range(1, OWN):
        total = total + recvs[i]
    mirrored = jnp.take_along_axis(total, 127 - lane, axis=1)
    for e in range(2):
        for c in range(2):
            out_ref[e : e + 1, 256 * c + 128 : 256 * c + 256] = total[2 * e + c : 2 * e + c + 1, :]
            out_ref[e : e + 1, 256 * c : 256 * c + 128] = mirrored[4 + 2 * e + c : 5 + 2 * e + c, :]
    batch.wait_send()
    rest = fields.at[pl.ds(1, RING - 1)]
    pltpu.make_async_remote_copy(
        src_ref=rest, dst_ref=rest, send_sem=a_send, recv_sem=a_recv.at[0], device_id=pair, device_id_type=MESH
    ).wait_send()


def body(visibility, destination, tile_slot, offsets, taper):
    any_space = pl.BlockSpec(memory_space=pl.ANY)
    return pl.pallas_call(
        kernel,
        out_shape=pltpu.VMEM((2, IMG), jnp.float32),
        in_specs=[any_space] * 5,
        out_specs=pl.BlockSpec(memory_space=pltpu.VMEM),
        scratch_shapes=[
            pltpu.VMEM((2, VIS), jnp.float32),
            pltpu.VMEM((1, VIS), jnp.int32),
            pltpu.VMEM((1, VIS), jnp.int32),
            pltpu.VMEM((2, VIS), jnp.int32),
            pltpu.SMEM((SUP,), jnp.float32),
            pltpu.VMEM((RING, 4, VIS), jnp.float32),
            pltpu.VMEM((2, 4 * CENTRE, VIS), jnp.bfloat16),
            pltpu.VMEM((2, 2, 4 * ROWS, VIS), jnp.bfloat16),
            pltpu.VMEM((6 * CENTRE, 4 * ROWS), jnp.float32),
            pltpu.VMEM((OWN * 8, 128), jnp.float32),
            pltpu.VMEM((OWN, 8, 128), jnp.float32),
            pltpu.SemaphoreType.DMA((5,)),
            pltpu.SemaphoreType.DMA,
            pltpu.SemaphoreType.DMA((RING,)),
            pltpu.SemaphoreType.DMA,
            pltpu.SemaphoreType.DMA,
            pltpu.SemaphoreType.REGULAR((2,)),
            pltpu.SemaphoreType.REGULAR((2,)),
            pltpu.SemaphoreType.REGULAR,
            pltpu.SemaphoreType.REGULAR,
        ],
        compiler_params=pltpu.CompilerParams(collective_id=0, has_side_effects=True),
    )(visibility.T, destination.T, tile_slot.reshape(1, -1), offsets.T, taper)


def solution(mesh):
    return jax.shard_map(
        body,
        mesh=mesh,
        in_specs=(
            P(("grp", "au", "vert"), None),
            P(("grp", "au", "vert"), None),
            P(("grp", "au", "vert")),
            P(("grp", "au", "vert"), None),
            P(),
        ),
        out_specs=P(("grp", "au", "vert"), None),
        check_vma=False,
    )
```

```python
import math

import jax
import jax.numpy as jnp
from jax import lax
from jax.experimental import pallas as pl
from jax.experimental.pallas import tpu as pltpu
from jax.sharding import PartitionSpec as P

TILE = 128
SUP = 8
ROWS_DEV = 2048
COLS_DEV = 512
IMG = 512
CELLS = 8192
MESH = pl.DeviceIdType.MESH

RING = 8
OWN = 32
ROWS = 64
HALF = IMG // 2
CENTRE = IMG // 4
VIS = 256

ORDER = (
    (1, 2, 3, 7, 6, 5, 4),
    (2, 3, 0, 7, 6, 4, 5),
    (3, 1, 0, 4, 5, 7, 6),
    (2, 1, 0, 4, 5, 6, 7),
    (5, 6, 3, 2, 7, 1, 0),
    (4, 6, 7, 3, 0, 2, 1),
    (5, 7, 4, 0, 3, 1, 2),
    (6, 5, 0, 1, 4, 2, 3),
)


def sincos(turns):
    turns = turns - jnp.floor(turns + 0.5)
    square = turns * turns
    sine = jnp.full_like(turns, -(math.pi**11) / math.factorial(11))
    for order in (9, 7, 5, 3, 1):
        sign = 1.0 if order % 4 == 1 else -1.0
        sine = sine * square + sign * math.pi**order / math.factorial(order)
    sine = sine * turns
    cosine = jnp.full_like(turns, math.pi**12 / math.factorial(12))
    for order in (10, 8, 6, 4, 2, 0):
        sign = 1.0 if order % 4 == 0 else -1.0
        cosine = cosine * square + sign * math.pi**order / math.factorial(order)
    return 1.0 - 2.0 * sine * sine, 2.0 * sine * cosine


def times(a, b):
    return a[0] * b[0] - a[1] * b[1], a[0] * b[1] + a[1] * b[0]


def stack(a, b):
    return jnp.concatenate([a[0], b[0]], axis=0), jnp.concatenate([a[1], b[1]], axis=0)


def split(value):
    high = value.astype(jnp.bfloat16)
    return high, (value - high.astype(jnp.float32)).astype(jnp.bfloat16)


def taper_sum(taper, pixel):
    step = sincos(pixel * (1.0 / CELLS))
    total = (jnp.full_like(pixel, taper[SUP - 1]), jnp.zeros_like(pixel))
    for tap in range(SUP - 2, -1, -1):
        re, im = times(total, step)
        total = (re + taper[tap], im)
    return total


def rows_of(shape):
    return lax.broadcasted_iota(jnp.int32, shape, 0)


def lanes_of(shape):
    return lax.broadcasted_iota(jnp.int32, shape, 1)


def phases(fields, first_pixel, v_ref, w_ref):
    unit = 1.0 / CELLS
    row = rows_of((8, 128))

    def v_at(part, place):
        return v_ref.at[part, pl.ds(place, 16), :]

    def w_at(part, place):
        return w_ref.at[pl.ds(4 * ROWS * part + place, 16), :]

    rowf = row.astype(jnp.float32)
    power = jnp.where(row < 2, 8 << jnp.minimum(row, 1), jnp.where(row == 2, CENTRE, 16 << jnp.maximum(row - 3, 0)))
    power = jnp.where(row == 5, 1, power).astype(jnp.float32) * unit
    for lane in range(0, VIS, 128):
        re, im, x, y = (fields[i : i + 1, lane : lane + 128] for i in range(4))
        col = sincos((rowf + 0.5) * (y * unit))
        line = sincos(((first_pixel + 2.0 * rowf) * x - 0.5 * y) * unit)
        turn = sincos(power * jnp.where(row < 3, y, x))
        steps = [(turn[0][i : i + 1, :], turn[1][i : i + 1, :]) for i in range(6)]

        def store(ref, place, value):
            high, low = split(value)
            ref(0, place)[:, lane : lane + 128] = high
            ref(1, place)[:, lane : lane + 128] = low

        line = times((re, im), line)
        tiles = [stack(line, times(line, steps[3]))]
        tiles.append(times(tiles[0], steps[4]))
        tiles += [times(tile, steps[5]) for tile in tiles]
        for i, tile in enumerate(tiles):
            rr, ii, ri, ir = (tile[a] * steps[2][b] for a, b in ((0, 0), (1, 1), (0, 1), (1, 0)))
            for place, value in ((0, rr + ii), (64, ir - ri), (128, rr - ii), (192, ri + ir)):
                store(w_at, place + 16 * i, value)
        tile = stack(col, times(col, steps[0]))
        for i in range(CENTRE // 16):
            store(v_at, 16 * i, tile[0])
            store(v_at, CENTRE + 16 * i, tile[1])
            tile = times(tile, steps[1])


def early(place):
    core, y, x = place // 16, place // 4 % 4, place % 4
    return min(y, 4 - y) + min(x, 4 - x) + 0.5 * (1 - core) + (2 if place == 0 else 0)


def kernel(
    vis_hbm, dest_hbm, slot_hbm, off_hbm, taper_hbm, out_ref,
    vis, dest, slot, off, taper, fields, v_ref, w_ref, acc, tt, sends, recvs,
    load_sem, a_send, a_recv, b_send, b_recv, ready, chain, here, everyone,
):
    grp, au, vert = lax.axis_index("grp"), lax.axis_index("au"), lax.axis_index("vert")
    core, half = au % 2, au // 2
    z = half * 4 + grp
    y, x = vert // 4, vert % 4

    shifts = [(c, b, a) for c in range(2) for b in range(4) for a in range(4)]
    shifts.sort(key=lambda s: -(min(s[1], 4 - s[1]) + min(s[2], 4 - s[2]) + 0.5 * s[0]))
    shifts = shifts[:-1]

    def own_vert(shift):
        return ((y + shift[1]) % 4) * 4 + (x + shift[2]) % 4

    def own_peer(shift):
        return grp, half * 2 + (core + shift[0]) % 2, own_vert(shift)

    def signal(sem, peer):
        pl.semaphore_signal(sem, inc=1, device_id=peer, device_id_type=MESH)

    def ring_peer(there):
        other = (there // 4 + half) % 2
        return there % 4, there // 4 * 2 + (core + other) % 2, vert

    pair = own_peer((1, 0, 0))
    hub = grp, half * 2 + 1, 0
    is_hub = (core == 1) & (vert == 0)

    def greet_plane(sem):
        for shift in shifts:
            signal(sem, own_peer(shift))

    step = 1 - 2 * core
    before, after = z - step, z + step
    before_exists = (half == 1) & (before >= 4) & (before < RING)
    after_exists = (half == 1) & (after >= 4) & (after < RING)

    def signal_if(sem, wanted, peer):
        @pl.when(wanted)
        def _():
            signal(sem, peer)

    def wait_if(sem, count):
        @pl.when(count > 0)
        def _():
            pl.semaphore_wait(sem, count)

    def gather(there):
        pltpu.make_async_remote_copy(
            src_ref=fields.at[z],
            dst_ref=fields.at[z],
            send_sem=a_send,
            recv_sem=a_recv.at[z],
            device_id=ring_peer(there),
            device_id_type=MESH,
        ).start()

    def gather_if(wanted, there):
        @pl.when(wanted)
        def _():
            gather(there)

    loads = [
        pltpu.make_async_copy(src, dst, load_sem.at[i])
        for i, (src, dst) in enumerate(
            ((vis_hbm, vis), (dest_hbm, dest), (slot_hbm, slot), (off_hbm, off), (taper_hbm, taper))
        )
    ]
    for load in loads:
        load.start()
    barrier = pltpu.get_barrier_semaphore()
    for there in range(1, RING):
        signal_if(barrier, ((half == 0) & (z < there)) | (after_exists & (there == after)), ring_peer(there))
    pl.when(is_hub)(lambda: greet_plane(barrier))

    for load in loads[:4]:
        load.wait()
    target, tile = dest[...], slot[...]
    row0 = target // 16 * ROWS_DEV + tile // 4 * TILE + off[0:1, :]
    col0 = target % 16 * COLS_DEV + tile % 4 * TILE + off[1:2, :]
    fields[z, 0:2, :] = vis[...]
    fields[z, 2:3, :] = (row0 - CELLS // 2).astype(jnp.float32)
    fields[z, 3:4, :] = (col0 - CELLS // 2).astype(jnp.float32)

    lower = jnp.where(half == 0, z, 4 + before_exists.astype(jnp.int32))
    wait_if(barrier, lower + jnp.where(is_hub, 0, 1))
    def below(there):
        return ((there < z) & ((half == 0) | (there < 4))) | (before_exists & (there == before))

    for there in range(RING):
        gather_if(below(there), there)
    for there in range(RING):
        signal_if(ready.at[jnp.where(there // 4 == half, 0, 1)], below(there), ring_peer(there))
    signal_if(here, jnp.logical_not(is_hub), hub)

    position = grp * 2 + half
    first_pixel = (position * ROWS - HALF).astype(jnp.float32)

    def project(index):
        v, w = v_ref.at[index % 2], w_ref.at[index % 2]

        def product(a, b):
            return lax.dot_general(a, b, (((1,), (1,)), ((), ())), preferred_element_type=jnp.float32)

        both, cross = product(w[...], v[0]), product(w[0 : 4 * ROWS, :], v[1])
        if index == 0:
            acc[0 : 8 * ROWS, :] = both
            acc[8 * ROWS :, :] = cross
        else:
            acc[0 : 8 * ROWS, :] += both
            acc[8 * ROWS :, :] += cross

    phases(fields[z], first_pixel, v_ref.at[0], w_ref.at[0])
    loads[4].wait()
    taps = [taper[i] for i in range(SUP)]
    lane, level = lanes_of((8, 128)), rows_of((8, 128))
    line_row = rows_of((ROWS, 128))
    line = taper_sum(taps, first_pixel + (2 * (line_row % 32) + line_row // 32).astype(jnp.float32))
    centre = CENTRE * (2 * (level % 2) - 1)
    columns = taper_sum(taps, centre + jnp.where(level < 2, lane, -1 - lane).astype(jnp.float32))
    norm = 1.0 / (SUP * math.sqrt(65536))
    for i in range(4):
        pair_re, pair_im = times(line, (columns[0][i : i + 1, :] * norm, columns[1][i : i + 1, :] * norm))
        tt[i, 0] = pair_re
        tt[i, 1] = pair_im
    @pl.when(half == 0)
    def _():
        wait_if(ready.at[0], 3 - grp)
        for there in range(1, 4):
            gather_if(there > z, there)

    @pl.when(half == 1)
    def _():
        wait_if(ready.at[0], after_exists.astype(jnp.int32))
        sides = [(grp + step >= 0) & (grp + step < 4) for step in (1, -1)]
        for there in range(4, RING):
            gather_if(after_exists & (there == after), there)
        for distance in (2, 3):
            for step, side in zip((1, -1), sides):
                signal_if(chain.at[distance - 2], side, ((grp + step) % 4, au, vert))
            pl.semaphore_wait(chain.at[distance - 2], sum(side.astype(jnp.int32) for side in sides))
            for there in range(4, RING):
                gather_if((there == z + distance) | (there == z - distance), there)

    @pl.when(is_hub)
    def _():
        pl.semaphore_wait(here, OWN - 1)
        greet_plane(everyone)

    for index in range(1, RING):
        if index == 3:

            @pl.when(half == 0)
            def _():
                pl.semaphore_wait(ready.at[1], 4)
                for there in range(4, RING):
                    gather(there)

        source = ORDER[0][index - 1]
        for place in range(1, RING):
            source = jnp.where(z == place, ORDER[place][index - 1], source)
        pltpu.make_async_remote_copy(
            src_ref=fields.at[source],
            dst_ref=fields.at[source],
            send_sem=a_send,
            recv_sem=a_recv.at[source],
            device_id=pair,
            device_id_type=MESH,
        ).wait_recv()
        project(index - 1)
        phases(fields[source], first_pixel, v_ref.at[index % 2], w_ref.at[index % 2])
    project(RING - 1)
    for c in range(2):
        re_cos, re_sin, im_cos, im_sin = (
            sum(acc[first + 4 * ROWS * i : first + 4 * ROWS * i + ROWS, place : place + 128] for i in range(3))
            for first in (128 * c, 128 * c + ROWS)
            for place in (0, 128)
        )
        sides = (re_cos - im_sin, im_cos + re_sin), (re_cos + im_sin, im_cos - re_sin)
        for side, (real, imag) in enumerate(sides):
            facet = tt[2 * side + c, 0] * real - tt[2 * side + c, 1] * imag
            for e in range(2):
                for t in range(4):
                    sends[pl.ds(64 * t + 4 * side + 2 * e + c, 8, stride=8), :] = facet[
                        32 * e + 8 * t : 32 * e + 8 * t + 8, :
                    ]

    wait_if(everyone, jnp.where(is_hub, 0, 1))
    mine = core * 16 + vert
    for place in sorted(range(OWN), key=early):
        there = grp, half * 2 + place // 16, place % 16

        @pl.when(mine != place)
        def _():
            pltpu.make_async_remote_copy(
                src_ref=sends.at[pl.ds(8 * place, 8), :],
                dst_ref=recvs.at[mine],
                send_sem=b_send,
                recv_sem=b_recv,
                device_id=there,
                device_id_type=MESH,
            ).start()

    recvs[mine] = sends[pl.ds(pl.multiple_of(8 * mine, 8), 8), :]
    others = recvs.at[pl.ds(1, OWN - 1)]
    batch = pltpu.make_async_remote_copy(
        src_ref=others, dst_ref=others, send_sem=b_send, recv_sem=b_recv, device_id=pair, device_id_type=MESH
    )
    batch.wait_recv()
    total = recvs[0]
    for i in range(1, OWN):
        total = total + recvs[i]
    mirrored = jnp.take_along_axis(total, 127 - lane, axis=1)
    for e in range(2):
        for c in range(2):
            out_ref[e : e + 1, 256 * c + 128 : 256 * c + 256] = total[2 * e + c : 2 * e + c + 1, :]
            out_ref[e : e + 1, 256 * c : 256 * c + 128] = mirrored[4 + 2 * e + c : 5 + 2 * e + c, :]
    batch.wait_send()
    rest = fields.at[pl.ds(1, RING - 1)]
    pltpu.make_async_remote_copy(
        src_ref=rest, dst_ref=rest, send_sem=a_send, recv_sem=a_recv.at[0], device_id=pair, device_id_type=MESH
    ).wait_send()


def body(visibility, destination, tile_slot, offsets, taper):
    any_space = pl.BlockSpec(memory_space=pl.ANY)
    return pl.pallas_call(
        kernel,
        out_shape=pltpu.VMEM((2, IMG), jnp.float32),
        in_specs=[any_space] * 5,
        out_specs=pl.BlockSpec(memory_space=pltpu.VMEM),
        scratch_shapes=[
            pltpu.VMEM((2, VIS), jnp.float32),
            pltpu.VMEM((1, VIS), jnp.int32),
            pltpu.VMEM((1, VIS), jnp.int32),
            pltpu.VMEM((2, VIS), jnp.int32),
            pltpu.SMEM((SUP,), jnp.float32),
            pltpu.VMEM((RING, 4, VIS), jnp.float32),
            pltpu.VMEM((2, 2, 2 * CENTRE, VIS), jnp.bfloat16),
            pltpu.VMEM((2, 8 * ROWS, VIS), jnp.bfloat16),
            pltpu.VMEM((12 * ROWS, 2 * CENTRE), jnp.float32),
            pltpu.VMEM((4, 2, ROWS, 128), jnp.float32),
            pltpu.VMEM((OWN * 8, 128), jnp.float32),
            pltpu.VMEM((OWN, 8, 128), jnp.float32),
            pltpu.SemaphoreType.DMA((5,)),
            pltpu.SemaphoreType.DMA,
            pltpu.SemaphoreType.DMA((RING,)),
            pltpu.SemaphoreType.DMA,
            pltpu.SemaphoreType.DMA,
            pltpu.SemaphoreType.REGULAR((2,)),
            pltpu.SemaphoreType.REGULAR((2,)),
            pltpu.SemaphoreType.REGULAR,
            pltpu.SemaphoreType.REGULAR,
        ],
        compiler_params=pltpu.CompilerParams(collective_id=0, has_side_effects=True),
    )(visibility.T, destination.T, tile_slot.reshape(1, -1), offsets.T, taper)


def solution(mesh):
    return jax.shard_map(
        body,
        mesh=mesh,
        in_specs=(
            P(("grp", "au", "vert"), None),
            P(("grp", "au", "vert"), None),
            P(("grp", "au", "vert")),
            P(("grp", "au", "vert"), None),
            P(),
        ),
        out_specs=P(("grp", "au", "vert"), None),
        check_vma=False,
    )
```

```python
import math

import jax
import jax.numpy as jnp
from jax import lax
from jax.experimental import pallas as pl
from jax.experimental.pallas import tpu as pltpu
from jax.sharding import PartitionSpec as P

TILE = 128
SUP = 8
ROWS_DEV = 2048
COLS_DEV = 512
IMG = 512
CELLS = 8192
MESH = pl.DeviceIdType.MESH

RING = 8
OWN = 32
ROWS = 64
HALF = IMG // 2
CENTRE = IMG // 4
VIS = 256

ORDER = (
    (1, 2, 3, 6, 5, 7),
    (2, 3, 0, 7, 6, 5),
    (3, 1, 0, 5, 7, 6),
    (2, 1, 0, 5, 6, 7),
    (5, 6, 3, 2, 7, 1, 0),
    (4, 6, 7, 3, 0, 2, 1),
    (5, 7, 4, 0, 3, 1, 2),
    (6, 5, 0, 1, 4, 2, 3),
    (1, 2, 3, 7, 6, 8, 5, 4),
    (2, 3, 0, 7, 8, 6, 4, 5),
    (3, 1, 0, 8, 4, 5, 7, 6),
    (2, 1, 0, 8, 4, 5, 6, 7),
    (5, 6, 3, 2, 7, 1, 0),
    (4, 6, 7, 3, 0, 2, 1),
    (5, 7, 4, 0, 3, 1, 2),
    (6, 5, 0, 1, 4, 2, 3),
)


def sincos(turns):
    turns = turns - jnp.floor(turns + 0.5)
    square = turns * turns
    sine = jnp.full_like(turns, -(math.pi**11) / math.factorial(11))
    for order in (9, 7, 5, 3, 1):
        sign = 1.0 if order % 4 == 1 else -1.0
        sine = sine * square + sign * math.pi**order / math.factorial(order)
    sine = sine * turns
    cosine = jnp.full_like(turns, math.pi**12 / math.factorial(12))
    for order in (10, 8, 6, 4, 2, 0):
        sign = 1.0 if order % 4 == 0 else -1.0
        cosine = cosine * square + sign * math.pi**order / math.factorial(order)
    return 1.0 - 2.0 * sine * sine, 2.0 * sine * cosine


def times(a, b):
    return a[0] * b[0] - a[1] * b[1], a[0] * b[1] + a[1] * b[0]


def stack(a, b):
    return jnp.concatenate([a[0], b[0]], axis=0), jnp.concatenate([a[1], b[1]], axis=0)


def split(value):
    high = value.astype(jnp.bfloat16)
    return high, (value - high.astype(jnp.float32)).astype(jnp.bfloat16)


def taper_sum(taper, pixel):
    step = sincos(pixel * (1.0 / CELLS))
    total = (jnp.full_like(pixel, taper[SUP - 1]), jnp.zeros_like(pixel))
    for tap in range(SUP - 2, -1, -1):
        re, im = times(total, step)
        total = (re + taper[tap], im)
    return total


def rows_of(shape):
    return lax.broadcasted_iota(jnp.int32, shape, 0)


def lanes_of(shape):
    return lax.broadcasted_iota(jnp.int32, shape, 1)


def phases(fields, first_pixel, v_ref, w_ref):
    unit = 1.0 / CELLS
    row = rows_of((8, 128))

    def v_at(part, place):
        return v_ref.at[part, pl.ds(place, 16), :]

    def w_at(part, place):
        return w_ref.at[pl.ds(4 * ROWS * part + place, 16), :]

    rowf = row.astype(jnp.float32)
    power = jnp.where(row < 2, 8 << jnp.minimum(row, 1), jnp.where(row == 2, CENTRE, 16 << jnp.maximum(row - 3, 0)))
    power = jnp.where(row == 5, 1, power).astype(jnp.float32) * unit
    for lane in range(0, VIS, 128):
        re, im, x, y = (fields[i : i + 1, lane : lane + 128] for i in range(4))
        col = sincos((rowf + 0.5) * (y * unit))
        line = sincos(((first_pixel + 2.0 * rowf) * x - 0.5 * y) * unit)
        turn = sincos(power * jnp.where(row < 3, y, x))
        steps = [(turn[0][i : i + 1, :], turn[1][i : i + 1, :]) for i in range(6)]

        def store(ref, place, value):
            high, low = split(value)
            ref(0, place)[:, lane : lane + 128] = high
            ref(1, place)[:, lane : lane + 128] = low

        line = times((re, im), line)
        tiles = [stack(line, times(line, steps[3]))]
        tiles.append(times(tiles[0], steps[4]))
        tiles += [times(tile, steps[5]) for tile in tiles]
        for i, tile in enumerate(tiles):
            rr, ii, ri, ir = (tile[a] * steps[2][b] for a, b in ((0, 0), (1, 1), (0, 1), (1, 0)))
            for place, value in ((0, rr + ii), (64, ir - ri), (128, rr - ii), (192, ri + ir)):
                store(w_at, place + 16 * i, value)
        tile = stack(col, times(col, steps[0]))
        for i in range(CENTRE // 16):
            store(v_at, 16 * i, tile[0])
            store(v_at, CENTRE + 16 * i, tile[1])
            tile = times(tile, steps[1])


def early(place):
    core, y, x = place // 16, place // 4 % 4, place % 4
    return min(y, 4 - y) + min(x, 4 - x) + 0.5 * (1 - core) + (2 if place == 0 else 0)


def kernel(
    vis_hbm, dest_hbm, slot_hbm, off_hbm, taper_hbm, out_ref,
    vis, dest, slot, off, taper, fields, v_ref, w_ref, acc, tt, sends, recvs,
    load_sem, a_send, a_recv, b_send, b_recv, ready, chain, here, everyone,
):
    grp, au, vert = lax.axis_index("grp"), lax.axis_index("au"), lax.axis_index("vert")
    core, half = au % 2, au // 2
    z = half * 4 + grp
    y, x = vert // 4, vert % 4

    shifts = [(c, b, a) for c in range(2) for b in range(4) for a in range(4)]
    shifts.sort(key=lambda s: -(min(s[1], 4 - s[1]) + min(s[2], 4 - s[2]) + 0.5 * s[0]))
    shifts = shifts[:-1]

    def own_vert(shift):
        return ((y + shift[1]) % 4) * 4 + (x + shift[2]) % 4

    def own_peer(shift):
        return grp, half * 2 + (core + shift[0]) % 2, own_vert(shift)

    def signal(sem, peer):
        pl.semaphore_signal(sem, inc=1, device_id=peer, device_id_type=MESH)

    def ring_peer(there):
        other = (there // 4 + half) % 2
        return there % 4, there // 4 * 2 + (core + other) % 2, vert

    pair = own_peer((1, 0, 0))
    hub = grp, half * 2 + 1, 0
    is_hub = (core == 1) & (vert == 0)

    def greet_plane(sem):
        for shift in shifts:
            signal(sem, own_peer(shift))

    step = 1 - 2 * core
    before, after = z - step, z + step
    before_exists = (half == 1) & (before >= 4) & (before < RING)
    after_exists = (half == 1) & (after >= 4) & (after < RING)

    def signal_if(sem, wanted, peer):
        @pl.when(wanted)
        def _():
            signal(sem, peer)

    def wait_if(sem, count):
        @pl.when(count > 0)
        def _():
            pl.semaphore_wait(sem, count)

    turned = (z == 4) & (core == 1)

    def gather(there):
        straight = turned & (there < 4)
        place, target, line = ring_peer(there)
        slot_there = jnp.where(straight, RING, z)
        pltpu.make_async_remote_copy(
            src_ref=fields.at[z],
            dst_ref=fields.at[slot_there],
            send_sem=a_send,
            recv_sem=a_recv.at[slot_there],
            device_id=(place, target + straight.astype(jnp.int32), line),
            device_id_type=MESH,
        ).start()

    def gather_if(wanted, there):
        @pl.when(wanted)
        def _():
            gather(there)

    loads = [
        pltpu.make_async_copy(src, dst, load_sem.at[i])
        for i, (src, dst) in enumerate(
            ((vis_hbm, vis), (dest_hbm, dest), (slot_hbm, slot), (off_hbm, off), (taper_hbm, taper))
        )
    ]
    for load in loads:
        load.start()
    barrier = pltpu.get_barrier_semaphore()
    for there in range(1, RING):
        signal_if(barrier, ((half == 0) & (z < there)) | (after_exists & (there == after)), ring_peer(there))
    signal_if(barrier, (half == 0) & (core == 1), (0, 3, vert))
    pl.when(is_hub)(lambda: greet_plane(barrier))

    for load in loads[:4]:
        load.wait()
    target, tile = dest[...], slot[...]
    row0 = target // 16 * ROWS_DEV + tile // 4 * TILE + off[0:1, :]
    col0 = target % 16 * COLS_DEV + tile % 4 * TILE + off[1:2, :]
    fields[z, 0:2, :] = vis[...]
    fields[z, 2:3, :] = (row0 - CELLS // 2).astype(jnp.float32)
    fields[z, 3:4, :] = (col0 - CELLS // 2).astype(jnp.float32)

    lower = jnp.where(half == 0, z, 4 + before_exists.astype(jnp.int32) + jnp.where(turned, 4, 0))
    wait_if(barrier, lower + jnp.where(is_hub, 0, 1))
    def below(there):
        return ((there < z) & ((half == 0) | (there < 4))) | (before_exists & (there == before))

    for there in range(RING):
        gather_if(below(there), there)
    for there in range(RING):
        signal_if(ready.at[jnp.where(there // 4 == half, 0, 1)], below(there), ring_peer(there))
    signal_if(here, jnp.logical_not(is_hub), hub)

    position = grp * 2 + half
    first_pixel = (position * ROWS - HALF).astype(jnp.float32)

    def project(buffer, first=False):
        v, w = v_ref.at[buffer], w_ref.at[buffer]

        def product(a, b):
            return lax.dot_general(a, b, (((1,), (1,)), ((), ())), preferred_element_type=jnp.float32)

        both, cross = product(w[...], v[0]), product(w[0 : 4 * ROWS, :], v[1])
        if first:
            acc[0 : 8 * ROWS, :] = both
            acc[8 * ROWS :, :] = cross
        else:
            acc[0 : 8 * ROWS, :] += both
            acc[8 * ROWS :, :] += cross

    phases(fields.at[z], first_pixel, v_ref.at[0], w_ref.at[0])
    loads[4].wait()
    taps = [taper[i] for i in range(SUP)]
    lane, level = lanes_of((8, 128)), rows_of((8, 128))
    line_row = rows_of((ROWS, 128))
    line = taper_sum(taps, first_pixel + (2 * (line_row % 32) + line_row // 32).astype(jnp.float32))
    centre = CENTRE * (2 * (level % 2) - 1)
    columns = taper_sum(taps, centre + jnp.where(level < 2, lane, -1 - lane).astype(jnp.float32))
    norm = 1.0 / (SUP * math.sqrt(65536))
    for i in range(4):
        pair_re, pair_im = times(line, (columns[0][i : i + 1, :] * norm, columns[1][i : i + 1, :] * norm))
        tt[i, 0] = pair_re
        tt[i, 1] = pair_im
    @pl.when(half == 0)
    def _():
        wait_if(ready.at[0], 3 - grp)
        for there in range(1, 4):
            gather_if(there > z, there)

    @pl.when(half == 1)
    def _():
        wait_if(ready.at[0], after_exists.astype(jnp.int32))
        sides = [(grp + step >= 0) & (grp + step < 4) for step in (1, -1)]
        for there in range(4, RING):
            gather_if(after_exists & (there == after), there)
        for distance in (2, 3):
            for step, side in zip((1, -1), sides):
                signal_if(chain.at[distance - 2], side, ((grp + step) % 4, au, vert))
            pl.semaphore_wait(chain.at[distance - 2], sum(side.astype(jnp.int32) for side in sides))
            for there in range(4, RING):
                gather_if((there == z + distance) | (there == z - distance), there)

    @pl.when(is_hub)
    def _():
        pl.semaphore_wait(here, OWN - 1)
        greet_plane(everyone)

    count = jnp.where(half == 1, 7, jnp.where(core == 1, 8, 6))

    def take(index):
        source = 0
        for place, order in enumerate(ORDER):
            if index <= len(order):
                source = jnp.where(z + RING * core == place, order[index - 1], source)
        pltpu.make_async_remote_copy(
            src_ref=fields.at[source],
            dst_ref=fields.at[source],
            send_sem=a_send,
            recv_sem=a_recv.at[source],
            device_id=pair,
            device_id_type=MESH,
        ).wait_recv()
        project((index - 1) % 2, index == 1)
        phases(fields.at[source], first_pixel, v_ref.at[index % 2], w_ref.at[index % 2])

    for index in range(1, RING + 1):
        if index == 3:

            @pl.when(half == 0)
            def _():
                pl.semaphore_wait(ready.at[1], 4)
                for there in range(4, RING):
                    gather(there)

        if index < 7:
            take(index)
        else:
            pl.when(count >= index)(lambda: take(index))

    project(count % 2)
    for c in range(2):
        re_cos, re_sin, im_cos, im_sin = (
            sum(acc[first + 4 * ROWS * i : first + 4 * ROWS * i + ROWS, place : place + 128] for i in range(3))
            for first in (128 * c, 128 * c + ROWS)
            for place in (0, 128)
        )
        sides = (re_cos - im_sin, im_cos + re_sin), (re_cos + im_sin, im_cos - re_sin)
        for side, (real, imag) in enumerate(sides):
            facet = tt[2 * side + c, 0] * real - tt[2 * side + c, 1] * imag
            for e in range(2):
                for t in range(4):
                    sends[pl.ds(64 * t + 4 * side + 2 * e + c, 8, stride=8), :] = facet[
                        32 * e + 8 * t : 32 * e + 8 * t + 8, :
                    ]

    wait_if(everyone, jnp.where(is_hub, 0, 1))
    mine = core * 16 + vert
    for place in sorted(range(OWN), key=early):
        there = grp, half * 2 + place // 16, place % 16

        @pl.when(mine != place)
        def _():
            pltpu.make_async_remote_copy(
                src_ref=sends.at[pl.ds(8 * place, 8), :],
                dst_ref=recvs.at[mine],
                send_sem=b_send,
                recv_sem=b_recv,
                device_id=there,
                device_id_type=MESH,
            ).start()

    recvs[mine] = sends[pl.ds(pl.multiple_of(8 * mine, 8), 8), :]
    others = recvs.at[pl.ds(1, OWN - 1)]
    batch = pltpu.make_async_remote_copy(
        src_ref=others, dst_ref=others, send_sem=b_send, recv_sem=b_recv, device_id=pair, device_id_type=MESH
    )
    batch.wait_recv()
    total = recvs[0]
    for i in range(1, OWN):
        total = total + recvs[i]
    mirrored = jnp.take_along_axis(total, 127 - lane, axis=1)
    for e in range(2):
        for c in range(2):
            out_ref[e : e + 1, 256 * c + 128 : 256 * c + 256] = total[2 * e + c : 2 * e + c + 1, :]
            out_ref[e : e + 1, 256 * c : 256 * c + 128] = mirrored[4 + 2 * e + c : 5 + 2 * e + c, :]
    batch.wait_send()
    rest = fields.at[pl.ds(1, RING - 1)]
    pltpu.make_async_remote_copy(
        src_ref=rest, dst_ref=rest, send_sem=a_send, recv_sem=a_recv.at[0], device_id=pair, device_id_type=MESH
    ).wait_send()


def body(visibility, destination, tile_slot, offsets, taper):
    any_space = pl.BlockSpec(memory_space=pl.ANY)
    return pl.pallas_call(
        kernel,
        out_shape=pltpu.VMEM((2, IMG), jnp.float32),
        in_specs=[any_space] * 5,
        out_specs=pl.BlockSpec(memory_space=pltpu.VMEM),
        scratch_shapes=[
            pltpu.VMEM((2, VIS), jnp.float32),
            pltpu.VMEM((1, VIS), jnp.int32),
            pltpu.VMEM((1, VIS), jnp.int32),
            pltpu.VMEM((2, VIS), jnp.int32),
            pltpu.SMEM((SUP,), jnp.float32),
            pltpu.VMEM((RING + 1, 4, VIS), jnp.float32),
            pltpu.VMEM((2, 2, 2 * CENTRE, VIS), jnp.bfloat16),
            pltpu.VMEM((2, 8 * ROWS, VIS), jnp.bfloat16),
            pltpu.VMEM((12 * ROWS, 2 * CENTRE), jnp.float32),
            pltpu.VMEM((4, 2, ROWS, 128), jnp.float32),
            pltpu.VMEM((OWN * 8, 128), jnp.float32),
            pltpu.VMEM((OWN, 8, 128), jnp.float32),
            pltpu.SemaphoreType.DMA((5,)),
            pltpu.SemaphoreType.DMA,
            pltpu.SemaphoreType.DMA((RING + 1,)),
            pltpu.SemaphoreType.DMA,
            pltpu.SemaphoreType.DMA,
            pltpu.SemaphoreType.REGULAR((2,)),
            pltpu.SemaphoreType.REGULAR((2,)),
            pltpu.SemaphoreType.REGULAR,
            pltpu.SemaphoreType.REGULAR,
        ],
        compiler_params=pltpu.CompilerParams(collective_id=0, has_side_effects=True),
    )(visibility.T, destination.T, tile_slot.reshape(1, -1), offsets.T, taper)


def solution(mesh):
    return jax.shard_map(
        body,
        mesh=mesh,
        in_specs=(
            P(("grp", "au", "vert"), None),
            P(("grp", "au", "vert"), None),
            P(("grp", "au", "vert")),
            P(("grp", "au", "vert"), None),
            P(),
        ),
        out_specs=P(("grp", "au", "vert"), None),
        check_vma=False,
    )
```

```python
import math

import jax
import jax.numpy as jnp
from jax import lax
from jax.experimental import pallas as pl
from jax.experimental.pallas import tpu as pltpu
from jax.sharding import PartitionSpec as P

TILE = 128
SUP = 8
ROWS_DEV = 2048
COLS_DEV = 512
IMG = 512
CELLS = 8192
MESH = pl.DeviceIdType.MESH

RING = 8
OWN = 32
ROWS = 64
HALF = IMG // 2
CENTRE = IMG // 4
VIS = 256

ORDER = (
    (1, 2, 3, 6, 5, 7),
    (2, 3, 0, 7, 6, 5),
    (3, 1, 0, 5, 7, 6),
    (2, 1, 0, 5, 6, 7),
    (5, 6, 3, 2, 7, 1, 0),
    (4, 6, 7, 3, 0, 2, 1),
    (5, 7, 4, 0, 3, 1, 2),
    (6, 5, 0, 1, 4, 2, 3),
    (1, 2, 3, 7, 6, 8, 5, 4),
    (2, 3, 0, 7, 8, 6, 4, 5),
    (3, 1, 0, 8, 4, 5, 7, 6),
    (2, 1, 0, 8, 4, 5, 6, 7),
    (5, 6, 3, 2, 7, 1, 0),
    (4, 6, 7, 3, 0, 2, 1),
    (5, 7, 4, 0, 3, 1, 2),
    (6, 5, 0, 1, 4, 2, 3),
)


def sincos(turns):
    turns = turns - jnp.floor(turns + 0.5)
    square = turns * turns
    sine = jnp.full_like(turns, -(math.pi**11) / math.factorial(11))
    for order in (9, 7, 5, 3, 1):
        sign = 1.0 if order % 4 == 1 else -1.0
        sine = sine * square + sign * math.pi**order / math.factorial(order)
    sine = sine * turns
    cosine = jnp.full_like(turns, math.pi**12 / math.factorial(12))
    for order in (10, 8, 6, 4, 2, 0):
        sign = 1.0 if order % 4 == 0 else -1.0
        cosine = cosine * square + sign * math.pi**order / math.factorial(order)
    return 1.0 - 2.0 * sine * sine, 2.0 * sine * cosine


def times(a, b):
    return a[0] * b[0] - a[1] * b[1], a[0] * b[1] + a[1] * b[0]


def stack(a, b):
    return jnp.concatenate([a[0], b[0]], axis=0), jnp.concatenate([a[1], b[1]], axis=0)


def split(value):
    high = value.astype(jnp.bfloat16)
    return high, (value - high.astype(jnp.float32)).astype(jnp.bfloat16)


def taper_sum(taper, pixel):
    step = sincos(pixel * (1.0 / CELLS))
    total = (jnp.full_like(pixel, taper[SUP - 1]), jnp.zeros_like(pixel))
    for tap in range(SUP - 2, -1, -1):
        re, im = times(total, step)
        total = (re + taper[tap], im)
    return total


def rows_of(shape):
    return lax.broadcasted_iota(jnp.int32, shape, 0)


def lanes_of(shape):
    return lax.broadcasted_iota(jnp.int32, shape, 1)


def phases(fields, first_pixel, v_ref, w_ref):
    unit = 1.0 / CELLS
    row = rows_of((8, 128))

    def v_at(part, place):
        return v_ref.at[part, pl.ds(place, 16), :]

    def w_at(part, place):
        return w_ref.at[pl.ds(4 * ROWS * part + place, 16), :]

    rowf = row.astype(jnp.float32)
    power = jnp.where(row < 2, 8 << jnp.minimum(row, 1), jnp.where(row == 2, CENTRE, 16 << jnp.maximum(row - 3, 0)))
    power = jnp.where(row == 5, 1, power).astype(jnp.float32) * unit
    for lane in range(0, VIS, 128):
        re, im, x, y = (fields[i : i + 1, lane : lane + 128] for i in range(4))
        col = sincos((rowf + 0.5) * (y * unit))
        line = sincos(((first_pixel + 2.0 * rowf) * x - 0.5 * y) * unit)
        turn = sincos(power * jnp.where(row < 3, y, x))
        steps = [(turn[0][i : i + 1, :], turn[1][i : i + 1, :]) for i in range(6)]

        def store(ref, place, value):
            high, low = split(value)
            ref(0, place)[:, lane : lane + 128] = high
            ref(1, place)[:, lane : lane + 128] = low

        line = times((re, im), line)
        tiles = [stack(line, times(line, steps[3]))]
        tiles.append(times(tiles[0], steps[4]))
        tiles += [times(tile, steps[5]) for tile in tiles]
        for i, tile in enumerate(tiles):
            rr, ii, ri, ir = (tile[a] * steps[2][b] for a, b in ((0, 0), (1, 1), (0, 1), (1, 0)))
            for place, value in ((0, rr + ii), (64, ir - ri), (128, rr - ii), (192, ri + ir)):
                store(w_at, place + 16 * i, value)
        tile = stack(col, times(col, steps[0]))
        for i in range(CENTRE // 16):
            store(v_at, 16 * i, tile[0])
            store(v_at, CENTRE + 16 * i, tile[1])
            tile = times(tile, steps[1])


def early(place):
    core, y, x = place // 16, place // 4 % 4, place % 4
    return min(y, 4 - y) + min(x, 4 - x) + 0.5 * (1 - core) + (2 if place == 0 else 0)


def kernel(
    vis_hbm, dest_hbm, slot_hbm, off_hbm, taper_hbm, out_ref,
    vis, dest, slot, off, taper, fields, v_ref, w_ref, acc, tt, sends, recvs,
    load_sem, a_send, a_recv, b_send, b_recv, ready, chain, here, everyone,
):
    grp, au, vert = lax.axis_index("grp"), lax.axis_index("au"), lax.axis_index("vert")
    core, half = au % 2, au // 2
    z = half * 4 + grp
    y, x = vert // 4, vert % 4

    shifts = [(c, b, a) for c in range(2) for b in range(4) for a in range(4)]
    shifts.sort(key=lambda s: -(min(s[1], 4 - s[1]) + min(s[2], 4 - s[2]) + 0.5 * s[0]))
    shifts = shifts[:-1]

    def own_vert(shift):
        return ((y + shift[1]) % 4) * 4 + (x + shift[2]) % 4

    def own_peer(shift):
        return grp, half * 2 + (core + shift[0]) % 2, own_vert(shift)

    def signal(sem, peer):
        pl.semaphore_signal(sem, inc=1, device_id=peer, device_id_type=MESH)

    def ring_peer(there):
        other = (there // 4 + half) % 2
        return there % 4, there // 4 * 2 + (core + other) % 2, vert

    pair = own_peer((1, 0, 0))
    hub = grp, half * 2 + 1, 0
    is_hub = (core == 1) & (vert == 0)

    def greet_plane(sem):
        for shift in shifts:
            signal(sem, own_peer(shift))

    step = 1 - 2 * core
    before, after = z - step, z + step
    before_exists = (half == 1) & (before >= 4) & (before < RING)
    after_exists = (half == 1) & (after >= 4) & (after < RING)

    def signal_if(sem, wanted, peer):
        @pl.when(wanted)
        def _():
            signal(sem, peer)

    def wait_if(sem, count):
        @pl.when(count > 0)
        def _():
            pl.semaphore_wait(sem, count)

    turned = (z == 4) & (core == 1)

    def gather(there):
        straight = turned & (there < 4)
        place, target, line = ring_peer(there)
        slot_there = jnp.where(straight, RING, z)
        pltpu.make_async_remote_copy(
            src_ref=fields.at[z],
            dst_ref=fields.at[slot_there],
            send_sem=a_send,
            recv_sem=a_recv.at[slot_there],
            device_id=(place, target + straight.astype(jnp.int32), line),
            device_id_type=MESH,
        ).start()

    def gather_if(wanted, there):
        @pl.when(wanted)
        def _():
            gather(there)

    loads = [
        pltpu.make_async_copy(src, dst, load_sem.at[i])
        for i, (src, dst) in enumerate(
            ((vis_hbm, vis), (dest_hbm, dest), (slot_hbm, slot), (off_hbm, off), (taper_hbm, taper))
        )
    ]
    for load in loads:
        load.start()
    barrier = pltpu.get_barrier_semaphore()
    for there in range(1, RING):
        signal_if(barrier, ((half == 0) & (z < there)) | (after_exists & (there == after)), ring_peer(there))
    signal_if(barrier, (half == 0) & (core == 1), (0, 3, vert))
    pl.when(is_hub)(lambda: greet_plane(barrier))

    for load in loads[:4]:
        load.wait()
    target, tile = dest[...], slot[...]
    row0 = target // 16 * ROWS_DEV + tile // 4 * TILE + off[0:1, :]
    col0 = target % 16 * COLS_DEV + tile % 4 * TILE + off[1:2, :]
    fields[z, 0:2, :] = vis[...]
    fields[z, 2:3, :] = (row0 - CELLS // 2).astype(jnp.float32)
    fields[z, 3:4, :] = (col0 - CELLS // 2).astype(jnp.float32)

    lower = jnp.where(half == 0, z, 4 + before_exists.astype(jnp.int32) + jnp.where(turned, 4, 0))
    wait_if(barrier, lower + jnp.where(is_hub, 0, 1))
    def below(there):
        return ((there < z) & ((half == 0) | (there < 4))) | (before_exists & (there == before))

    for there in range(RING):
        gather_if(below(there), there)
    for there in range(RING):
        signal_if(ready.at[jnp.where(there // 4 == half, 0, 1)], below(there), ring_peer(there))
    signal_if(here, jnp.logical_not(is_hub), hub)

    position = grp * 2 + half
    first_pixel = (position * ROWS - HALF).astype(jnp.float32)

    def project(buffer, first=False):
        v, w = v_ref.at[buffer], w_ref.at[buffer]

        def product(a, b):
            return lax.dot_general(a, b, (((1,), (1,)), ((), ())), preferred_element_type=jnp.float32)

        both, cross = product(w[...], v[0]), product(w[0 : 4 * ROWS, :], v[1])
        if first:
            acc[0 : 8 * ROWS, :] = both
            acc[8 * ROWS :, :] = cross
        else:
            acc[0 : 8 * ROWS, :] += both
            acc[8 * ROWS :, :] += cross

    phases(fields.at[z], first_pixel, v_ref.at[0], w_ref.at[0])
    loads[4].wait()
    taps = [taper[i] for i in range(SUP)]
    lane, level = lanes_of((8, 128)), rows_of((8, 128))
    line_row = rows_of((ROWS, 128))
    line = taper_sum(taps, first_pixel + (2 * (line_row % 32) + line_row // 32).astype(jnp.float32))
    centre = CENTRE * (2 * (level % 2) - 1)
    columns = taper_sum(taps, centre + jnp.where(level < 2, lane, -1 - lane).astype(jnp.float32))
    norm = 1.0 / (SUP * math.sqrt(65536))
    for i in range(4):
        pair_re, pair_im = times(line, (columns[0][i : i + 1, :] * norm, columns[1][i : i + 1, :] * norm))
        tt[i, 0] = pair_re
        tt[i, 1] = pair_im
    @pl.when(half == 0)
    def _():
        wait_if(ready.at[0], 3 - grp)
        for there in range(1, 4):
            gather_if(there > z, there)

    @pl.when(half == 1)
    def _():
        wait_if(ready.at[0], after_exists.astype(jnp.int32))
        sides = [(grp + step >= 0) & (grp + step < 4) for step in (1, -1)]
        for there in range(4, RING):
            gather_if(after_exists & (there == after), there)
        for distance in (2, 3):
            for step, side in zip((1, -1), sides):
                signal_if(chain.at[distance - 2], side, ((grp + step) % 4, au, vert))
            pl.semaphore_wait(chain.at[distance - 2], sum(side.astype(jnp.int32) for side in sides))
            for there in range(4, RING):
                gather_if((there == z + distance) | (there == z - distance), there)

    @pl.when(is_hub)
    def _():
        pl.semaphore_wait(here, OWN - 1)
        greet_plane(everyone)

    def take(index):
        source = 0
        for place, order in enumerate(ORDER):
            if index <= len(order):
                source = jnp.where(z + RING * core == place, order[index - 1], source)
        pltpu.make_async_remote_copy(
            src_ref=fields.at[source],
            dst_ref=fields.at[source],
            send_sem=a_send,
            recv_sem=a_recv.at[source],
            device_id=pair,
            device_id_type=MESH,
        ).wait_recv()
        project((index - 1) % 2, index == 1)
        phases(fields.at[source], first_pixel, v_ref.at[index % 2], w_ref.at[index % 2])

    def rest_of(count):
        for index in range(4, count + 1):
            take(index)
        project(count % 2)

    for index in range(1, 4):
        if index == 3:

            @pl.when(half == 0)
            def _():
                pl.semaphore_wait(ready.at[1], 4)
                for there in range(4, RING):
                    gather(there)

        take(index)
    pl.when((half == 0) & (core == 0))(lambda: rest_of(6))
    pl.when(half == 1)(lambda: rest_of(7))
    pl.when((half == 0) & (core == 1))(lambda: rest_of(8))
    for c in range(2):
        re_cos, re_sin, im_cos, im_sin = (
            sum(acc[first + 4 * ROWS * i : first + 4 * ROWS * i + ROWS, place : place + 128] for i in range(3))
            for first in (128 * c, 128 * c + ROWS)
            for place in (0, 128)
        )
        sides = (re_cos - im_sin, im_cos + re_sin), (re_cos + im_sin, im_cos - re_sin)
        for side, (real, imag) in enumerate(sides):
            facet = tt[2 * side + c, 0] * real - tt[2 * side + c, 1] * imag
            for e in range(2):
                for t in range(4):
                    sends[pl.ds(64 * t + 4 * side + 2 * e + c, 8, stride=8), :] = facet[
                        32 * e + 8 * t : 32 * e + 8 * t + 8, :
                    ]

    wait_if(everyone, jnp.where(is_hub, 0, 1))
    mine = core * 16 + vert
    for place in sorted(range(OWN), key=early):
        there = grp, half * 2 + place // 16, place % 16

        @pl.when(mine != place)
        def _():
            pltpu.make_async_remote_copy(
                src_ref=sends.at[pl.ds(8 * place, 8), :],
                dst_ref=recvs.at[mine],
                send_sem=b_send,
                recv_sem=b_recv,
                device_id=there,
                device_id_type=MESH,
            ).start()

    recvs[mine] = sends[pl.ds(pl.multiple_of(8 * mine, 8), 8), :]
    others = recvs.at[pl.ds(1, OWN - 1)]
    batch = pltpu.make_async_remote_copy(
        src_ref=others, dst_ref=others, send_sem=b_send, recv_sem=b_recv, device_id=pair, device_id_type=MESH
    )
    batch.wait_recv()
    total = recvs[0]
    for i in range(1, OWN):
        total = total + recvs[i]
    mirrored = jnp.take_along_axis(total, 127 - lane, axis=1)
    for e in range(2):
        for c in range(2):
            out_ref[e : e + 1, 256 * c + 128 : 256 * c + 256] = total[2 * e + c : 2 * e + c + 1, :]
            out_ref[e : e + 1, 256 * c : 256 * c + 128] = mirrored[4 + 2 * e + c : 5 + 2 * e + c, :]
    batch.wait_send()
    rest = fields.at[pl.ds(1, RING - 1)]
    pltpu.make_async_remote_copy(
        src_ref=rest, dst_ref=rest, send_sem=a_send, recv_sem=a_recv.at[0], device_id=pair, device_id_type=MESH
    ).wait_send()


def body(visibility, destination, tile_slot, offsets, taper):
    any_space = pl.BlockSpec(memory_space=pl.ANY)
    return pl.pallas_call(
        kernel,
        out_shape=pltpu.VMEM((2, IMG), jnp.float32),
        in_specs=[any_space] * 5,
        out_specs=pl.BlockSpec(memory_space=pltpu.VMEM),
        scratch_shapes=[
            pltpu.VMEM((2, VIS), jnp.float32),
            pltpu.VMEM((1, VIS), jnp.int32),
            pltpu.VMEM((1, VIS), jnp.int32),
            pltpu.VMEM((2, VIS), jnp.int32),
            pltpu.SMEM((SUP,), jnp.float32),
            pltpu.VMEM((RING + 1, 4, VIS), jnp.float32),
            pltpu.VMEM((2, 2, 2 * CENTRE, VIS), jnp.bfloat16),
            pltpu.VMEM((2, 8 * ROWS, VIS), jnp.bfloat16),
            pltpu.VMEM((12 * ROWS, 2 * CENTRE), jnp.float32),
            pltpu.VMEM((4, 2, ROWS, 128), jnp.float32),
            pltpu.VMEM((OWN * 8, 128), jnp.float32),
            pltpu.VMEM((OWN, 8, 128), jnp.float32),
            pltpu.SemaphoreType.DMA((5,)),
            pltpu.SemaphoreType.DMA,
            pltpu.SemaphoreType.DMA((RING + 1,)),
            pltpu.SemaphoreType.DMA,
            pltpu.SemaphoreType.DMA,
            pltpu.SemaphoreType.REGULAR((2,)),
            pltpu.SemaphoreType.REGULAR((2,)),
            pltpu.SemaphoreType.REGULAR,
            pltpu.SemaphoreType.REGULAR,
        ],
        compiler_params=pltpu.CompilerParams(collective_id=0, has_side_effects=True),
    )(visibility.T, destination.T, tile_slot.reshape(1, -1), offsets.T, taper)


def solution(mesh):
    return jax.shard_map(
        body,
        mesh=mesh,
        in_specs=(
            P(("grp", "au", "vert"), None),
            P(("grp", "au", "vert"), None),
            P(("grp", "au", "vert")),
            P(("grp", "au", "vert"), None),
            P(),
        ),
        out_specs=P(("grp", "au", "vert"), None),
        check_vma=False,
    )
```

```python
import math

import jax
import jax.numpy as jnp
from jax import lax
from jax.experimental import pallas as pl
from jax.experimental.pallas import tpu as pltpu
from jax.sharding import PartitionSpec as P

TILE = 128
SUP = 8
ROWS_DEV = 2048
COLS_DEV = 512
IMG = 512
CELLS = 8192
MESH = pl.DeviceIdType.MESH

RING = 8
OWN = 32
ROWS = 64
HALF = IMG // 2
CENTRE = IMG // 4
VIS = 256

ORDER = (
    (1, 2, 3, 6, 5, 7),
    (2, 3, 0, 7, 6, 5),
    (3, 1, 0, 5, 7, 6),
    (2, 1, 0, 5, 6, 7),
    (5, 6, 3, 2, 7, 1, 0),
    (4, 6, 7, 3, 0, 2, 1),
    (5, 7, 4, 0, 3, 1, 2),
    (6, 5, 0, 1, 4, 2, 3),
    (1, 2, 3, 7, 6, 8, 5, 4),
    (2, 3, 0, 7, 8, 6, 4, 5),
    (3, 1, 0, 8, 4, 5, 7, 6),
    (2, 1, 0, 8, 4, 5, 6, 7),
    (5, 6, 3, 2, 7, 1, 0),
    (4, 6, 7, 3, 0, 2, 1),
    (5, 7, 4, 0, 3, 1, 2),
    (6, 5, 0, 1, 4, 2, 3),
)


def sincos(turns):
    turns = turns - jnp.floor(turns + 0.5)
    square = turns * turns
    sine = jnp.full_like(turns, -(math.pi**11) / math.factorial(11))
    for order in (9, 7, 5, 3, 1):
        sign = 1.0 if order % 4 == 1 else -1.0
        sine = sine * square + sign * math.pi**order / math.factorial(order)
    sine = sine * turns
    cosine = jnp.full_like(turns, math.pi**12 / math.factorial(12))
    for order in (10, 8, 6, 4, 2, 0):
        sign = 1.0 if order % 4 == 0 else -1.0
        cosine = cosine * square + sign * math.pi**order / math.factorial(order)
    return 1.0 - 2.0 * sine * sine, 2.0 * sine * cosine


def times(a, b):
    return a[0] * b[0] - a[1] * b[1], a[0] * b[1] + a[1] * b[0]


def stack(a, b):
    return jnp.concatenate([a[0], b[0]], axis=0), jnp.concatenate([a[1], b[1]], axis=0)


def split(value):
    high = value.astype(jnp.bfloat16)
    return high, (value - high.astype(jnp.float32)).astype(jnp.bfloat16)


def taper_sum(taper, pixel):
    step = sincos(pixel * (1.0 / CELLS))
    total = (jnp.full_like(pixel, taper[SUP - 1]), jnp.zeros_like(pixel))
    for tap in range(SUP - 2, -1, -1):
        re, im = times(total, step)
        total = (re + taper[tap], im)
    return total


def rows_of(shape):
    return lax.broadcasted_iota(jnp.int32, shape, 0)


def lanes_of(shape):
    return lax.broadcasted_iota(jnp.int32, shape, 1)


def phases(fields, first_pixel, v_ref, w_ref):
    unit = 1.0 / CELLS
    row = rows_of((8, 128))

    def v_at(part, place):
        return v_ref.at[part, pl.ds(place, 16), :]

    def w_at(part, place):
        return w_ref.at[pl.ds(4 * ROWS * part + place, 16), :]

    rowf = row.astype(jnp.float32)
    power = jnp.where(row < 2, 8 << jnp.minimum(row, 1), jnp.where(row == 2, CENTRE, 16 << jnp.maximum(row - 3, 0)))
    power = jnp.where(row == 5, 1, power).astype(jnp.float32) * unit
    for lane in range(0, VIS, 128):
        re, im, x, y = (fields[i : i + 1, lane : lane + 128] for i in range(4))
        col = sincos((rowf + 0.5) * (y * unit))
        line = sincos(((first_pixel + 2.0 * rowf) * x - 0.5 * y) * unit)
        turn = sincos(power * jnp.where(row < 3, y, x))
        steps = [(turn[0][i : i + 1, :], turn[1][i : i + 1, :]) for i in range(6)]

        def store(ref, place, value):
            high, low = split(value)
            ref(0, place)[:, lane : lane + 128] = high
            ref(1, place)[:, lane : lane + 128] = low

        line = times((re, im), line)
        tiles = [stack(line, times(line, steps[3]))]
        tiles.append(times(tiles[0], steps[4]))
        tiles += [times(tile, steps[5]) for tile in tiles]
        for i, tile in enumerate(tiles):
            rr, ii, ri, ir = (tile[a] * steps[2][b] for a, b in ((0, 0), (1, 1), (0, 1), (1, 0)))
            for place, value in ((0, rr + ii), (64, ir - ri), (128, rr - ii), (192, ri + ir)):
                store(w_at, place + 16 * i, value)
        tile = stack(col, times(col, steps[0]))
        for i in range(CENTRE // 16):
            store(v_at, 16 * i, tile[0])
            store(v_at, CENTRE + 16 * i, tile[1])
            tile = times(tile, steps[1])


def early(place):
    core, y, x = place // 16, place // 4 % 4, place % 4
    return min(y, 4 - y) + min(x, 4 - x) + 0.5 * (1 - core) + (2 if place == 0 else 0)


def kernel(
    vis_hbm, dest_hbm, slot_hbm, off_hbm, taper_hbm, out_ref,
    vis, dest, slot, off, taper, fields, v_ref, w_ref, acc, tt, sends, recvs,
    load_sem, a_send, a_recv, b_send, b_recv, ready, chain, here, everyone,
):
    grp, au, vert = lax.axis_index("grp"), lax.axis_index("au"), lax.axis_index("vert")
    core, half = au % 2, au // 2
    z = half * 4 + grp
    y, x = vert // 4, vert % 4

    shifts = [(c, b, a) for c in range(2) for b in range(4) for a in range(4)]
    shifts.sort(key=lambda s: -(min(s[1], 4 - s[1]) + min(s[2], 4 - s[2]) + 0.5 * s[0]))
    shifts = shifts[:-1]

    def own_vert(shift):
        return ((y + shift[1]) % 4) * 4 + (x + shift[2]) % 4

    def own_peer(shift):
        return grp, half * 2 + (core + shift[0]) % 2, own_vert(shift)

    def signal(sem, peer):
        pl.semaphore_signal(sem, inc=1, device_id=peer, device_id_type=MESH)

    def ring_peer(there):
        other = (there // 4 + half) % 2
        return there % 4, there // 4 * 2 + (core + other) % 2, vert

    pair = own_peer((1, 0, 0))
    hub = grp, half * 2 + 1, 0
    is_hub = (core == 1) & (vert == 0)

    def greet_plane(sem):
        for shift in shifts:
            signal(sem, own_peer(shift))

    step = 1 - 2 * core
    before, after = z - step, z + step
    before_exists = (half == 1) & (before >= 4) & (before < RING)
    after_exists = (half == 1) & (after >= 4) & (after < RING)

    def signal_if(sem, wanted, peer):
        @pl.when(wanted)
        def _():
            signal(sem, peer)

    def wait_if(sem, count):
        @pl.when(count > 0)
        def _():
            pl.semaphore_wait(sem, count)

    turned = (z == 4) & (core == 1)

    def gather(there):
        straight = turned & (there < 4)
        place, target, line = ring_peer(there)
        slot_there = jnp.where(straight, RING, z)
        pltpu.make_async_remote_copy(
            src_ref=fields.at[z],
            dst_ref=fields.at[slot_there],
            send_sem=a_send,
            recv_sem=a_recv.at[slot_there],
            device_id=(place, target + straight.astype(jnp.int32), line),
            device_id_type=MESH,
        ).start()

    def gather_if(wanted, there):
        @pl.when(wanted)
        def _():
            gather(there)

    loads = [
        pltpu.make_async_copy(src, dst, load_sem.at[i])
        for i, (src, dst) in enumerate(
            ((vis_hbm, vis), (dest_hbm, dest), (slot_hbm, slot), (off_hbm, off), (taper_hbm, taper))
        )
    ]
    for load in loads:
        load.start()
    barrier = pltpu.get_barrier_semaphore()
    for there in range(1, RING):
        signal_if(barrier, ((half == 0) & (z < there)) | (after_exists & (there == after)), ring_peer(there))
    signal_if(barrier, (half == 0) & (core == 1), (0, 3, vert))
    pl.when(is_hub)(lambda: greet_plane(barrier))

    for load in loads[:4]:
        load.wait()
    target, tile = dest[...], slot[...]
    row0 = target // 16 * ROWS_DEV + tile // 4 * TILE + off[0:1, :]
    col0 = target % 16 * COLS_DEV + tile % 4 * TILE + off[1:2, :]
    fields[z, 0:2, :] = vis[...]
    fields[z, 2:3, :] = (row0 - CELLS // 2).astype(jnp.float32)
    fields[z, 3:4, :] = (col0 - CELLS // 2).astype(jnp.float32)

    lower = jnp.where(half == 0, z, 4 + before_exists.astype(jnp.int32) + jnp.where(turned, 4, 0))
    wait_if(barrier, lower + jnp.where(is_hub, 0, 1))
    def below(there):
        return ((there < z) & ((half == 0) | (there < 4))) | (before_exists & (there == before))

    for there in range(RING):
        gather_if(below(there), there)
    for there in range(RING):
        signal_if(ready.at[jnp.where(there // 4 == half, 0, 1)], below(there), ring_peer(there))
    signal_if(here, jnp.logical_not(is_hub), hub)

    position = grp * 2 + half
    first_pixel = (position * ROWS - HALF).astype(jnp.float32)

    def project(buffer, first=False):
        v, w = v_ref.at[buffer], w_ref.at[buffer]

        def product(a, b):
            return lax.dot_general(a, b, (((1,), (1,)), ((), ())), preferred_element_type=jnp.float32)

        both, cross = product(w[...], v[0]), product(w[0 : 4 * ROWS, :], v[1])
        if first:
            acc[0 : 8 * ROWS, :] = both
            acc[8 * ROWS :, :] = cross
        else:
            acc[0 : 8 * ROWS, :] += both
            acc[8 * ROWS :, :] += cross

    phases(fields.at[z], first_pixel, v_ref.at[0], w_ref.at[0])
    loads[4].wait()
    taps = [taper[i] for i in range(SUP)]
    lane, level = lanes_of((8, 128)), rows_of((8, 128))
    line_row = rows_of((ROWS, 128))
    line = taper_sum(taps, first_pixel + (2 * (line_row % 32) + line_row // 32).astype(jnp.float32))
    centre = CENTRE * (2 * (level % 2) - 1)
    columns = taper_sum(taps, centre + jnp.where(level < 2, lane, -1 - lane).astype(jnp.float32))
    norm = 1.0 / (SUP * math.sqrt(65536))
    for i in range(4):
        pair_re, pair_im = times(line, (columns[0][i : i + 1, :] * norm, columns[1][i : i + 1, :] * norm))
        tt[i, 0] = pair_re
        tt[i, 1] = pair_im
    @pl.when(half == 0)
    def _():
        wait_if(ready.at[0], 3 - grp)
        for there in range(1, 4):
            gather_if(there > z, there)

    @pl.when(half == 1)
    def _():
        wait_if(ready.at[0], after_exists.astype(jnp.int32))
        sides = [(grp + step >= 0) & (grp + step < 4) for step in (1, -1)]
        for there in range(4, RING):
            gather_if(after_exists & (there == after), there)
        for distance in (2, 3):
            for step, side in zip((1, -1), sides):
                signal_if(chain.at[distance - 2], side, ((grp + step) % 4, au, vert))
            pl.semaphore_wait(chain.at[distance - 2], sum(side.astype(jnp.int32) for side in sides))
            for there in range(4, RING):
                gather_if((there == z + distance) | (there == z - distance), there)

    @pl.when(is_hub)
    def _():
        pl.semaphore_wait(here, OWN - 1)
        greet_plane(everyone)

    def take(index):
        source = 0
        for place, order in enumerate(ORDER):
            if index <= len(order):
                source = jnp.where(z + RING * core == place, order[index - 1], source)
        pltpu.make_async_remote_copy(
            src_ref=fields.at[source],
            dst_ref=fields.at[source],
            send_sem=a_send,
            recv_sem=a_recv.at[source],
            device_id=pair,
            device_id_type=MESH,
        ).wait_recv()
        project((index - 1) % 2, index == 1)
        phases(fields.at[source], first_pixel, v_ref.at[index % 2], w_ref.at[index % 2])

    def rest_of(count):
        for index in range(3, count + 1):
            if index == 3 and count != 7:
                pl.semaphore_wait(ready.at[1], 4)
                for there in range(4, RING):
                    gather(there)

            take(index)
        project(count % 2)

    for index in range(1, 3):
        take(index)
    pl.when((half == 0) & (core == 0))(lambda: rest_of(6))
    pl.when(half == 1)(lambda: rest_of(7))
    pl.when((half == 0) & (core == 1))(lambda: rest_of(8))
    for c in range(2):
        re_cos, re_sin, im_cos, im_sin = (
            sum(acc[first + 4 * ROWS * i : first + 4 * ROWS * i + ROWS, place : place + 128] for i in range(3))
            for first in (128 * c, 128 * c + ROWS)
            for place in (0, 128)
        )
        sides = (re_cos - im_sin, im_cos + re_sin), (re_cos + im_sin, im_cos - re_sin)
        for side, (real, imag) in enumerate(sides):
            facet = tt[2 * side + c, 0] * real - tt[2 * side + c, 1] * imag
            for e in range(2):
                for t in range(4):
                    sends[pl.ds(64 * t + 4 * side + 2 * e + c, 8, stride=8), :] = facet[
                        32 * e + 8 * t : 32 * e + 8 * t + 8, :
                    ]

    wait_if(everyone, jnp.where(is_hub, 0, 1))
    mine = core * 16 + vert
    for place in sorted(range(OWN), key=early):
        there = grp, half * 2 + place // 16, place % 16

        @pl.when(mine != place)
        def _():
            pltpu.make_async_remote_copy(
                src_ref=sends.at[pl.ds(8 * place, 8), :],
                dst_ref=recvs.at[mine],
                send_sem=b_send,
                recv_sem=b_recv,
                device_id=there,
                device_id_type=MESH,
            ).start()

    recvs[mine] = sends[pl.ds(pl.multiple_of(8 * mine, 8), 8), :]
    others = recvs.at[pl.ds(1, OWN - 1)]
    batch = pltpu.make_async_remote_copy(
        src_ref=others, dst_ref=others, send_sem=b_send, recv_sem=b_recv, device_id=pair, device_id_type=MESH
    )
    batch.wait_recv()
    total = recvs[0]
    for i in range(1, OWN):
        total = total + recvs[i]
    mirrored = jnp.take_along_axis(total, 127 - lane, axis=1)
    for e in range(2):
        for c in range(2):
            out_ref[e : e + 1, 256 * c + 128 : 256 * c + 256] = total[2 * e + c : 2 * e + c + 1, :]
            out_ref[e : e + 1, 256 * c : 256 * c + 128] = mirrored[4 + 2 * e + c : 5 + 2 * e + c, :]
    batch.wait_send()
    rest = fields.at[pl.ds(1, RING - 1)]
    pltpu.make_async_remote_copy(
        src_ref=rest, dst_ref=rest, send_sem=a_send, recv_sem=a_recv.at[0], device_id=pair, device_id_type=MESH
    ).wait_send()


def body(visibility, destination, tile_slot, offsets, taper):
    any_space = pl.BlockSpec(memory_space=pl.ANY)
    return pl.pallas_call(
        kernel,
        out_shape=pltpu.VMEM((2, IMG), jnp.float32),
        in_specs=[any_space] * 5,
        out_specs=pl.BlockSpec(memory_space=pltpu.VMEM),
        scratch_shapes=[
            pltpu.VMEM((2, VIS), jnp.float32),
            pltpu.VMEM((1, VIS), jnp.int32),
            pltpu.VMEM((1, VIS), jnp.int32),
            pltpu.VMEM((2, VIS), jnp.int32),
            pltpu.SMEM((SUP,), jnp.float32),
            pltpu.VMEM((RING + 1, 4, VIS), jnp.float32),
            pltpu.VMEM((2, 2, 2 * CENTRE, VIS), jnp.bfloat16),
            pltpu.VMEM((2, 8 * ROWS, VIS), jnp.bfloat16),
            pltpu.VMEM((12 * ROWS, 2 * CENTRE), jnp.float32),
            pltpu.VMEM((4, 2, ROWS, 128), jnp.float32),
            pltpu.VMEM((OWN * 8, 128), jnp.float32),
            pltpu.VMEM((OWN, 8, 128), jnp.float32),
            pltpu.SemaphoreType.DMA((5,)),
            pltpu.SemaphoreType.DMA,
            pltpu.SemaphoreType.DMA((RING + 1,)),
            pltpu.SemaphoreType.DMA,
            pltpu.SemaphoreType.DMA,
            pltpu.SemaphoreType.REGULAR((2,)),
            pltpu.SemaphoreType.REGULAR((2,)),
            pltpu.SemaphoreType.REGULAR,
            pltpu.SemaphoreType.REGULAR,
        ],
        compiler_params=pltpu.CompilerParams(collective_id=0, has_side_effects=True),
    )(visibility.T, destination.T, tile_slot.reshape(1, -1), offsets.T, taper)


def solution(mesh):
    return jax.shard_map(
        body,
        mesh=mesh,
        in_specs=(
            P(("grp", "au", "vert"), None),
            P(("grp", "au", "vert"), None),
            P(("grp", "au", "vert")),
            P(("grp", "au", "vert"), None),
            P(),
        ),
        out_specs=P(("grp", "au", "vert"), None),
        check_vma=False,
    )
```

```python
import math

import jax
import jax.numpy as jnp
from jax import lax
from jax.experimental import pallas as pl
from jax.experimental.pallas import tpu as pltpu
from jax.sharding import PartitionSpec as P

TILE = 128
SUP = 8
ROWS_DEV = 2048
COLS_DEV = 512
IMG = 512
CELLS = 8192
MESH = pl.DeviceIdType.MESH

RING = 8
OWN = 32
ROWS = 64
HALF = IMG // 2
CENTRE = IMG // 4
VIS = 256

ORDER = (
    (1, 2, 3, 6, 5, 7),
    (2, 3, 0, 7, 6, 5),
    (3, 1, 0, 5, 7, 6),
    (2, 1, 0, 5, 6, 7),
    (5, 6, 7, 2, 1, 3, 0),
    (4, 6, 7, 0, 2, 1, 3),
    (5, 7, 4, 0, 1, 2, 3),
    (6, 5, 0, 1, 4, 2, 3),
    (1, 2, 3, 7, 6, 8, 5, 4),
    (2, 3, 0, 7, 8, 6, 4, 5),
    (3, 1, 0, 8, 4, 5, 7, 6),
    (2, 1, 0, 8, 4, 5, 6, 7),
    (5, 6, 7, 2, 1, 3, 0),
    (4, 6, 7, 0, 2, 1, 3),
    (5, 7, 4, 0, 1, 2, 3),
    (6, 5, 0, 1, 4, 2, 3),
)


def sincos(turns):
    turns = turns - jnp.floor(turns + 0.5)
    square = turns * turns
    sine = jnp.full_like(turns, -(math.pi**11) / math.factorial(11))
    for order in (9, 7, 5, 3, 1):
        sign = 1.0 if order % 4 == 1 else -1.0
        sine = sine * square + sign * math.pi**order / math.factorial(order)
    sine = sine * turns
    cosine = jnp.full_like(turns, math.pi**12 / math.factorial(12))
    for order in (10, 8, 6, 4, 2, 0):
        sign = 1.0 if order % 4 == 0 else -1.0
        cosine = cosine * square + sign * math.pi**order / math.factorial(order)
    return 1.0 - 2.0 * sine * sine, 2.0 * sine * cosine


def times(a, b):
    return a[0] * b[0] - a[1] * b[1], a[0] * b[1] + a[1] * b[0]


def stack(a, b):
    return jnp.concatenate([a[0], b[0]], axis=0), jnp.concatenate([a[1], b[1]], axis=0)


def split(value):
    high = value.astype(jnp.bfloat16)
    return high, (value - high.astype(jnp.float32)).astype(jnp.bfloat16)


def taper_sum(taper, pixel):
    step = sincos(pixel * (1.0 / CELLS))
    total = (jnp.full_like(pixel, taper[SUP - 1]), jnp.zeros_like(pixel))
    for tap in range(SUP - 2, -1, -1):
        re, im = times(total, step)
        total = (re + taper[tap], im)
    return total


def rows_of(shape):
    return lax.broadcasted_iota(jnp.int32, shape, 0)


def lanes_of(shape):
    return lax.broadcasted_iota(jnp.int32, shape, 1)


def phases(fields, first_pixel, v_ref, w_ref):
    unit = 1.0 / CELLS
    row = rows_of((8, 128))

    def v_at(part, place):
        return v_ref.at[part, pl.ds(place, 16), :]

    def w_at(part, place):
        return w_ref.at[pl.ds(4 * ROWS * part + place, 16), :]

    rowf = row.astype(jnp.float32)
    power = jnp.where(row < 2, 8 << jnp.minimum(row, 1), jnp.where(row == 2, CENTRE, 16 << jnp.maximum(row - 3, 0)))
    power = jnp.where(row == 5, 1, power).astype(jnp.float32) * unit
    for lane in range(0, VIS, 128):
        re, im, x, y = (fields[i : i + 1, lane : lane + 128] for i in range(4))
        col = sincos((rowf + 0.5) * (y * unit))
        line = sincos(((first_pixel + 2.0 * rowf) * x - 0.5 * y) * unit)
        turn = sincos(power * jnp.where(row < 3, y, x))
        steps = [(turn[0][i : i + 1, :], turn[1][i : i + 1, :]) for i in range(6)]

        def store(ref, place, value):
            high, low = split(value)
            ref(0, place)[:, lane : lane + 128] = high
            ref(1, place)[:, lane : lane + 128] = low

        tile = stack(col, times(col, steps[0]))
        for i in range(CENTRE // 16):
            store(v_at, 16 * i, tile[0])
            store(v_at, CENTRE + 16 * i, tile[1])
            tile = times(tile, steps[1])
        line = times((re, im), line)
        tiles = [stack(line, times(line, steps[3]))]
        tiles.append(times(tiles[0], steps[4]))
        tiles += [times(tile, steps[5]) for tile in tiles]
        for i, tile in enumerate(tiles):
            rr, ii, ri, ir = (tile[a] * steps[2][b] for a, b in ((0, 0), (1, 1), (0, 1), (1, 0)))
            for place, value in ((0, rr + ii), (64, ir - ri), (128, rr - ii), (192, ri + ir)):
                store(w_at, place + 16 * i, value)


def early(place):
    core, y, x = place // 16, place // 4 % 4, place % 4
    return min(y, 4 - y) + min(x, 4 - x) + 0.5 * (1 - core) + (2 if place == 0 else 0)


def kernel(
    vis_hbm, dest_hbm, slot_hbm, off_hbm, taper_hbm, out_ref,
    vis, dest, slot, off, taper, fields, v_ref, w_ref, acc, tt, sends, recvs,
    load_sem, a_send, a_recv, b_send, b_recv, ready, chain, here, everyone,
):
    grp, au, vert = lax.axis_index("grp"), lax.axis_index("au"), lax.axis_index("vert")
    core, half = au % 2, au // 2
    z = half * 4 + grp
    y, x = vert // 4, vert % 4

    shifts = [(c, b, a) for c in range(2) for b in range(4) for a in range(4)]
    shifts.sort(key=lambda s: -(min(s[1], 4 - s[1]) + min(s[2], 4 - s[2]) + 0.5 * s[0]))
    shifts = shifts[:-1]

    def own_vert(shift):
        return ((y + shift[1]) % 4) * 4 + (x + shift[2]) % 4

    def own_peer(shift):
        return grp, half * 2 + (core + shift[0]) % 2, own_vert(shift)

    def signal(sem, peer):
        pl.semaphore_signal(sem, inc=1, device_id=peer, device_id_type=MESH)

    def ring_peer(there):
        other = (there // 4 + half) % 2
        return there % 4, there // 4 * 2 + (core + other) % 2, vert

    pair = own_peer((1, 0, 0))
    hub = grp, half * 2 + 1, 0
    is_hub = (core == 1) & (vert == 0)

    def greet_plane(sem):
        for shift in shifts:
            signal(sem, own_peer(shift))

    step = 1 - 2 * core
    before, after = z - step, z + step
    before_exists = (half == 1) & (before >= 4) & (before < RING)
    after_exists = (half == 1) & (after >= 4) & (after < RING)

    def signal_if(sem, wanted, peer):
        @pl.when(wanted)
        def _():
            signal(sem, peer)

    def wait_if(sem, count):
        @pl.when(count > 0)
        def _():
            pl.semaphore_wait(sem, count)

    turned = (z == 4) & (core == 1)

    def gather(there):
        straight = turned & (there < 4)
        place, target, line = ring_peer(there)
        slot_there = jnp.where(straight, RING, z)
        pltpu.make_async_remote_copy(
            src_ref=fields.at[z],
            dst_ref=fields.at[slot_there],
            send_sem=a_send,
            recv_sem=a_recv.at[slot_there],
            device_id=(place, target + straight.astype(jnp.int32), line),
            device_id_type=MESH,
        ).start()

    def gather_if(wanted, there):
        @pl.when(wanted)
        def _():
            gather(there)

    loads = [
        pltpu.make_async_copy(src, dst, load_sem.at[i])
        for i, (src, dst) in enumerate(
            ((vis_hbm, vis), (dest_hbm, dest), (slot_hbm, slot), (off_hbm, off), (taper_hbm, taper))
        )
    ]
    for load in loads:
        load.start()
    barrier = pltpu.get_barrier_semaphore()
    for there in range(1, RING):
        signal_if(barrier, ((half == 0) & (z < there)) | (after_exists & (there == after)), ring_peer(there))
    signal_if(barrier, (half == 0) & (core == 1), (0, 3, vert))
    pl.when(is_hub)(lambda: greet_plane(barrier))

    for load in loads[:4]:
        load.wait()
    target, tile = dest[...], slot[...]
    row0 = target // 16 * ROWS_DEV + tile // 4 * TILE + off[0:1, :]
    col0 = target % 16 * COLS_DEV + tile % 4 * TILE + off[1:2, :]
    fields[z, 0:2, :] = vis[...]
    fields[z, 2:3, :] = (row0 - CELLS // 2).astype(jnp.float32)
    fields[z, 3:4, :] = (col0 - CELLS // 2).astype(jnp.float32)

    lower = jnp.where(half == 0, z, 4 + before_exists.astype(jnp.int32) + jnp.where(turned, 4, 0))
    wait_if(barrier, lower + jnp.where(is_hub, 0, 1))
    def below(there):
        return ((there < z) & ((half == 0) | (there < 4))) | (before_exists & (there == before))

    for there in range(RING):
        gather_if(below(there), there)
    for there in range(RING):
        signal_if(ready.at[jnp.where(there // 4 == half, 0, 1)], below(there), ring_peer(there))
    signal_if(here, jnp.logical_not(is_hub), hub)

    position = grp * 2 + half
    first_pixel = (position * ROWS - HALF).astype(jnp.float32)

    def project(buffer, first=False):
        v, w = v_ref.at[buffer], w_ref.at[buffer]

        def product(a, b):
            return lax.dot_general(a, b, (((1,), (1,)), ((), ())), preferred_element_type=jnp.float32)

        both, cross = product(w[...], v[0]), product(w[0 : 4 * ROWS, :], v[1])
        if first:
            acc[0 : 8 * ROWS, :] = both
            acc[8 * ROWS :, :] = cross
        else:
            acc[0 : 8 * ROWS, :] += both
            acc[8 * ROWS :, :] += cross

    phases(fields.at[z], first_pixel, v_ref.at[0], w_ref.at[0])
    loads[4].wait()
    taps = [taper[i] for i in range(SUP)]
    lane, level = lanes_of((8, 128)), rows_of((8, 128))
    line_row = rows_of((ROWS, 128))
    line = taper_sum(taps, first_pixel + (2 * (line_row % 32) + line_row // 32).astype(jnp.float32))
    centre = CENTRE * (2 * (level % 2) - 1)
    columns = taper_sum(taps, centre + jnp.where(level < 2, lane, -1 - lane).astype(jnp.float32))
    norm = 1.0 / (SUP * math.sqrt(65536))
    for i in range(4):
        pair_re, pair_im = times(line, (columns[0][i : i + 1, :] * norm, columns[1][i : i + 1, :] * norm))
        tt[i, 0] = pair_re
        tt[i, 1] = pair_im
    @pl.when(half == 0)
    def _():
        wait_if(ready.at[0], 3 - grp)
        for there in range(1, 4):
            gather_if(there > z, there)

    @pl.when(half == 1)
    def _():
        wait_if(ready.at[0], after_exists.astype(jnp.int32))
        sides = [(grp + step >= 0) & (grp + step < 4) for step in (1, -1)]
        for there in range(4, RING):
            gather_if(after_exists & (there == after), there)
        for distance in (2, 3):
            for step, side in zip((1, -1), sides):
                signal_if(chain.at[distance - 2], side, ((grp + step) % 4, au, vert))
            pl.semaphore_wait(chain.at[distance - 2], sum(side.astype(jnp.int32) for side in sides))
            for there in range(4, RING):
                gather_if((there == z + distance) | (there == z - distance), there)

    @pl.when(is_hub)
    def _():
        pl.semaphore_wait(here, OWN - 1)
        greet_plane(everyone)

    def take(index):
        source = 0
        for place, order in enumerate(ORDER):
            if index <= len(order):
                source = jnp.where(z + RING * core == place, order[index - 1], source)
        pltpu.make_async_remote_copy(
            src_ref=fields.at[source],
            dst_ref=fields.at[source],
            send_sem=a_send,
            recv_sem=a_recv.at[source],
            device_id=pair,
            device_id_type=MESH,
        ).wait_recv()
        project((index - 1) % 2, index == 1)
        phases(fields.at[source], first_pixel, v_ref.at[index % 2], w_ref.at[index % 2])

    def rest_of(count):
        for index in range(3, count + 1):
            if index == 3 and count != 7:
                pl.semaphore_wait(ready.at[1], 4)
                for there in range(4, RING):
                    gather(there)

            take(index)
        project(count % 2)

    for index in range(1, 3):
        take(index)
    pl.when((half == 0) & (core == 0))(lambda: rest_of(6))
    pl.when(half == 1)(lambda: rest_of(7))
    pl.when((half == 0) & (core == 1))(lambda: rest_of(8))
    for c in range(2):
        re_cos, re_sin, im_cos, im_sin = (
            sum(acc[first + 4 * ROWS * i : first + 4 * ROWS * i + ROWS, place : place + 128] for i in range(3))
            for first in (128 * c, 128 * c + ROWS)
            for place in (0, 128)
        )
        sides = (re_cos - im_sin, im_cos + re_sin), (re_cos + im_sin, im_cos - re_sin)
        for side, (real, imag) in enumerate(sides):
            facet = tt[2 * side + c, 0] * real - tt[2 * side + c, 1] * imag
            for e in range(2):
                for t in range(4):
                    sends[pl.ds(64 * t + 4 * side + 2 * e + c, 8, stride=8), :] = facet[
                        32 * e + 8 * t : 32 * e + 8 * t + 8, :
                    ]

    wait_if(everyone, jnp.where(is_hub, 0, 1))
    mine = core * 16 + vert
    for place in sorted(range(OWN), key=early):
        there = grp, half * 2 + place // 16, place % 16

        @pl.when(mine != place)
        def _():
            pltpu.make_async_remote_copy(
                src_ref=sends.at[pl.ds(8 * place, 8), :],
                dst_ref=recvs.at[mine],
                send_sem=b_send,
                recv_sem=b_recv,
                device_id=there,
                device_id_type=MESH,
            ).start()

    recvs[mine] = sends[pl.ds(pl.multiple_of(8 * mine, 8), 8), :]
    others = recvs.at[pl.ds(1, OWN - 1)]
    batch = pltpu.make_async_remote_copy(
        src_ref=others, dst_ref=others, send_sem=b_send, recv_sem=b_recv, device_id=pair, device_id_type=MESH
    )
    batch.wait_recv()
    total = recvs[0]
    for i in range(1, OWN):
        total = total + recvs[i]
    mirrored = jnp.take_along_axis(total, 127 - lane, axis=1)
    for e in range(2):
        for c in range(2):
            out_ref[e : e + 1, 256 * c + 128 : 256 * c + 256] = total[2 * e + c : 2 * e + c + 1, :]
            out_ref[e : e + 1, 256 * c : 256 * c + 128] = mirrored[4 + 2 * e + c : 5 + 2 * e + c, :]
    batch.wait_send()
    rest = fields.at[pl.ds(1, RING - 1)]
    pltpu.make_async_remote_copy(
        src_ref=rest, dst_ref=rest, send_sem=a_send, recv_sem=a_recv.at[0], device_id=pair, device_id_type=MESH
    ).wait_send()


def body(visibility, destination, tile_slot, offsets, taper):
    any_space = pl.BlockSpec(memory_space=pl.ANY)
    return pl.pallas_call(
        kernel,
        out_shape=pltpu.VMEM((2, IMG), jnp.float32),
        in_specs=[any_space] * 5,
        out_specs=pl.BlockSpec(memory_space=pltpu.VMEM),
        scratch_shapes=[
            pltpu.VMEM((2, VIS), jnp.float32),
            pltpu.VMEM((1, VIS), jnp.int32),
            pltpu.VMEM((1, VIS), jnp.int32),
            pltpu.VMEM((2, VIS), jnp.int32),
            pltpu.SMEM((SUP,), jnp.float32),
            pltpu.VMEM((RING + 1, 4, VIS), jnp.float32),
            pltpu.VMEM((2, 2, 2 * CENTRE, VIS), jnp.bfloat16),
            pltpu.VMEM((2, 8 * ROWS, VIS), jnp.bfloat16),
            pltpu.VMEM((12 * ROWS, 2 * CENTRE), jnp.float32),
            pltpu.VMEM((4, 2, ROWS, 128), jnp.float32),
            pltpu.VMEM((OWN * 8, 128), jnp.float32),
            pltpu.VMEM((OWN, 8, 128), jnp.float32),
            pltpu.SemaphoreType.DMA((5,)),
            pltpu.SemaphoreType.DMA,
            pltpu.SemaphoreType.DMA((RING + 1,)),
            pltpu.SemaphoreType.DMA,
            pltpu.SemaphoreType.DMA,
            pltpu.SemaphoreType.REGULAR((2,)),
            pltpu.SemaphoreType.REGULAR((2,)),
            pltpu.SemaphoreType.REGULAR,
            pltpu.SemaphoreType.REGULAR,
        ],
        compiler_params=pltpu.CompilerParams(collective_id=0, has_side_effects=True),
    )(visibility.T, destination.T, tile_slot.reshape(1, -1), offsets.T, taper)


def solution(mesh):
    return jax.shard_map(
        body,
        mesh=mesh,
        in_specs=(
            P(("grp", "au", "vert"), None),
            P(("grp", "au", "vert"), None),
            P(("grp", "au", "vert")),
            P(("grp", "au", "vert"), None),
            P(),
        ),
        out_specs=P(("grp", "au", "vert"), None),
        check_vma=False,
    )
```

```python
import math

import jax
import jax.numpy as jnp
from jax import lax
from jax.experimental import pallas as pl
from jax.experimental.pallas import tpu as pltpu
from jax.sharding import PartitionSpec as P

TILE = 128
SUP = 8
ROWS_DEV = 2048
COLS_DEV = 512
IMG = 512
CELLS = 8192
MESH = pl.DeviceIdType.MESH

RING = 8
OWN = 32
ROWS = 64
HALF = IMG // 2
CENTRE = IMG // 4
VIS = 256

ORDER = (
    (1, 2, 3, 6, 5, 7),
    (2, 3, 0, 7, 6, 5),
    (3, 1, 0, 5, 7, 6),
    (2, 1, 0, 5, 6, 7),
    (5, 6, 7, 2, 1, 3, 0),
    (4, 6, 7, 0, 2, 1, 3),
    (5, 7, 4, 0, 1, 2, 3),
    (6, 5, 0, 1, 4, 2, 3),
    (1, 2, 3, 7, 6, 8, 5, 4),
    (2, 3, 0, 7, 8, 6, 4, 5),
    (3, 1, 0, 8, 4, 5, 7, 6),
    (2, 1, 0, 8, 4, 5, 6, 7),
    (5, 6, 7, 2, 1, 3, 0),
    (4, 6, 7, 0, 2, 1, 3),
    (5, 7, 4, 0, 1, 2, 3),
    (6, 5, 0, 1, 4, 2, 3),
)


def sincos(turns):
    turns = turns - jnp.floor(turns + 0.5)
    square = turns * turns
    sine = jnp.full_like(turns, -(math.pi**11) / math.factorial(11))
    for order in (9, 7, 5, 3, 1):
        sign = 1.0 if order % 4 == 1 else -1.0
        sine = sine * square + sign * math.pi**order / math.factorial(order)
    sine = sine * turns
    cosine = jnp.full_like(turns, math.pi**12 / math.factorial(12))
    for order in (10, 8, 6, 4, 2, 0):
        sign = 1.0 if order % 4 == 0 else -1.0
        cosine = cosine * square + sign * math.pi**order / math.factorial(order)
    return 1.0 - 2.0 * sine * sine, 2.0 * sine * cosine


def times(a, b):
    return a[0] * b[0] - a[1] * b[1], a[0] * b[1] + a[1] * b[0]


def stack(a, b):
    return jnp.concatenate([a[0], b[0]], axis=0), jnp.concatenate([a[1], b[1]], axis=0)


def split(value):
    high = value.astype(jnp.bfloat16)
    return high, (value - high.astype(jnp.float32)).astype(jnp.bfloat16)


def taper_sum(taper, pixel):
    step = sincos(pixel * (1.0 / CELLS))
    total = (jnp.full_like(pixel, taper[SUP - 1]), jnp.zeros_like(pixel))
    for tap in range(SUP - 2, -1, -1):
        re, im = times(total, step)
        total = (re + taper[tap], im)
    return total


def rows_of(shape):
    return lax.broadcasted_iota(jnp.int32, shape, 0)


def lanes_of(shape):
    return lax.broadcasted_iota(jnp.int32, shape, 1)


def phases(fields, first_pixel, v_ref, w_ref):
    unit = 1.0 / CELLS
    row = rows_of((8, 128))

    def v_at(part, place):
        return v_ref.at[part, pl.ds(place, 16), :]

    def w_at(part, place):
        return w_ref.at[pl.ds(4 * ROWS * part + place, 16), :]

    rowf = row.astype(jnp.float32)
    power = jnp.where(row < 2, 8 << jnp.minimum(row, 1), jnp.where(row == 2, CENTRE, 16 << jnp.maximum(row - 3, 0)))
    power = jnp.where(row == 5, 1, power).astype(jnp.float32) * unit
    for lane in range(0, VIS, 128):
        re, im, x, y = (fields[i : i + 1, lane : lane + 128] for i in range(4))
        col = sincos((rowf + 0.5) * (y * unit))
        line = sincos(((first_pixel + 2.0 * rowf) * x - 0.5 * y) * unit)
        turn = sincos(power * jnp.where(row < 3, y, x))
        steps = [(turn[0][i : i + 1, :], turn[1][i : i + 1, :]) for i in range(6)]

        def store(ref, place, value):
            high, low = split(value)
            ref(0, place)[:, lane : lane + 128] = high
            ref(1, place)[:, lane : lane + 128] = low

        tile = stack(col, times(col, steps[0]))
        for i in range(CENTRE // 16):
            store(v_at, 16 * i, tile[0])
            store(v_at, CENTRE + 16 * i, tile[1])
            tile = times(tile, steps[1])
        line = times((re, im), line)
        tiles = [stack(line, times(line, steps[3]))]
        tiles.append(times(tiles[0], steps[4]))
        tiles += [times(tile, steps[5]) for tile in tiles]
        for i, tile in enumerate(tiles):
            rr, ii, ri, ir = (tile[a] * steps[2][b] for a, b in ((0, 0), (1, 1), (0, 1), (1, 0)))
            for place, value in ((0, rr + ii), (64, ir - ri), (128, rr - ii), (192, ri + ir)):
                store(w_at, place + 16 * i, value)


def kernel(
    vis_hbm, dest_hbm, slot_hbm, off_hbm, taper_hbm, out_ref,
    vis, dest, slot, off, taper, fields, v_ref, w_ref, acc, tt, sends, recvs,
    load_sem, a_send, a_recv, b_send, b_recv, ready, chain, here, everyone,
):
    grp, au, vert = lax.axis_index("grp"), lax.axis_index("au"), lax.axis_index("vert")
    core, half = au % 2, au // 2
    z = half * 4 + grp
    y, x = vert // 4, vert % 4

    shifts = [(c, b, a) for c in range(2) for b in range(4) for a in range(4)]
    shifts.sort(key=lambda s: -(min(s[1], 4 - s[1]) + min(s[2], 4 - s[2]) + 0.5 * s[0]))
    shifts = shifts[:-1]

    def own_vert(shift):
        return ((y + shift[1]) % 4) * 4 + (x + shift[2]) % 4

    def own_peer(shift):
        return grp, half * 2 + (core + shift[0]) % 2, own_vert(shift)

    def signal(sem, peer):
        pl.semaphore_signal(sem, inc=1, device_id=peer, device_id_type=MESH)

    def ring_peer(there):
        other = (there // 4 + half) % 2
        return there % 4, there // 4 * 2 + (core + other) % 2, vert

    pair = own_peer((1, 0, 0))
    hub = grp, half * 2 + 1, 0
    is_hub = (core == 1) & (vert == 0)

    def greet_plane(sem):
        for shift in shifts:
            signal(sem, own_peer(shift))

    step = 1 - 2 * core
    before, after = z - step, z + step
    before_exists = (half == 1) & (before >= 4) & (before < RING)
    after_exists = (half == 1) & (after >= 4) & (after < RING)

    def signal_if(sem, wanted, peer):
        @pl.when(wanted)
        def _():
            signal(sem, peer)

    def wait_if(sem, count):
        @pl.when(count > 0)
        def _():
            pl.semaphore_wait(sem, count)

    turned = (z == 4) & (core == 1)

    def gather(there):
        straight = turned & (there < 4)
        place, target, line = ring_peer(there)
        slot_there = jnp.where(straight, RING, z)
        pltpu.make_async_remote_copy(
            src_ref=fields.at[z],
            dst_ref=fields.at[slot_there],
            send_sem=a_send,
            recv_sem=a_recv.at[slot_there],
            device_id=(place, target + straight.astype(jnp.int32), line),
            device_id_type=MESH,
        ).start()

    def gather_if(wanted, there):
        @pl.when(wanted)
        def _():
            gather(there)

    loads = [
        pltpu.make_async_copy(src, dst, load_sem.at[i])
        for i, (src, dst) in enumerate(
            ((vis_hbm, vis), (dest_hbm, dest), (slot_hbm, slot), (off_hbm, off), (taper_hbm, taper))
        )
    ]
    for load in loads:
        load.start()
    barrier = pltpu.get_barrier_semaphore()
    for there in range(1, RING):
        signal_if(barrier, ((half == 0) & (z < there)) | (after_exists & (there == after)), ring_peer(there))
    signal_if(barrier, (half == 0) & (core == 1), (0, 3, vert))
    pl.when(is_hub)(lambda: greet_plane(barrier))

    for load in loads[:4]:
        load.wait()
    target, tile = dest[...], slot[...]
    row0 = target // 16 * ROWS_DEV + tile // 4 * TILE + off[0:1, :]
    col0 = target % 16 * COLS_DEV + tile % 4 * TILE + off[1:2, :]
    fields[z, 0:2, :] = vis[...]
    fields[z, 2:3, :] = (row0 - CELLS // 2).astype(jnp.float32)
    fields[z, 3:4, :] = (col0 - CELLS // 2).astype(jnp.float32)

    lower = jnp.where(half == 0, z, 4 + before_exists.astype(jnp.int32) + jnp.where(turned, 4, 0))
    wait_if(barrier, lower + jnp.where(is_hub, 0, 1))
    def below(there):
        return ((there < z) & ((half == 0) | (there < 4))) | (before_exists & (there == before))

    for there in range(RING):
        gather_if(below(there), there)
    for there in range(RING):
        signal_if(ready.at[jnp.where(there // 4 == half, 0, 1)], below(there), ring_peer(there))
    signal_if(here, jnp.logical_not(is_hub), hub)

    position = grp * 2 + half
    first_pixel = (position * ROWS - HALF).astype(jnp.float32)

    def project(buffer, first=False):
        v, w = v_ref.at[buffer], w_ref.at[buffer]

        def product(a, b):
            return lax.dot_general(a, b, (((1,), (1,)), ((), ())), preferred_element_type=jnp.float32)

        both, cross = product(w[...], v[0]), product(w[0 : 4 * ROWS, :], v[1])
        if first:
            acc[0 : 8 * ROWS, :] = both
            acc[8 * ROWS :, :] = cross
        else:
            acc[0 : 8 * ROWS, :] += both
            acc[8 * ROWS :, :] += cross

    phases(fields.at[z], first_pixel, v_ref.at[0], w_ref.at[0])
    loads[4].wait()
    taps = [taper[i] for i in range(SUP)]
    lane, level = lanes_of((8, 128)), rows_of((8, 128))
    line_row = rows_of((ROWS, 128))
    line = taper_sum(taps, first_pixel + (2 * (line_row % 32) + line_row // 32).astype(jnp.float32))
    centre = CENTRE * (2 * (level % 2) - 1)
    columns = taper_sum(taps, centre + jnp.where(level < 2, lane, -1 - lane).astype(jnp.float32))
    norm = 1.0 / (SUP * math.sqrt(65536))
    for i in range(4):
        pair_re, pair_im = times(line, (columns[0][i : i + 1, :] * norm, columns[1][i : i + 1, :] * norm))
        tt[i, 0] = pair_re
        tt[i, 1] = pair_im
    @pl.when(half == 0)
    def _():
        wait_if(ready.at[0], 3 - grp)
        for there in range(1, 4):
            gather_if(there > z, there)

    @pl.when(half == 1)
    def _():
        wait_if(ready.at[0], after_exists.astype(jnp.int32))
        sides = [(grp + step >= 0) & (grp + step < 4) for step in (1, -1)]
        for there in range(4, RING):
            gather_if(after_exists & (there == after), there)
        for distance in (2, 3):
            for step, side in zip((1, -1), sides):
                signal_if(chain.at[distance - 2], side, ((grp + step) % 4, au, vert))
            pl.semaphore_wait(chain.at[distance - 2], sum(side.astype(jnp.int32) for side in sides))
            for there in range(4, RING):
                gather_if((there == z + distance) | (there == z - distance), there)

    @pl.when(is_hub)
    def _():
        pl.semaphore_wait(here, OWN - 1)
        greet_plane(everyone)

    def take(index):
        source = 0
        for place, order in enumerate(ORDER):
            if index <= len(order):
                source = jnp.where(z + RING * core == place, order[index - 1], source)
        pltpu.make_async_remote_copy(
            src_ref=fields.at[source],
            dst_ref=fields.at[source],
            send_sem=a_send,
            recv_sem=a_recv.at[source],
            device_id=pair,
            device_id_type=MESH,
        ).wait_recv()
        project((index - 1) % 2, index == 1)
        phases(fields.at[source], first_pixel, v_ref.at[index % 2], w_ref.at[index % 2])

    def rest_of(count):
        for index in range(3, count + 1):
            if index == 3 and count != 7:
                pl.semaphore_wait(ready.at[1], 4)
                for there in range(4, RING):
                    gather(there)

            take(index)
        project(count % 2)

    for index in range(1, 3):
        take(index)
    pl.when((half == 0) & (core == 0))(lambda: rest_of(6))
    pl.when(half == 1)(lambda: rest_of(7))
    pl.when((half == 0) & (core == 1))(lambda: rest_of(8))
    for c in range(2):
        re_cos, re_sin, im_cos, im_sin = (
            sum(acc[first + 4 * ROWS * i : first + 4 * ROWS * i + ROWS, place : place + 128] for i in range(3))
            for first in (128 * c, 128 * c + ROWS)
            for place in (0, 128)
        )
        sides = (re_cos - im_sin, im_cos + re_sin), (re_cos + im_sin, im_cos - re_sin)
        for side, (real, imag) in enumerate(sides):
            facet = tt[2 * side + c, 0] * real - tt[2 * side + c, 1] * imag
            for e in range(2):
                for t in range(4):
                    sends[pl.ds(64 * t + 4 * side + 2 * e + c, 8, stride=8), :] = facet[
                        32 * e + 8 * t : 32 * e + 8 * t + 8, :
                    ]

    wait_if(everyone, jnp.where(is_hub, 0, 1))
    mine = core * 16 + vert
    for shift in shifts:
        start = pl.multiple_of(8 * ((core + shift[0]) % 2 * 16 + own_vert(shift)), 8)
        pltpu.make_async_remote_copy(
            src_ref=sends.at[pl.ds(start, 8), :],
            dst_ref=recvs.at[mine],
            send_sem=b_send,
            recv_sem=b_recv,
            device_id=own_peer(shift),
            device_id_type=MESH,
        ).start()
    recvs[mine] = sends[pl.ds(pl.multiple_of(8 * mine, 8), 8), :]
    others = recvs.at[pl.ds(1, OWN - 1)]
    batch = pltpu.make_async_remote_copy(
        src_ref=others, dst_ref=others, send_sem=b_send, recv_sem=b_recv, device_id=pair, device_id_type=MESH
    )
    batch.wait_recv()
    total = recvs[0]
    for i in range(1, OWN):
        total = total + recvs[i]
    mirrored = jnp.take_along_axis(total, 127 - lane, axis=1)
    for e in range(2):
        for c in range(2):
            out_ref[e : e + 1, 256 * c + 128 : 256 * c + 256] = total[2 * e + c : 2 * e + c + 1, :]
            out_ref[e : e + 1, 256 * c : 256 * c + 128] = mirrored[4 + 2 * e + c : 5 + 2 * e + c, :]
    batch.wait_send()
    rest = fields.at[pl.ds(1, RING - 1)]
    pltpu.make_async_remote_copy(
        src_ref=rest, dst_ref=rest, send_sem=a_send, recv_sem=a_recv.at[0], device_id=pair, device_id_type=MESH
    ).wait_send()


def body(visibility, destination, tile_slot, offsets, taper):
    any_space = pl.BlockSpec(memory_space=pl.ANY)
    return pl.pallas_call(
        kernel,
        out_shape=pltpu.VMEM((2, IMG), jnp.float32),
        in_specs=[any_space] * 5,
        out_specs=pl.BlockSpec(memory_space=pltpu.VMEM),
        scratch_shapes=[
            pltpu.VMEM((2, VIS), jnp.float32),
            pltpu.VMEM((1, VIS), jnp.int32),
            pltpu.VMEM((1, VIS), jnp.int32),
            pltpu.VMEM((2, VIS), jnp.int32),
            pltpu.SMEM((SUP,), jnp.float32),
            pltpu.VMEM((RING + 1, 4, VIS), jnp.float32),
            pltpu.VMEM((2, 2, 2 * CENTRE, VIS), jnp.bfloat16),
            pltpu.VMEM((2, 8 * ROWS, VIS), jnp.bfloat16),
            pltpu.VMEM((12 * ROWS, 2 * CENTRE), jnp.float32),
            pltpu.VMEM((4, 2, ROWS, 128), jnp.float32),
            pltpu.VMEM((OWN * 8, 128), jnp.float32),
            pltpu.VMEM((OWN, 8, 128), jnp.float32),
            pltpu.SemaphoreType.DMA((5,)),
            pltpu.SemaphoreType.DMA,
            pltpu.SemaphoreType.DMA((RING + 1,)),
            pltpu.SemaphoreType.DMA,
            pltpu.SemaphoreType.DMA,
            pltpu.SemaphoreType.REGULAR((2,)),
            pltpu.SemaphoreType.REGULAR((2,)),
            pltpu.SemaphoreType.REGULAR,
            pltpu.SemaphoreType.REGULAR,
        ],
        compiler_params=pltpu.CompilerParams(collective_id=0, has_side_effects=True),
    )(visibility.T, destination.T, tile_slot.reshape(1, -1), offsets.T, taper)


def solution(mesh):
    return jax.shard_map(
        body,
        mesh=mesh,
        in_specs=(
            P(("grp", "au", "vert"), None),
            P(("grp", "au", "vert"), None),
            P(("grp", "au", "vert")),
            P(("grp", "au", "vert"), None),
            P(),
        ),
        out_specs=P(("grp", "au", "vert"), None),
        check_vma=False,
    )
```
